16 devices in a mesh: dp: 2 (over y, z), tp: 8 (over x, core).
Axes of the slice: x: 4, y: 2, z: 1, core: 2. Of those that a mesh axis runs over, the one named last changes fastest.
The devices are a block of a 4x4x8 slice.
Arguments:
- x_seq: bfloat16 [8, 2048, 4096], P('dp', 'tp'), parts along dimension 0
- ln_gain: float32 [4096], replicated
- ln_bias: float32 [4096], replicated
- w_qkv: bfloat16 [4096, 16, 3, 256], P(None, 'tp')
- w_out: bfloat16 [4096, 4096], P('tp')
- w_up: bfloat16 [4096, 16384], P(None, 'tp')
- w_down: bfloat16 [16384, 4096], P('tp')
Outputs:
- output: bfloat16 [8, 2048, 4096], P('dp', 'tp'), parts along dimension 0
There are 2 independent parts. The reference program is written for one: setup_inputs(seed, part) draws one part's arguments, and reference() takes and returns one part's arrays. A program takes and returns all parts, laid end to end along the dimension named above; an argument that names none is the same for every part.
All inputs are finite; a program needn't handle non-finite values.
Results may differ from the reference program's by a relative error of at most 0.011671.
Values are sent between devices in bfloat16 or wider.
A program may use at most 768 MiB of HBM per device.

```python
import jax
import jax.numpy as jnp
from jax import lax

D = 4096
HEADS = 16
KV_HEADS = 16
HEAD = 256
FF = 16384
BATCH = 4
SEQ = 2048

LN_EPS = 1e-5
GROUP_Q = HEADS // KV_HEADS


def normal_weights(key_w, shape, fan_in):
    return (jax.random.normal(key_w, shape, jnp.float32) * fan_in ** -0.5).astype(jnp.bfloat16)


def setup_inputs(seed: int = 0, part: int = 0) -> dict:
    root_key = jax.random.key(seed)
    key_x, key_c, key_g, key_b, key_qkv, key_o, key_up, key_dn = jax.random.split(root_key, 8)
    key_x = jax.random.fold_in(key_x, part)
    key_c = jax.random.fold_in(key_c, part)
    noise = jax.random.normal(key_x, (BATCH, SEQ, D), jnp.float32)
    shared = jax.random.normal(key_c, (BATCH, 1, D), jnp.float32)
    x_seq = ((noise + shared) * 0.7071).astype(jnp.bfloat16)
    ln_gain = 1.0 + 0.5 * jax.random.normal(key_g, (D,), jnp.float32)
    ln_bias = 0.5 * jax.random.normal(key_b, (D,), jnp.float32)
    w_qkv = normal_weights(key_qkv, (D, KV_HEADS, GROUP_Q + 2, HEAD), D)
    w_out = normal_weights(key_o, (HEADS * HEAD, D), HEADS * HEAD)
    w_up = normal_weights(key_up, (D, FF), D)
    w_down = normal_weights(key_dn, (FF, D), FF)
    return {"x_seq": x_seq, "ln_gain": ln_gain, "ln_bias": ln_bias, "w_qkv": w_qkv,
            "w_out": w_out, "w_up": w_up, "w_down": w_down}


def layer_norm(x_f32, ln_gain, ln_bias):
    row_mean = jnp.mean(x_f32, axis=-1, keepdims=True)
    centered = x_f32 - row_mean
    variance = jnp.mean(centered * centered, axis=-1, keepdims=True)
    return centered * lax.rsqrt(variance + LN_EPS) * ln_gain + ln_bias


def reference(x_seq, ln_gain, ln_bias, w_qkv, w_out, w_up, w_down):
    tokens = x_seq.reshape(BATCH * SEQ, D)
    normed = layer_norm(tokens.astype(jnp.float32), ln_gain, ln_bias).astype(jnp.bfloat16)
    proj_qkv = jnp.dot(normed, w_qkv.reshape(D, KV_HEADS * (GROUP_Q + 2) * HEAD),
                       preferred_element_type=jnp.float32).astype(jnp.bfloat16)
    proj_qkv = proj_qkv.reshape(BATCH, SEQ, KV_HEADS, GROUP_Q + 2, HEAD)
    proj_qkv = proj_qkv.transpose(0, 2, 3, 1, 4).reshape(BATCH * KV_HEADS, GROUP_Q + 2, SEQ, HEAD)
    causal = jnp.arange(SEQ)[:, None] >= jnp.arange(SEQ)[None, :]

    def one_group(group_item):
        query_rows = group_item[:GROUP_Q].astype(jnp.float32)
        key_rows = group_item[GROUP_Q].astype(jnp.float32)
        value_rows = group_item[GROUP_Q + 1].astype(jnp.float32)
        scores = jnp.einsum("jsh,th->jst", query_rows, key_rows) * (HEAD ** -0.5)
        scores = jnp.where(causal, scores, -jnp.inf)
        attn_prob = jax.nn.softmax(scores, axis=-1).astype(jnp.bfloat16)
        context = jnp.einsum("jst,th->jsh", attn_prob.astype(jnp.float32), value_rows)
        return context.astype(jnp.bfloat16)

    context = lax.map(one_group, proj_qkv)
    context = context.reshape(BATCH, KV_HEADS, GROUP_Q, SEQ, HEAD).transpose(0, 3, 1, 2, 4)
    context = context.reshape(BATCH * SEQ, HEADS * HEAD)
    attn_part = jnp.dot(context, w_out, preferred_element_type=jnp.float32)
    hidden = jnp.dot(normed, w_up, preferred_element_type=jnp.float32)
    activated = jax.nn.gelu(hidden, approximate=False).astype(jnp.bfloat16)
    mlp_part = jnp.dot(activated, w_down, preferred_element_type=jnp.float32)
    branch = (attn_part + mlp_part).astype(jnp.bfloat16)
    out_rows = (tokens.astype(jnp.float32) + branch.astype(jnp.float32)).astype(jnp.bfloat16)
    return out_rows.reshape(BATCH, SEQ, D)
```

```python
import functools

import jax
import jax.numpy as jnp
from jax import lax
from jax.experimental import pallas as pl
from jax.experimental.pallas import tpu as pltpu
from jax.sharding import PartitionSpec as P

LN_EPS = 1e-5
NJ = 4


def layer_kernel(x_ref, gain_ref, bias_ref, wqkv_hbm, wout_hbm, wup_hbm, wdown_hbm,
                 own_out, left_out, right_out, n_all, ho, pbuf, pout, tin,
                 wqkv, wup, wdo, gain, bias,
                 ag_is, ag_ir, ag_ds, ag_dr, p_s, p_r, t_s, t_r, m_s, m_r,
                 w_sem, v_sem, ln_sem, a_sem, h_sem, o_sem, d_sem, pb_sem, os_sem, f_sem):
    batch, rows, dim = x_ref.shape
    half = rows // 2
    ff = wup.shape[1]
    attn = wdo.shape[0] - ff
    qkv_cols = wqkv.shape[1]
    n_heads = 2
    head = attn // n_heads
    n_chips = n_all.shape[1]
    seq = n_chips * 2 * rows
    ncol = dim // NJ
    f32, bf16 = jnp.float32, jnp.bfloat16

    me = lax.axis_index("tp")
    chip, core = me // 2, me % 2
    other = 1 - core
    partner = chip * 2 + other
    right = ((chip + 1) % n_chips) * 2 + core
    left = ((chip + n_chips - 1) % n_chips) * 2 + core

    def remote(src, dst, send, recv, dev):
        return pltpu.make_async_remote_copy(
            src_ref=src, dst_ref=dst, send_sem=send, recv_sem=recv,
            device_id={"tp": dev}, device_id_type=pl.DeviceIdType.MESH)

    barrier = pltpu.get_barrier_semaphore()
    for dev in (partner, right, left):
        pl.semaphore_signal(barrier, inc=1, device_id={"tp": dev}, device_id_type=pl.DeviceIdType.MESH)
    pl.semaphore_wait(barrier, 3)

    w_copies = (
        pltpu.make_async_copy(wqkv_hbm, wqkv, w_sem.at[0]),
        pltpu.make_async_copy(wup_hbm, wup, w_sem.at[1]),
        pltpu.make_async_copy(wdown_hbm, wdo.at[pl.ds(0, ff)], w_sem.at[2]),
        pltpu.make_async_copy(wout_hbm, wdo.at[pl.ds(ff, attn)], w_sem.at[3]),
    )
    v_copies = (pltpu.make_async_copy(gain_ref, gain, v_sem.at[0]),
                pltpu.make_async_copy(bias_ref, bias, v_sem.at[1]))
    for cp in v_copies:
        cp.start()

    def unit(u):
        g, b = u // 2, u % 2
        near = (g * (3 - g)) // 2
        off = near * (2 * b - 1) + 2 * (g // 3)
        hf = (b + near * (g - 1)) % 2
        return (chip + off + n_chips) % n_chips, hf

    def piece(s, d, hf, k):
        return n_all.at[s, d, hf, pl.ds(pl.multiple_of(k * half, half), half)]

    def ici_copy(s, u, d, hf, dev):
        return remote(piece(s, d, hf, core), piece(s, d, hf, core), ag_is.at[s, u], ag_ir.at[s, u], dev)

    def d2d_copy(s, u, d, hf, k):
        return remote(piece(s, d, hf, k), piece(s, d, hf, k), ag_ds.at[s, u], ag_dr.at[s, u], partner)

    def ag_send(s, buf):
        part, step = rows // 4, 32

        def load(q):
            at = pl.ds(q * part, part)
            return pltpu.make_async_copy(x_ref.at[s, at], buf.at[at], ln_sem.at[0, q])

        def store(q):
            dst = n_all.at[s, chip, q // 2, pl.ds(pl.multiple_of(core * half + (q % 2) * part, part), part)]
            return pltpu.make_async_copy(buf.at[pl.ds(q * part, part)], dst, ln_sem.at[1, q])

        for q in range(4):
            load(q).start()
        for q in range(4):
            load(q).wait()

            @pl.loop(0, part // step)
            def _(r):
                at = pl.ds(pl.multiple_of(q * part + r * step, step), step)
                v = buf[at, :].astype(f32)
                mean = jnp.mean(v, axis=-1, keepdims=True)
                cen = v - mean
                var = jnp.mean(cen * cen, axis=-1, keepdims=True)
                buf[at, :] = (cen * lax.rsqrt(var + LN_EPS) * gain[...] + bias[...]).astype(bf16)
            store(q).start()
        for q in range(4):
            store(q).wait()
        ici_copy(s, 2, chip, 0, right).start()
        ici_copy(s, 3, chip, 1, left).start()
        d2d_copy(s, 0, chip, 0, core).start()
        d2d_copy(s, 1, chip, 1, core).start()
        ici_copy(s, 4, chip, 1, right).start()
        ici_copy(s, 5, chip, 0, left).start()

    def forward(s, us):
        for u in us:
            d, hf = unit(u)
            ici_copy(s, u, d, hf, right).wait_recv()
            if u == 2:
                ici_copy(s, 6, d, hf, right).start()
            if u == 3:
                ici_copy(s, 7, d, hf, left).start()
            d2d_copy(s, u, d, hf, core).start()

    def dest(i):
        is2 = (i * (i - 1) * (3 - i) * (4 - i)) // 4
        is3 = (i * (i - 1) * (i - 2) * (4 - i)) // 6
        return (chip + 2 - i + 3 * is2 + is3 + n_chips) % n_chips

    def cols(j):
        return pl.ds(pl.multiple_of(j * ncol, ncol), ncol)

    def to_right(s, ii, j):
        return remote(pout.at[s, ii, :, cols(j)], left_out.at[s, :, cols(j)], m_s.at[s, j], m_r.at[s, j], right)

    def to_left(s, ii, j):
        return remote(pout.at[s, ii, :, cols(j)], right_out.at[s, :, cols(j)], m_s.at[s, NJ + j], m_r.at[s, NJ + j],
                      left)

    def transit(s, j, dev):
        return remote(pout.at[s, 0, :, cols(j)], tin.at[s, :, cols(j)], t_s.at[s, j], t_r.at[s, j], dev)

    def relay(s):
        def scope(a, b):
            def loads(j):
                return (pltpu.make_async_copy(pout.at[s, 1 + j // 2, :, cols(j)], a.at[j % 2], f_sem.at[0, j % 2]),
                        pltpu.make_async_copy(tin.at[s, :, cols(j)], b.at[j % 2], f_sem.at[1, j % 2]))

            def store(j):
                return pltpu.make_async_copy(a.at[j % 2], pout.at[s, 1 + j // 2, :, cols(j)], f_sem.at[2, j % 2])

            def send(j):
                return to_right(s, 1, j) if j < NJ // 2 else to_left(s, 2, j)

            order = tuple(range(NJ))
            for n, j in enumerate(order):
                if n == 0:
                    transit(s, j, right).wait_recv()
                    for cp in loads(j):
                        cp.start()
                if n >= 1:
                    store(order[n - 1]).wait()
                    send(order[n - 1]).start()
                if n + 1 < NJ:
                    transit(s, order[n + 1], right).wait_recv()
                    for cp in loads(order[n + 1]):
                        cp.start()
                for cp in loads(j):
                    cp.wait()
                step = 64

                @pl.loop(0, rows // step)
                def _(r):
                    at = pl.ds(pl.multiple_of(r * step, step), step)
                    a[j % 2, at, :] = (a[j % 2, at, :].astype(f32) + b[j % 2, at, :].astype(f32)).astype(bf16)
                store(j).start()
            store(order[-1]).wait()
            send(order[-1]).start()
        pl.run_scoped(scope, pltpu.VMEM((2, rows, ncol), bf16), pltpu.VMEM((2, rows, ncol), bf16))

    def phase_a(s, qkv):
        def scope(nbuf, hbuf):
            def load(u):
                d, hf = unit(u)
                return pltpu.make_async_copy(n_all.at[s, d, hf], nbuf.at[u % 2], a_sem.at[u % 2])

            def arrived(u):
                d, hf = unit(u)
                d2d_copy(s, u, d, hf, other).wait_recv()

            def hstore(u, k):
                d, hf = unit(u)
                return pltpu.make_async_copy(
                    hbuf.at[u % 2, pl.ds(k * half, half)],
                    ho.at[2 * d + k, pl.ds(pl.multiple_of(hf * half, half), half), pl.ds(0, ff)],
                    h_sem.at[u % 2, k])

            arrived(0)
            load(0).start()

            @pl.loop(0, 2 * n_chips)
            def _(u):
                load(u).wait()

                @pl.when(jnp.logical_and(s > 0, u == 3))
                def _():
                    forward(s, (6, 7))

                @pl.when(jnp.logical_and(s > 0, u < 7))
                def _():
                    arrived(u + 1)
                    load(u + 1).start()

                @pl.when(u >= 2)
                def _():
                    for k in range(2):
                        hstore(u - 2, k).wait()

                @pl.when(jnp.logical_and(s == 0, u == 0))
                def _():
                    w_copies[0].wait()
                    w_copies[1].wait()

                d, hf = unit(u)
                slot = u % 2
                r = jnp.dot(nbuf[slot], wqkv[...], preferred_element_type=f32).astype(bf16)
                for k in range(2):
                    pos = pl.multiple_of(d * (2 * rows) + k * rows + hf * half, half)
                    qkv[pl.ds(pos, half), :] = r[k * half:(k + 1) * half]
                h = jnp.dot(nbuf[slot], wup[...], preferred_element_type=f32)
                hbuf[slot] = (0.5 * h * (1.0 + lax.erf(h * (2.0 ** -0.5)))).astype(bf16)
                for k in range(2):
                    hstore(u, k).start()

                @pl.when(s == 0)
                def _():
                    @pl.when(u == 1)
                    def _():
                        forward(0, (2, 3))
                        ag_send(1, nbuf.at[0])

                    @pl.when(u == 3)
                    def _():
                        forward(0, (4, 5))

                    @pl.when(u == 5)
                    def _():
                        forward(0, (6, 7))

                    @pl.when(u < 7)
                    def _():
                        arrived(u + 1)
                        load(u + 1).start()

            for u in (6, 7):
                for k in range(2):
                    hstore(u, k).wait()
        pl.run_scoped(scope, pltpu.VMEM((2, rows, dim), bf16), pltpu.VMEM((2, rows, ff), bf16))

    def phase_b(qkv):
        def ostore(t):
            return pltpu.make_async_copy(qkv.at[pl.ds(t * rows, rows), pl.ds(0, attn)],
                                         ho.at[t, :, pl.ds(ff, attn)], o_sem.at[t])
        scale = head ** -0.5

        def scope(scores, probs):
            keep = (lax.broadcasted_iota(jnp.int32, (rows, rows), 0)
                    >= lax.broadcasted_iota(jnp.int32, (rows, rows), 1))
            for t in range(seq // rows):
                r0, n = t * rows, (t + 1) * rows
                tops = []
                for h in range(n_heads):
                    q = qkv[r0:r0 + rows, h * head:(h + 1) * head]
                    k = qkv[0:n, attn + h * head:attn + (h + 1) * head]
                    sc = lax.dot_general(q, k, (((1,), (1,)), ((), ())), preferred_element_type=f32)
                    diag = jnp.where(keep, sc[:, n - rows:], -jnp.inf)
                    top = jnp.max(diag, axis=1, keepdims=True)
                    if t:
                        scores[h, :, 0:n - rows] = sc[:, :n - rows]
                        top = jnp.maximum(top, jnp.max(sc[:, :n - rows], axis=1, keepdims=True))
                    scores[h, :, n - rows:n] = diag
                    tops.append(top)
                for h in range(n_heads):
                    v = qkv[0:n, 2 * attn + h * head:2 * attn + (h + 1) * head]
                    total = jnp.zeros((rows, 1), f32)
                    for c in range(0, n, rows):
                        e = jnp.exp((scores[h, :, c:c + rows] - tops[h]) * scale)
                        scores[h, :, c:c + rows] = e
                        total = total + jnp.sum(e, axis=1, keepdims=True)
                    inverse = 1.0 / total
                    for c in range(0, n, rows):
                        probs[h, :, c:c + rows] = (scores[h, :, c:c + rows] * inverse).astype(bf16)
                    o = jnp.dot(probs[h, :, 0:n], v, preferred_element_type=f32)
                    qkv[r0:r0 + rows, h * head:(h + 1) * head] = o.astype(bf16)
                if t % 4 == 3:
                    for done in range(t - 3, t + 1):
                        ostore(done).start()
            for t in range(seq // rows):
                ostore(t).wait()
        pl.run_scoped(scope, pltpu.VMEM((n_heads, rows, seq), f32), pltpu.VMEM((n_heads, rows, seq), bf16))

    def phase_d(s):
        def scope(lhs, pst, ost, pb):
            def load_p(i):
                return pltpu.make_async_copy(ho.at[2 * dest(i) + other], lhs.at[i % 2, pl.ds(0, rows)],
                                             d_sem.at[i % 2, 0])

            def load_o(i):
                return pltpu.make_async_copy(ho.at[2 * dest(i - 1) + core], lhs.at[i % 2, pl.ds(rows, rows)],
                                             d_sem.at[i % 2, 1])

            def swap(p):
                return remote(pst.at[p % 2], pbuf.at[s, p // NJ, p % NJ], p_s.at[p % 2], p_r.at[s, p], partner)

            def pb_load(m):
                return pltpu.make_async_copy(pbuf.at[s, m // NJ, m % NJ], pb.at[m % 2], pb_sem.at[m % 2])

            def pb_start(m):
                swap(m).wait_recv()
                pb_load(m).start()

            def ostore(m):
                return pltpu.make_async_copy(ost.at[m % 2], pout.at[s, m // NJ, :, cols(m % NJ)], os_sem.at[m % 2])

            def ostored(m):
                pltpu.make_async_copy(ost.at[m % 2], pout.at[s, 0, :, cols(m % NJ)], os_sem.at[m % 2]).wait()

            def post(m):
                ostored(m)
                ii, j = m // NJ, m % NJ

                @pl.when(jnp.logical_and(ii == 0, j < NJ // 2))
                def _():
                    transit(s, j, right).start()

                @pl.when(jnp.logical_and(ii == 0, j >= NJ // 2))
                def _():
                    transit(s, j, left).start()

                @pl.when(jnp.logical_and(ii == 1, j >= NJ // 2))
                def _():
                    to_right(s, 1, j).start()

                @pl.when(jnp.logical_and(ii == 2, j < NJ // 2))
                def _():
                    to_left(s, 2, j).start()

            load_p(0).start()

            @pl.when(s == 0)
            def _():
                w_copies[2].wait()
                w_copies[3].wait()
            load_p(0).wait()
            load_p(1).start()
            load_o(1).start()

            @pl.loop(0, NJ)
            def _(j):
                @pl.when(j >= 2)
                def _():
                    swap(j - 2).wait_send()

                @pl.when(j == NJ - 1)
                def _():
                    pb_start(0)
                r = jnp.dot(lhs[0, 0:rows], wdo[:, cols(j)], preferred_element_type=f32)
                pst[j % 2] = r.astype(bf16)
                swap(j).start()

            @pl.when(s < batch - 1)
            def _():
                forward(s + 1, (2, 3))

            @pl.loop(0, 3 * NJ)
            def _(m):
                p = m + NJ
                i, j = p // NJ, p % NJ

                @pl.when(j == 0)
                def _():
                    load_p(i).wait()
                    load_o(i).wait()
                    load_o(i + 1).start()

                @pl.when(jnp.logical_and(j == 0, i < 3))
                def _():
                    load_p(i + 1).start()
                swap(p - 2).wait_send()
                pb_load(m).wait()
                pb_start(m + 1)
                r = jnp.dot(lhs[i % 2], wdo[:, cols(j)], preferred_element_type=f32)
                pst[m % 2] = r[:rows].astype(bf16)
                ost[m % 2] = (r[rows:] + pb[m % 2].astype(f32)).astype(bf16)
                swap(p).start()
                ostore(m).start()

                @pl.when(m >= 1)
                def _():
                    post(m - 1)

            @pl.when(s < batch - 1)
            def _():
                forward(s + 1, (4, 5))
            load_o(4).wait()

            @pl.loop(3 * NJ, 4 * NJ)
            def _(m):
                j = m % NJ
                pb_load(m).wait()

                @pl.when(j < NJ - 1)
                def _():
                    pb_start(m + 1)
                r = jnp.dot(lhs[0, rows:], wdo[:, cols(j)], preferred_element_type=f32)
                ost[m % 2] = (r + pb[m % 2].astype(f32)).astype(bf16)
                post(m - 1)
                pltpu.make_async_copy(ost.at[m % 2], own_out.at[s, :, cols(j)], os_sem.at[m % 2]).start()
            ostored(4 * NJ - 1)
            for p in (4 * NJ - 2, 4 * NJ - 1):
                swap(p).wait_send()
        pl.run_scoped(scope, pltpu.VMEM((2, 2 * rows, ff + attn), bf16), pltpu.VMEM((2, rows, ncol), bf16),
                      pltpu.VMEM((2, rows, ncol), bf16), pltpu.VMEM((2, rows, ncol), bf16))

    for cp in v_copies:
        cp.wait()
    pl.run_scoped(functools.partial(ag_send, 0), pltpu.VMEM((rows, dim), bf16))
    for cp in w_copies:
        cp.start()

    @pl.loop(0, batch)
    def _(s):
        def scope(qkv):
            phase_a(s, qkv)

            @pl.when(s > 0)
            def _():
                relay(s - 1)
            phase_b(qkv)
        pl.run_scoped(scope, pltpu.VMEM((seq, qkv_cols), bf16))
        phase_d(s)

        @pl.when(s < batch - 2)
        def _():
            pl.run_scoped(functools.partial(ag_send, s + 2), pltpu.VMEM((rows, dim), bf16))

    relay(batch - 1)

    @pl.loop(0, batch)
    def _(s):
        for j in range(NJ):
            to_right(s, 1, j).wait_recv()
            to_left(s, 2, j).wait_recv()
            to_right(s, 1, j).wait_send()
            to_left(s, 2, j).wait_send()
            transit(s, j, right).wait_send()
        for u in range(2 * n_chips):
            d, hf = unit(u)
            d2d_copy(s, u, d, hf, core).wait_send()
            if u >= 2:
                ici_copy(s, u, d, hf, right).wait_send()


def layer_call(x_blk, ln_gain, ln_bias, wqkv, w_out, w_up, w_down, n_tp):
    batch, rows, dim = x_blk.shape
    ff, attn, qkv_cols = w_up.shape[1], w_out.shape[0], wqkv.shape[1]
    n_chips = n_tp // 2
    ncol = dim // NJ
    bf16 = jnp.bfloat16
    dma = pltpu.SemaphoreType.DMA
    flops = 2 * batch * n_tp * rows * dim * (qkv_cols + 2 * ff + attn)
    outs = pl.pallas_call(
        layer_kernel,
        name="parallel_layer",
        out_shape=[
            jax.ShapeDtypeStruct((batch, rows, dim), bf16),
            jax.ShapeDtypeStruct((batch, rows, dim), bf16),
            jax.ShapeDtypeStruct((batch, rows, dim), bf16),
            jax.ShapeDtypeStruct((batch, n_chips, 2, rows, dim), bf16),
            jax.ShapeDtypeStruct((n_tp, rows, ff + attn), bf16),
            jax.ShapeDtypeStruct((batch, 4, NJ, rows, ncol), bf16),
            jax.ShapeDtypeStruct((batch, 3, rows, dim), bf16),
            jax.ShapeDtypeStruct((batch, rows, dim), bf16),
        ],
        in_specs=[pl.BlockSpec(memory_space=pl.ANY)] * 7,
        out_specs=[pl.BlockSpec(memory_space=pl.ANY)] * 8,
        scratch_shapes=[
            pltpu.VMEM((dim, qkv_cols), bf16), pltpu.VMEM((dim, ff), bf16), pltpu.VMEM((ff + attn, dim), bf16),
            pltpu.VMEM((1, dim), jnp.float32), pltpu.VMEM((1, dim), jnp.float32),
            dma((batch, 8)), dma((batch, 8)), dma((batch, 8)), dma((batch, 8)),
            dma((2,)), dma((batch, 4 * NJ)), dma((batch, NJ)), dma((batch, NJ)),
            dma((batch, 2 * NJ)), dma((batch, 2 * NJ)),
            dma((4,)), dma((2,)), dma((2, 4)), dma((2,)), dma((2, 2)), dma((n_tp,)), dma((2, 2)), dma((2,)), dma((2,)),
            dma((3, 2)),
        ],
        compiler_params=pltpu.CompilerParams(
            collective_id=0, has_side_effects=True, vmem_limit_bytes=67043328),
        cost_estimate=pl.CostEstimate(flops=flops, bytes_accessed=256 << 20, transcendentals=0),
    )(x_blk, ln_gain.reshape(1, dim), ln_bias.reshape(1, dim), wqkv, w_out, w_up, w_down)
    return outs[:3]


def solution(mesh):
    n_tp = mesh.shape["tp"]

    def local_layer(x_blk, ln_gain, ln_bias, w_qkv, w_out, w_up, w_down):
        dim = x_blk.shape[2]
        wqkv = w_qkv.transpose(0, 2, 1, 3).reshape(dim, -1)
        own, from_left, from_right = layer_call(x_blk, ln_gain, ln_bias, wqkv, w_out, w_up, w_down, n_tp)
        branch = (own.astype(jnp.float32) + from_left.astype(jnp.float32)
                  + from_right.astype(jnp.float32)).astype(jnp.bfloat16)
        return (x_blk.astype(jnp.float32) + branch.astype(jnp.float32)).astype(jnp.bfloat16)

    return jax.shard_map(
        local_layer, mesh=mesh,
        in_specs=(P("dp", "tp", None), P(), P(), P(None, "tp", None, None),
                  P("tp", None), P(None, "tp"), P("tp", None)),
        out_specs=P("dp", "tp", None), check_vma=False)
```

```python
import functools

import jax
import jax.numpy as jnp
from jax import lax
from jax.experimental import pallas as pl
from jax.experimental.pallas import tpu as pltpu
from jax.sharding import PartitionSpec as P

LN_EPS = 1e-5
NJ = 4


def layer_kernel(x_ref, gain_ref, bias_ref, wqkv_hbm, wout_hbm, wup_hbm, wdown_hbm,
                 own_out, left_out, right_out, n_all, ho, pbuf, pout, tin,
                 wqkv, wup, wdo, gain, bias,
                 ag_is, ag_ir, ag_ds, ag_dr, p_s, p_r, t_s, t_r, m_s, m_r,
                 w_sem, v_sem, ln_sem, a_sem, h_sem, o_sem, d_sem, pb_sem, os_sem, f_sem):
    batch, rows, dim = x_ref.shape
    half = rows // 2
    ff = wup.shape[1]
    attn = wdo.shape[0] - ff
    qkv_cols = wqkv.shape[1]
    n_heads = 2
    head = attn // n_heads
    n_chips = n_all.shape[1]
    seq = n_chips * 2 * rows
    ncol = dim // NJ
    f32, bf16 = jnp.float32, jnp.bfloat16

    me = lax.axis_index("tp")
    chip, core = me // 2, me % 2
    other = 1 - core
    partner = chip * 2 + other
    right = ((chip + 1) % n_chips) * 2 + core
    left = ((chip + n_chips - 1) % n_chips) * 2 + core

    def remote(src, dst, send, recv, dev):
        return pltpu.make_async_remote_copy(
            src_ref=src, dst_ref=dst, send_sem=send, recv_sem=recv,
            device_id={"tp": dev}, device_id_type=pl.DeviceIdType.MESH)

    barrier = pltpu.get_barrier_semaphore()
    for dev in (partner, right, left):
        pl.semaphore_signal(barrier, inc=1, device_id={"tp": dev}, device_id_type=pl.DeviceIdType.MESH)
    pl.semaphore_wait(barrier, 3)

    w_copies = (
        pltpu.make_async_copy(wup_hbm, wup, w_sem.at[2]),
        pltpu.make_async_copy(wdown_hbm, wdo.at[pl.ds(0, ff)], w_sem.at[3]),
        pltpu.make_async_copy(wout_hbm, wdo.at[pl.ds(ff, attn)], w_sem.at[4]),
    )
    v_copies = (pltpu.make_async_copy(gain_ref, gain, v_sem.at[0]),
                pltpu.make_async_copy(bias_ref, bias, v_sem.at[1]))
    for cp in v_copies:
        cp.start()

    def unit(u):
        g, b = u // 2, u % 2
        near = (g * (3 - g)) // 2
        off = near * (2 * b - 1) + 2 * (g // 3)
        hf = (b + near * (g - 1)) % 2
        return (chip + off + n_chips) % n_chips, hf

    def piece(s, d, hf, k):
        return n_all.at[s, d, hf, pl.ds(pl.multiple_of(k * half, half), half)]

    def ici_copy(s, u, d, hf, dev):
        return remote(piece(s, d, hf, core), piece(s, d, hf, core), ag_is.at[s, u], ag_ir.at[s, u], dev)

    def d2d_copy(s, u, d, hf, k):
        return remote(piece(s, d, hf, k), piece(s, d, hf, k), ag_ds.at[s, u], ag_dr.at[s, u], partner)

    def ag_send(s, buf):
        part, step = rows // 4, 32

        def load(q):
            at = pl.ds(q * part, part)
            return pltpu.make_async_copy(x_ref.at[s, at], buf.at[at], ln_sem.at[0, q])

        def store(q):
            dst = n_all.at[s, chip, q // 2, pl.ds(pl.multiple_of(core * half + (q % 2) * part, part), part)]
            return pltpu.make_async_copy(buf.at[pl.ds(q * part, part)], dst, ln_sem.at[1, q])

        for q in range(4):
            load(q).start()
        for q in range(4):
            load(q).wait()

            @pl.loop(0, part // step)
            def _(r):
                at = pl.ds(pl.multiple_of(q * part + r * step, step), step)
                v = buf[at, :].astype(f32)
                mean = jnp.mean(v, axis=-1, keepdims=True)
                cen = v - mean
                var = jnp.mean(cen * cen, axis=-1, keepdims=True)
                buf[at, :] = (cen * lax.rsqrt(var + LN_EPS) * gain[...] + bias[...]).astype(bf16)
            store(q).start()
            if q == 1:
                store(0).wait()
                store(1).wait()
                ici_copy(s, 2, chip, 0, right).start()
                d2d_copy(s, 0, chip, 0, core).start()
        store(2).wait()
        store(3).wait()
        ici_copy(s, 3, chip, 1, left).start()
        d2d_copy(s, 1, chip, 1, core).start()
        ici_copy(s, 4, chip, 1, right).start()
        ici_copy(s, 5, chip, 0, left).start()

    def forward(s, us):
        for u in us:
            d, hf = unit(u)
            with jax.named_scope(f"ici_wait_{u}"):
                ici_copy(s, u, d, hf, right).wait_recv()
            if u == 2:
                ici_copy(s, 6, d, hf, right).start()
            if u == 3:
                ici_copy(s, 7, d, hf, left).start()
            d2d_copy(s, u, d, hf, core).start()

    def dest(i):
        is2 = (i * (i - 1) * (3 - i) * (4 - i)) // 4
        is3 = (i * (i - 1) * (i - 2) * (4 - i)) // 6
        return (chip + 2 - i + 3 * is2 + is3 + n_chips) % n_chips

    def cols(j):
        return pl.ds(pl.multiple_of(j * ncol, ncol), ncol)

    def to_right(s, ii, j):
        return remote(pout.at[s, ii, :, cols(j)], left_out.at[s, :, cols(j)], m_s.at[s, j], m_r.at[s, j], right)

    def to_left(s, ii, j):
        return remote(pout.at[s, ii, :, cols(j)], right_out.at[s, :, cols(j)], m_s.at[s, NJ + j], m_r.at[s, NJ + j],
                      left)

    def transit(s, j, dev):
        return remote(pout.at[s, 0, :, cols(j)], tin.at[s, :, cols(j)], t_s.at[s, j], t_r.at[s, j], dev)

    def relay(s):
        def scope(a, b):
            def loads(j):
                return (pltpu.make_async_copy(pout.at[s, 1 + j // 2, :, cols(j)], a.at[j % 2], f_sem.at[0, j % 2]),
                        pltpu.make_async_copy(tin.at[s, :, cols(j)], b.at[j % 2], f_sem.at[1, j % 2]))

            def store(j):
                return pltpu.make_async_copy(a.at[j % 2], pout.at[s, 1 + j // 2, :, cols(j)], f_sem.at[2, j % 2])

            def send(j):
                return to_right(s, 1, j) if j < NJ // 2 else to_left(s, 2, j)

            order = tuple(range(NJ))
            for n, j in enumerate(order):
                if n == 0:
                    with jax.named_scope("relay_wait"):
                        transit(s, j, right).wait_recv()
                    for cp in loads(j):
                        cp.start()
                if n >= 1:
                    store(order[n - 1]).wait()
                    send(order[n - 1]).start()
                if n + 1 < NJ:
                    with jax.named_scope("relay_wait"):
                        transit(s, order[n + 1], right).wait_recv()
                    for cp in loads(order[n + 1]):
                        cp.start()
                for cp in loads(j):
                    cp.wait()
                step = 64

                @pl.loop(0, rows // step)
                def _(r):
                    at = pl.ds(pl.multiple_of(r * step, step), step)
                    a[j % 2, at, :] = (a[j % 2, at, :].astype(f32) + b[j % 2, at, :].astype(f32)).astype(bf16)
                store(j).start()
            store(order[-1]).wait()
            send(order[-1]).start()
        pl.run_scoped(scope, pltpu.VMEM((2, rows, ncol), bf16), pltpu.VMEM((2, rows, ncol), bf16))

    def phase_a(s, qkv):
        def scope(nbuf, hbuf):
            def load(u):
                d, hf = unit(u)
                return pltpu.make_async_copy(n_all.at[s, d, hf], nbuf.at[u % 2], a_sem.at[u % 2])

            def arrived(u):
                d, hf = unit(u)
                with jax.named_scope("d2d_wait"):
                    d2d_copy(s, u, d, hf, other).wait_recv()

            def hstore(u, k):
                d, hf = unit(u)
                return pltpu.make_async_copy(
                    hbuf.at[u % 2, pl.ds(k * half, half)],
                    ho.at[2 * d + k, pl.ds(pl.multiple_of(hf * half, half), half), pl.ds(0, ff)],
                    h_sem.at[u % 2, k])

            arrived(0)
            load(0).start()

            @pl.loop(0, 2 * n_chips)
            def _(u):
                with jax.named_scope("load_wait"):
                    load(u).wait()

                @pl.when(jnp.logical_and(s > 0, u == 3))
                def _():
                    forward(s, (6, 7))

                @pl.when(jnp.logical_and(s > 0, u < 7))
                def _():
                    arrived(u + 1)
                    load(u + 1).start()

                @pl.when(u >= 2)
                def _():
                    for k in range(2):
                        hstore(u - 2, k).wait()

                @pl.when(jnp.logical_and(s == 0, u == 0))
                def _():
                    w_copies[0].wait()

                d, hf = unit(u)
                slot = u % 2
                r = jnp.dot(nbuf[slot], wqkv[...], preferred_element_type=f32).astype(bf16)
                for k in range(2):
                    pos = pl.multiple_of(d * (2 * rows) + k * rows + hf * half, half)
                    qkv[pl.ds(pos, half), :] = r[k * half:(k + 1) * half]
                h = jnp.dot(nbuf[slot], wup[...], preferred_element_type=f32)
                hbuf[slot] = (0.5 * h * (1.0 + lax.erf(h * (2.0 ** -0.5)))).astype(bf16)
                for k in range(2):
                    hstore(u, k).start()

                @pl.when(s == 0)
                def _():
                    @pl.when(u == 1)
                    def _():
                        forward(0, (2, 3))
                        ag_send(1, nbuf.at[0])

                    @pl.when(u == 3)
                    def _():
                        forward(0, (4, 5))

                    @pl.when(u == 5)
                    def _():
                        forward(0, (6, 7))

                    @pl.when(u < 7)
                    def _():
                        arrived(u + 1)
                        load(u + 1).start()

            for u in (6, 7):
                for k in range(2):
                    hstore(u, k).wait()
        pl.run_scoped(scope, pltpu.VMEM((2, rows, dim), bf16), pltpu.VMEM((2, rows, ff), bf16))

    def phase_b(qkv):
        def ostore(t):
            return pltpu.make_async_copy(qkv.at[pl.ds(t * rows, rows), pl.ds(0, attn)],
                                         ho.at[t, :, pl.ds(ff, attn)], o_sem.at[t])
        scale = head ** -0.5

        def scope(scores, probs):
            keep = (lax.broadcasted_iota(jnp.int32, (rows, rows), 0)
                    >= lax.broadcasted_iota(jnp.int32, (rows, rows), 1))
            for t in range(seq // rows):
                r0, n = t * rows, (t + 1) * rows
                tops = []
                for h in range(n_heads):
                    q = qkv[r0:r0 + rows, h * head:(h + 1) * head]
                    k = qkv[0:n, attn + h * head:attn + (h + 1) * head]
                    sc = lax.dot_general(q, k, (((1,), (1,)), ((), ())), preferred_element_type=f32)
                    diag = jnp.where(keep, sc[:, n - rows:], -jnp.inf)
                    top = jnp.max(diag, axis=1, keepdims=True)
                    if t:
                        scores[h, :, 0:n - rows] = sc[:, :n - rows]
                        top = jnp.maximum(top, jnp.max(sc[:, :n - rows], axis=1, keepdims=True))
                    scores[h, :, n - rows:n] = diag
                    tops.append(top)
                for h in range(n_heads):
                    v = qkv[0:n, 2 * attn + h * head:2 * attn + (h + 1) * head]
                    total = jnp.zeros((rows, 1), f32)
                    for c in range(0, n, rows):
                        e = jnp.exp((scores[h, :, c:c + rows] - tops[h]) * scale)
                        scores[h, :, c:c + rows] = e
                        total = total + jnp.sum(e, axis=1, keepdims=True)
                    inverse = 1.0 / total
                    for c in range(0, n, rows):
                        probs[h, :, c:c + rows] = (scores[h, :, c:c + rows] * inverse).astype(bf16)
                    o = jnp.dot(probs[h, :, 0:n], v, preferred_element_type=f32)
                    qkv[r0:r0 + rows, h * head:(h + 1) * head] = o.astype(bf16)
                if t % 4 == 3:
                    for done in range(t - 3, t + 1):
                        ostore(done).start()
            for t in range(seq // rows):
                ostore(t).wait()
        pl.run_scoped(scope, pltpu.VMEM((n_heads, rows, seq), f32), pltpu.VMEM((n_heads, rows, seq), bf16))

    def phase_d(s):
        def scope(lhs, pst, ost, pb):
            def load_p(i):
                return pltpu.make_async_copy(ho.at[2 * dest(i) + other], lhs.at[i % 2, pl.ds(0, rows)],
                                             d_sem.at[i % 2, 0])

            def load_o(i):
                return pltpu.make_async_copy(ho.at[2 * dest(i - 1) + core], lhs.at[i % 2, pl.ds(rows, rows)],
                                             d_sem.at[i % 2, 1])

            def swap(p):
                return remote(pst.at[p % 2], pbuf.at[s, p // NJ, p % NJ], p_s.at[p % 2], p_r.at[s, p], partner)

            def pb_load(m):
                return pltpu.make_async_copy(pbuf.at[s, m // NJ, m % NJ], pb.at[m % 2], pb_sem.at[m % 2])

            def pb_start(m):
                with jax.named_scope("swap_wait"):
                    swap(m).wait_recv()
                pb_load(m).start()

            def ostore(m):
                return pltpu.make_async_copy(ost.at[m % 2], pout.at[s, m // NJ, :, cols(m % NJ)], os_sem.at[m % 2])

            def ostored(m):
                pltpu.make_async_copy(ost.at[m % 2], pout.at[s, 0, :, cols(m % NJ)], os_sem.at[m % 2]).wait()

            def post(m):
                ostored(m)
                ii, j = m // NJ, m % NJ

                @pl.when(jnp.logical_and(ii == 0, j < NJ // 2))
                def _():
                    transit(s, j, right).start()

                @pl.when(jnp.logical_and(ii == 0, j >= NJ // 2))
                def _():
                    transit(s, j, left).start()

                @pl.when(jnp.logical_and(ii == 1, j >= NJ // 2))
                def _():
                    to_right(s, 1, j).start()

                @pl.when(jnp.logical_and(ii == 2, j < NJ // 2))
                def _():
                    to_left(s, 2, j).start()

            load_p(0).start()

            @pl.when(s == 0)
            def _():
                w_copies[1].wait()
                w_copies[2].wait()
            load_p(0).wait()
            load_p(1).start()
            load_o(1).start()

            @pl.loop(0, NJ)
            def _(j):
                @pl.when(j >= 2)
                def _():
                    swap(j - 2).wait_send()

                @pl.when(j == NJ - 1)
                def _():
                    pb_start(0)
                r = jnp.dot(lhs[0, 0:rows], wdo[:, cols(j)], preferred_element_type=f32)
                pst[j % 2] = r.astype(bf16)
                swap(j).start()

            @pl.when(s < batch - 1)
            def _():
                forward(s + 1, (2, 3))

            @pl.loop(0, 3 * NJ)
            def _(m):
                p = m + NJ
                i, j = p // NJ, p % NJ

                @pl.when(j == 0)
                def _():
                    load_p(i).wait()
                    load_o(i).wait()
                    load_o(i + 1).start()

                @pl.when(jnp.logical_and(j == 0, i < 3))
                def _():
                    load_p(i + 1).start()
                swap(p - 2).wait_send()
                pb_load(m).wait()
                pb_start(m + 1)
                r = jnp.dot(lhs[i % 2], wdo[:, cols(j)], preferred_element_type=f32)
                pst[m % 2] = r[:rows].astype(bf16)
                ost[m % 2] = (r[rows:] + pb[m % 2].astype(f32)).astype(bf16)
                swap(p).start()
                ostore(m).start()

                @pl.when(m >= 1)
                def _():
                    post(m - 1)

            @pl.when(s < batch - 1)
            def _():
                forward(s + 1, (4, 5))
            load_o(4).wait()

            @pl.loop(3 * NJ, 4 * NJ)
            def _(m):
                j = m % NJ
                pb_load(m).wait()

                @pl.when(j < NJ - 1)
                def _():
                    pb_start(m + 1)
                r = jnp.dot(lhs[0, rows:], wdo[:, cols(j)], preferred_element_type=f32)
                ost[m % 2] = (r + pb[m % 2].astype(f32)).astype(bf16)
                post(m - 1)
                pltpu.make_async_copy(ost.at[m % 2], own_out.at[s, :, cols(j)], os_sem.at[m % 2]).start()
            ostored(4 * NJ - 1)
            for p in (4 * NJ - 2, 4 * NJ - 1):
                swap(p).wait_send()
        pl.run_scoped(scope, pltpu.VMEM((2, 2 * rows, ff + attn), bf16), pltpu.VMEM((2, rows, ncol), bf16),
                      pltpu.VMEM((2, rows, ncol), bf16), pltpu.VMEM((2, rows, ncol), bf16))

    def place_qkv(raw, wide):
        kinds = qkv_cols // attn
        per = qkv_cols // 128
        chunk = raw.shape[1] // per
        n_chunks = dim // chunk

        def load(q):
            at = pl.ds(pl.multiple_of(q * (chunk * per), chunk * per), chunk * per)
            return pltpu.make_async_copy(wqkv_hbm.at[at], raw.at[q % 2], w_sem.at[q % 2])

        load(0).start()

        @pl.loop(0, n_chunks)
        def _(q):
            @pl.when(q + 1 < n_chunks)
            def _():
                load(q + 1).start()
            load(q).wait()
            wide[...] = raw[q % 2].astype(f32)
            for j in range(kinds):
                for c in range(head // 128):
                    for g in range(n_heads):
                        row = (j * (head // 128) + c) * n_heads + g
                        col = j * attn + g * head + c * 128
                        wqkv[pl.ds(pl.multiple_of(q * chunk, chunk), chunk), col:col + 128] = (
                            wide[pl.ds(row, chunk, stride=per), :].astype(bf16))

    for cp in v_copies:
        cp.wait()
    with jax.named_scope("send0"):
        pl.run_scoped(functools.partial(ag_send, 0), pltpu.VMEM((rows, dim), bf16))
    for cp in w_copies:
        cp.start()
    with jax.named_scope("place"):
        pl.run_scoped(place_qkv, pltpu.VMEM((2, 128 * (qkv_cols // 128), 128), bf16),
                      pltpu.VMEM((128 * (qkv_cols // 128), 128), f32))

    @pl.loop(0, batch)
    def _(s):
        def scope(qkv):
            with jax.named_scope("A"):
                phase_a(s, qkv)

            @pl.when(s > 0)
            def _():
                with jax.named_scope("relay"):
                    relay(s - 1)
            with jax.named_scope("B"):
                phase_b(qkv)
        pl.run_scoped(scope, pltpu.VMEM((seq, qkv_cols), bf16))
        with jax.named_scope("D"):
            phase_d(s)

        @pl.when(s < batch - 2)
        def _():
            pl.run_scoped(functools.partial(ag_send, s + 2), pltpu.VMEM((rows, dim), bf16))

    with jax.named_scope("relay_last"):
        relay(batch - 1)

    @pl.loop(0, batch)
    def _(s):
        with jax.named_scope("final"):
            for j in range(NJ):
                to_right(s, 1, j).wait_recv()
                to_left(s, 2, j).wait_recv()
                to_right(s, 1, j).wait_send()
                to_left(s, 2, j).wait_send()
                transit(s, j, right).wait_send()
            for u in range(2 * n_chips):
                d, hf = unit(u)
                d2d_copy(s, u, d, hf, core).wait_send()
                if u >= 2:
                    ici_copy(s, u, d, hf, right).wait_send()


def layer_call(x_blk, ln_gain, ln_bias, wqkv, w_out, w_up, w_down, n_tp):
    batch, rows, dim = x_blk.shape
    ff, attn, qkv_cols = w_up.shape[1], w_out.shape[0], wqkv.shape[0] * 128 // dim
    n_chips = n_tp // 2
    ncol = dim // NJ
    bf16 = jnp.bfloat16
    dma = pltpu.SemaphoreType.DMA
    flops = 2 * batch * n_tp * rows * dim * (qkv_cols + 2 * ff + attn)
    outs = pl.pallas_call(
        layer_kernel,
        name="parallel_layer",
        out_shape=[
            jax.ShapeDtypeStruct((batch, rows, dim), bf16),
            jax.ShapeDtypeStruct((batch, rows, dim), bf16),
            jax.ShapeDtypeStruct((batch, rows, dim), bf16),
            jax.ShapeDtypeStruct((batch, n_chips, 2, rows, dim), bf16),
            jax.ShapeDtypeStruct((n_tp, rows, ff + attn), bf16),
            jax.ShapeDtypeStruct((batch, 4, NJ, rows, ncol), bf16),
            jax.ShapeDtypeStruct((batch, 3, rows, dim), bf16),
            jax.ShapeDtypeStruct((batch, rows, dim), bf16),
        ],
        in_specs=[pl.BlockSpec(memory_space=pl.ANY)] * 7,
        out_specs=[pl.BlockSpec(memory_space=pl.ANY)] * 8,
        scratch_shapes=[
            pltpu.VMEM((dim, qkv_cols), bf16), pltpu.VMEM((dim, ff), bf16), pltpu.VMEM((ff + attn, dim), bf16),
            pltpu.VMEM((1, dim), jnp.float32), pltpu.VMEM((1, dim), jnp.float32),
            dma((batch, 8)), dma((batch, 8)), dma((batch, 8)), dma((batch, 8)),
            dma((2,)), dma((batch, 4 * NJ)), dma((batch, NJ)), dma((batch, NJ)),
            dma((batch, 2 * NJ)), dma((batch, 2 * NJ)),
            dma((5,)), dma((2,)), dma((2, 4)), dma((2,)), dma((2, 2)), dma((n_tp,)), dma((2, 2)), dma((2,)), dma((2,)),
            dma((3, 2)),
        ],
        compiler_params=pltpu.CompilerParams(
            collective_id=0, has_side_effects=True, vmem_limit_bytes=67043328),
        cost_estimate=pl.CostEstimate(flops=flops, bytes_accessed=256 << 20, transcendentals=0),
    )(x_blk, ln_gain.reshape(1, dim), ln_bias.reshape(1, dim), wqkv, w_out, w_up, w_down)
    return outs[:3]


def solution(mesh):
    n_tp = mesh.shape["tp"]

    def local_layer(x_blk, ln_gain, ln_bias, w_qkv, w_out, w_up, w_down):
        dim = x_blk.shape[2]
        groups, kinds, head = w_qkv.shape[1:]
        wqkv = w_qkv.reshape(dim, groups, kinds, head // 128, 128).transpose(0, 2, 3, 1, 4).reshape(-1, 128)
        own, from_left, from_right = layer_call(x_blk, ln_gain, ln_bias, wqkv, w_out, w_up, w_down, n_tp)
        branch = (own.astype(jnp.float32) + from_left.astype(jnp.float32)
                  + from_right.astype(jnp.float32)).astype(jnp.bfloat16)
        return (x_blk.astype(jnp.float32) + branch.astype(jnp.float32)).astype(jnp.bfloat16)

    return jax.shard_map(
        local_layer, mesh=mesh,
        in_specs=(P("dp", "tp", None), P(), P(), P(None, "tp", None, None),
                  P("tp", None), P(None, "tp"), P("tp", None)),
        out_specs=P("dp", "tp", None), check_vma=False)
```

```python
import jax
import jax.numpy as jnp
from jax import lax
from jax.experimental import pallas as pl
from jax.experimental.pallas import tpu as pltpu
from jax.sharding import PartitionSpec as P

LN_EPS = 1e-5
LOG2_E = 1.4426950408889634
NJ = 4


def layer_kernel(x_ref, gain_ref, bias_ref, wqkv_hbm, wout_hbm, wup_hbm, wdown_hbm,
                 own_out, left_out, right_out, n_all, ho, pbuf, pout, tin,
                 wqkv, wup, wdo, gain, bias,
                 ag_is, ag_ir, ag_ds, ag_dr, p_s, p_r, t_s, t_r, m_s, m_r,
                 w_sem, v_sem, ln_sem, a_sem, h_sem, o_sem, d_sem, pb_sem, os_sem, f_sem):
    batch, rows, dim = x_ref.shape
    half = rows // 2
    ff = wup.shape[1]
    attn = wdo.shape[0] - ff
    qkv_cols = wqkv.shape[1]
    n_heads = 2
    head = attn // n_heads
    n_chips = n_all.shape[1]
    seq = n_chips * 2 * rows
    ncol = dim // NJ
    f32, bf16 = jnp.float32, jnp.bfloat16

    me = lax.axis_index("tp")
    chip, core = me // 2, me % 2
    other = 1 - core
    partner = chip * 2 + other
    right = ((chip + 1) % n_chips) * 2 + core
    left = ((chip + n_chips - 1) % n_chips) * 2 + core

    def remote(src, dst, send, recv, dev):
        return pltpu.make_async_remote_copy(
            src_ref=src, dst_ref=dst, send_sem=send, recv_sem=recv,
            device_id={"tp": dev}, device_id_type=pl.DeviceIdType.MESH)

    barrier = pltpu.get_barrier_semaphore()
    for dev in (partner, right, left):
        pl.semaphore_signal(barrier, inc=1, device_id={"tp": dev}, device_id_type=pl.DeviceIdType.MESH)
    pl.semaphore_wait(barrier, 3)

    w_copies = (
        pltpu.make_async_copy(wup_hbm, wup, w_sem.at[0]),
        pltpu.make_async_copy(wdown_hbm, wdo.at[pl.ds(0, ff)], w_sem.at[1]),
        pltpu.make_async_copy(wout_hbm, wdo.at[pl.ds(ff, attn)], w_sem.at[2]),
    )
    v_copies = (pltpu.make_async_copy(gain_ref, gain, v_sem.at[0]),
                pltpu.make_async_copy(bias_ref, bias, v_sem.at[1]))
    for cp in v_copies:
        cp.start()

    def unit(u):
        g, b = u // 2, u % 2
        near = (g * (3 - g)) // 2
        off = near * (2 * b - 1) + 2 * (g // 3)
        hf = (b + near * (g - 1)) % 2
        return (chip + off + n_chips) % n_chips, hf

    def piece(s, d, hf, k):
        return n_all.at[s, d, hf, pl.ds(pl.multiple_of(k * half, half), half)]

    def ici_copy(s, u, d, hf, dev):
        return remote(piece(s, d, hf, core), piece(s, d, hf, core), ag_is.at[s, u], ag_ir.at[s, u], dev)

    def d2d_copy(s, u, d, hf, k):
        return remote(piece(s, d, hf, k), piece(s, d, hf, k), ag_ds.at[s, u], ag_dr.at[s, u], partner)

    part = rows // 4

    def x_load(s, buf, q):
        at = pl.ds(q * part, part)
        return pltpu.make_async_copy(x_ref.at[s, at], buf.at[at], ln_sem.at[0, q])

    def n_store(s, buf, q):
        dst = n_all.at[s, chip, q // 2, pl.ds(pl.multiple_of(core * half + (q % 2) * part, part), part)]
        return pltpu.make_async_copy(buf.at[pl.ds(q * part, part)], dst, ln_sem.at[1, q])

    def x_start(s, buf):
        for q in range(4):
            x_load(s, buf, q).start()

    def normalise(s, buf, q):
        x_load(s, buf, q).wait()
        at = pl.ds(q * part, part)
        lanes, wide = 128, 512
        total = jnp.zeros((part, lanes), f32)
        for c in range(0, dim, wide):
            v = buf[at, c:c + wide].astype(f32)
            for k in range(0, wide, lanes):
                total = total + v[:, k:k + lanes]
        mean = jnp.sum(total, axis=-1, keepdims=True) * (1.0 / dim)
        total = jnp.zeros((part, lanes), f32)
        for c in range(0, dim, wide):
            cen = buf[at, c:c + wide].astype(f32) - mean
            for k in range(0, wide, lanes):
                total = total + cen[:, k:k + lanes] * cen[:, k:k + lanes]
        inv = lax.rsqrt(jnp.sum(total, axis=-1, keepdims=True) * (1.0 / dim) + LN_EPS)
        for c in range(0, dim, wide):
            cen = buf[at, c:c + wide].astype(f32) - mean
            buf[at, c:c + wide] = (cen * inv * gain[:, c:c + wide] + bias[:, c:c + wide]).astype(bf16)
        n_store(s, buf, q).start()

    def send_first(s, buf):
        n_store(s, buf, 0).wait()
        n_store(s, buf, 1).wait()
        ici_copy(s, 2, chip, 0, right).start()
        d2d_copy(s, 0, chip, 0, core).start()

    def send_rest(s, buf):
        n_store(s, buf, 2).wait()
        n_store(s, buf, 3).wait()
        ici_copy(s, 3, chip, 1, left).start()
        d2d_copy(s, 1, chip, 1, core).start()
        ici_copy(s, 4, chip, 1, right).start()
        ici_copy(s, 5, chip, 0, left).start()

    def forward(s, us):
        for u in us:
            d, hf = unit(u)
            with jax.named_scope(f"ici_wait_{u}"):
                ici_copy(s, u, d, hf, right).wait_recv()
            if u == 2:
                ici_copy(s, 6, d, hf, right).start()
            if u == 3:
                ici_copy(s, 7, d, hf, left).start()
            d2d_copy(s, u, d, hf, core).start()

    def dest(i):
        is2 = (i * (i - 1) * (3 - i) * (4 - i)) // 4
        is3 = (i * (i - 1) * (i - 2) * (4 - i)) // 6
        return (chip + 2 - i + 3 * is2 + is3 + n_chips) % n_chips

    def cols(j):
        return pl.ds(pl.multiple_of(j * ncol, ncol), ncol)

    def to_right(s, ii, j):
        return remote(pout.at[s, ii, :, cols(j)], left_out.at[s, :, cols(j)], m_s.at[s, j], m_r.at[s, j], right)

    def to_left(s, ii, j):
        return remote(pout.at[s, ii, :, cols(j)], right_out.at[s, :, cols(j)], m_s.at[s, NJ + j], m_r.at[s, NJ + j],
                      left)

    def transit(s, j, dev):
        return remote(pout.at[s, 0, :, cols(j)], tin.at[s, :, cols(j)], t_s.at[s, j], t_r.at[s, j], dev)

    def relay_loads(s, q, k, a, b):
        return (pltpu.make_async_copy(pout.at[s, 1 + q // 2, :, cols(q)], a, f_sem.at[0, k]),
                pltpu.make_async_copy(tin.at[s, :, cols(q)], b, f_sem.at[1, k]))

    def relay_store(s, q, k, a):
        return pltpu.make_async_copy(a, pout.at[s, 1 + q // 2, :, cols(q)], f_sem.at[2, k])

    def relay_start(s, q, k, a, b):
        transit(s, q, right).wait_recv()
        for cp in relay_loads(s, q, k, a, b):
            cp.start()

    def relay_add(s, q, k, a, b):
        for cp in relay_loads(s, q, k, a, b):
            cp.wait()
        step = 64

        @pl.loop(0, rows // step)
        def _(r):
            at = pl.ds(pl.multiple_of(r * step, step), step)
            a[at, :] = (a[at, :].astype(f32) + b[at, :].astype(f32)).astype(bf16)
        relay_store(s, q, k, a).start()

    def relay_send(s, q, k, a):
        relay_store(s, q, k, a).wait()

        @pl.when(q < NJ // 2)
        def _():
            to_right(s, 1, q).start()

        @pl.when(q >= NJ // 2)
        def _():
            to_left(s, 2, q).start()

    def relay_all(s):
        def scope(a, b):
            order = (0, 2, 1, 3)

            def bufs(n):
                return n % 2, a.at[n % 2], b.at[n % 2]
            relay_start(s, order[0], *bufs(0))
            for n in range(NJ):
                if n + 1 < NJ:
                    if n >= 1:
                        relay_send(s, order[n - 1], *bufs(n - 1)[:2])
                    relay_start(s, order[n + 1], *bufs(n + 1))
                relay_add(s, order[n], *bufs(n))
            for n in (NJ - 2, NJ - 1):
                relay_send(s, order[n], *bufs(n)[:2])
        pl.run_scoped(scope, pltpu.VMEM((2, rows, ncol), bf16), pltpu.VMEM((2, rows, ncol), bf16))

    def phase_a(s, qkv):
        def scope(nbuf, hbuf, ra, rb):
            def load(u):
                d, hf = unit(u)
                return pltpu.make_async_copy(n_all.at[s, d, hf], nbuf.at[u % 2], a_sem.at[u % 2])

            def arrived(u):
                d, hf = unit(u)
                with jax.named_scope("d2d_wait"):
                    d2d_copy(s, u, d, hf, other).wait_recv()

            def hstore(u, k):
                d, hf = unit(u)
                return pltpu.make_async_copy(
                    hbuf.at[pl.ds(k * half, half)],
                    ho.at[2 * d + k, pl.ds(pl.multiple_of(hf * half, half), half), pl.ds(0, ff)],
                    h_sem.at[k])

            arrived(0)
            load(0).start()

            @pl.loop(0, 2 * n_chips)
            def _(u):
                with jax.named_scope("load_wait"):
                    load(u).wait()

                @pl.when(jnp.logical_and(s > 0, u == 3))
                def _():
                    forward(s, (6, 7))

                @pl.when(jnp.logical_or(jnp.logical_and(s > 0, u < 7), u % 2 == 0))
                def _():
                    arrived(u + 1)
                    load(u + 1).start()

                @pl.when(jnp.logical_and(s == 0, u == 1))
                def _():
                    x_start(1, nbuf.at[0])

                @pl.when(jnp.logical_and(s > 0, jnp.logical_and(u >= 3, u % 2 == 1)))
                def _():
                    relay_send(s - 1, (u - 3) // 2, 0, ra)

                @pl.when(jnp.logical_and(s > 0, u % 2 == 1))
                def _():
                    relay_start(s - 1, (u - 1) // 2, 0, ra, rb)

                @pl.when(jnp.logical_and(s > 0, jnp.logical_and(u >= 2, u % 2 == 0)))
                def _():
                    relay_add(s - 1, (u - 2) // 2, 0, ra, rb)

                @pl.when(jnp.logical_and(s == 0, u == 0))
                def _():
                    w_copies[0].wait()

                d, hf = unit(u)
                slot = u % 2
                r = jnp.dot(nbuf[slot], wqkv[...], preferred_element_type=f32).astype(bf16)
                for k in range(2):
                    pos = pl.multiple_of(d * (2 * rows) + k * rows + hf * half, half)
                    qkv[pl.ds(pos, half), :] = r[k * half:(k + 1) * half]

                @pl.when(u >= 1)
                def _():
                    for k in range(2):
                        hstore(u - 1, k).wait()
                h = jnp.dot(nbuf[slot], wup[...], preferred_element_type=f32)
                hbuf[...] = (0.5 * h * (1.0 + lax.erf(h * (2.0 ** -0.5)))).astype(bf16)
                for k in range(2):
                    hstore(u, k).start()

                @pl.when(s == 0)
                def _():
                    @pl.when(u == 1)
                    def _():
                        forward(0, (2, 3))
                        with jax.named_scope("send1"):
                            for q in range(4):
                                normalise(1, nbuf.at[0], q)
                            send_first(1, nbuf.at[0])
                            send_rest(1, nbuf.at[0])

                    @pl.when(u == 3)
                    def _():
                        forward(0, (4, 5))

                    @pl.when(u == 5)
                    def _():
                        forward(0, (6, 7))

                    @pl.when(jnp.logical_and(u < 7, u % 2 == 1))
                    def _():
                        arrived(u + 1)
                        load(u + 1).start()

            @pl.when(s > 0)
            def _():
                with jax.named_scope("relay_end"):
                    relay_add(s - 1, NJ - 1, 0, ra, rb)
                    relay_send(s - 1, NJ - 1, 0, ra)
            for k in range(2):
                hstore(7, k).wait()
        pl.run_scoped(scope, pltpu.VMEM((2, rows, dim), bf16), pltpu.VMEM((rows, ff), bf16),
                      pltpu.VMEM((rows, ncol), bf16), pltpu.VMEM((rows, ncol), bf16))

    def phase_b(qkv):
        def ostore(t):
            return pltpu.make_async_copy(qkv.at[pl.ds(t * rows, rows), pl.ds(0, attn)],
                                         ho.at[t, :, pl.ds(ff, attn)], o_sem.at[t])
        scale = head ** -0.5

        def scope(scores, probs):
            keep = (lax.broadcasted_iota(jnp.int32, (rows, rows), 0)
                    >= lax.broadcasted_iota(jnp.int32, (rows, rows), 1))
            tasks = [(t, h) for t in range(seq // rows) for h in range(n_heads)]
            tops = {}

            def score(i):
                t, h = tasks[i]
                r0, n = t * rows, (t + 1) * rows
                q = qkv[r0:n, h * head:(h + 1) * head]
                k = qkv[0:n, attn + h * head:attn + (h + 1) * head]
                sc = lax.dot_general(q, k, (((1,), (1,)), ((), ())), preferred_element_type=f32)
                diag = jnp.where(keep, sc[:, r0:], -jnp.inf)
                top = jnp.max(diag, axis=1, keepdims=True)
                if t:
                    scores[i % 2, :, 0:r0] = sc[:, :r0]
                    top = jnp.maximum(top, jnp.max(sc[:, :r0], axis=1, keepdims=True))
                scores[i % 2, :, r0:n] = diag
                tops[i] = top

            def soften(i):
                t, h = tasks[i]
                n = (t + 1) * rows
                total = jnp.zeros((rows, rows // 2), f32)
                for c in range(0, n, rows):
                    e = jnp.exp2((scores[i % 2, :, c:c + rows] - tops[i]) * (scale * LOG2_E))
                    scores[i % 2, :, c:c + rows] = e
                    total = total + e[:, :rows // 2] + e[:, rows // 2:]
                inverse = 1.0 / jnp.sum(total, axis=1, keepdims=True)
                for c in range(0, n, rows):
                    probs[i % 2, :, c:c + rows] = (scores[i % 2, :, c:c + rows] * inverse).astype(bf16)

            def mix(i):
                t, h = tasks[i]
                r0, n = t * rows, (t + 1) * rows
                v = qkv[0:n, 2 * attn + h * head:2 * attn + (h + 1) * head]
                o = jnp.dot(probs[i % 2, :, 0:n], v, preferred_element_type=f32)
                qkv[r0:n, h * head:(h + 1) * head] = o.astype(bf16)

            score(0)
            for i in range(len(tasks)):
                if i + 1 < len(tasks):
                    score(i + 1)
                soften(i)
                mix(i)
                if i % n_heads == n_heads - 1 and tasks[i][0] % 4 == 3:
                    for done in range(tasks[i][0] - 3, tasks[i][0] + 1):
                        ostore(done).start()
            for t in range(seq // rows):
                ostore(t).wait()
        pl.run_scoped(scope, pltpu.VMEM((n_heads, rows, seq), f32), pltpu.VMEM((n_heads, rows, seq), bf16))

    def phase_d(s):
        def scope(lhs, pst, ost, pb, xbuf):
            def load_p(i):
                return pltpu.make_async_copy(ho.at[2 * dest(i) + other], lhs.at[i % 2, pl.ds(0, rows)],
                                             d_sem.at[i % 2, 0])

            def load_o(i):
                return pltpu.make_async_copy(ho.at[2 * dest(i - 1) + core], lhs.at[i % 2, pl.ds(rows, rows)],
                                             d_sem.at[i % 2, 1])

            def swap(p):
                return remote(pst.at[p % 2], pbuf.at[s, p // NJ, p % NJ], p_s.at[p % 2], p_r.at[s, p], partner)

            def pb_load(m):
                return pltpu.make_async_copy(pbuf.at[s, m // NJ, m % NJ], pb.at[m % 2], pb_sem.at[m % 2])

            def pb_start(m):
                with jax.named_scope("swap_wait"):
                    swap(m).wait_recv()
                pb_load(m).start()

            def ostore(m):
                return pltpu.make_async_copy(ost.at[m % 2], pout.at[s, m // NJ, :, cols(m % NJ)], os_sem.at[m % 2])

            def ostored(m):
                pltpu.make_async_copy(ost.at[m % 2], pout.at[s, 0, :, cols(m % NJ)], os_sem.at[m % 2]).wait()

            def post(m):
                ostored(m)
                ii, j = m // NJ, m % NJ

                @pl.when(jnp.logical_and(ii == 0, j < NJ // 2))
                def _():
                    transit(s, j, right).start()

                @pl.when(jnp.logical_and(ii == 0, j >= NJ // 2))
                def _():
                    transit(s, j, left).start()

                @pl.when(jnp.logical_and(ii == 1, j >= NJ // 2))
                def _():
                    to_right(s, 1, j).start()

                @pl.when(jnp.logical_and(ii == 2, j < NJ // 2))
                def _():
                    to_left(s, 2, j).start()

            load_p(0).start()

            @pl.when(s == 0)
            def _():
                w_copies[1].wait()
                w_copies[2].wait()
            load_p(0).wait()
            load_p(1).start()
            load_o(1).start()

            @pl.when(s < batch - 2)
            def _():
                x_start(s + 2, xbuf)

            @pl.loop(0, NJ)
            def _(j):
                @pl.when(j >= 2)
                def _():
                    swap(j - 2).wait_send()

                @pl.when(j == NJ - 1)
                def _():
                    pb_start(0)
                r = jnp.dot(lhs[0, 0:rows], wdo[:, cols(j)], preferred_element_type=f32)
                pst[j % 2] = r.astype(bf16)
                swap(j).start()

            @pl.when(s < batch - 1)
            def _():
                forward(s + 1, (2, 3))

            @pl.loop(0, 3 * NJ)
            def _(m):
                p = m + NJ
                i, j = p // NJ, p % NJ

                @pl.when(j == 0)
                def _():
                    load_p(i).wait()
                    load_o(i).wait()
                    load_o(i + 1).start()

                @pl.when(jnp.logical_and(j == 0, i < 3))
                def _():
                    load_p(i + 1).start()
                swap(p - 2).wait_send()
                pb_load(m).wait()
                pb_start(m + 1)
                r = jnp.dot(lhs[i % 2], wdo[:, cols(j)], preferred_element_type=f32)
                pst[m % 2] = r[:rows].astype(bf16)
                ost[m % 2] = (r[rows:] + pb[m % 2].astype(f32)).astype(bf16)
                swap(p).start()
                ostore(m).start()

                @pl.when(m >= 1)
                def _():
                    post(m - 1)

            @pl.when(s < batch - 1)
            def _():
                forward(s + 1, (4, 5))

            @pl.when(s < batch - 2)
            def _():
                with jax.named_scope("norm2"):
                    for q in range(4):
                        normalise(s + 2, xbuf, q)
            load_o(4).wait()

            @pl.loop(3 * NJ, 4 * NJ)
            def _(m):
                j = m % NJ
                pb_load(m).wait()

                @pl.when(j < NJ - 1)
                def _():
                    pb_start(m + 1)
                r = jnp.dot(lhs[0, rows:], wdo[:, cols(j)], preferred_element_type=f32)
                ost[m % 2] = (r + pb[m % 2].astype(f32)).astype(bf16)
                post(m - 1)
                pltpu.make_async_copy(ost.at[m % 2], own_out.at[s, :, cols(j)], os_sem.at[m % 2]).start()
            ostored(4 * NJ - 1)
            for p in (4 * NJ - 2, 4 * NJ - 1):
                swap(p).wait_send()

            @pl.when(s < batch - 2)
            def _():
                send_first(s + 2, xbuf)
                send_rest(s + 2, xbuf)
        pl.run_scoped(scope, pltpu.VMEM((2, 2 * rows, ff + attn), bf16), pltpu.VMEM((2, rows, ncol), bf16),
                      pltpu.VMEM((2, rows, ncol), bf16), pltpu.VMEM((2, rows, ncol), bf16),
                      pltpu.VMEM((rows, dim), bf16))

    def opening(raw, wide, xbuf):
        kinds = qkv_cols // attn
        per = qkv_cols // 128
        n_parts = 8
        piece_rows = raw.shape[0] // n_parts
        chunk = wide.shape[0] // per

        def load(q):
            at = pl.ds(q * piece_rows, piece_rows)
            return pltpu.make_async_copy(wqkv_hbm.at[at], raw.at[at], o_sem.at[q])

        x_start(0, xbuf)
        for q in range(n_parts):
            load(q).start()
        w_copies[0].start()
        for cp in v_copies:
            cp.wait()
        with jax.named_scope("send0"):
            normalise(0, xbuf, 0)
            normalise(0, xbuf, 1)
            send_first(0, xbuf)
            normalise(0, xbuf, 2)
            normalise(0, xbuf, 3)
            send_rest(0, xbuf)
        with jax.named_scope("place"):
            for q in range(n_parts):
                load(q).wait()

            @pl.loop(0, dim // chunk)
            def _(q):
                wide[...] = raw[pl.ds(pl.multiple_of(q * (chunk * per), chunk * per), chunk * per), :].astype(f32)
                for j in range(kinds):
                    for c in range(head // 128):
                        for g in range(n_heads):
                            row = (j * (head // 128) + c) * n_heads + g
                            col = j * attn + g * head + c * 128
                            wqkv[pl.ds(pl.multiple_of(q * chunk, chunk), chunk), col:col + 128] = (
                                wide[pl.ds(row, chunk, stride=per), :].astype(bf16))
        for cp in w_copies[1:]:
            cp.start()

    pl.run_scoped(opening, pltpu.VMEM((dim * (qkv_cols // 128), 128), bf16),
                  pltpu.VMEM((128 * (qkv_cols // 128), 128), f32), pltpu.VMEM((rows, dim), bf16))

    @pl.loop(0, batch)
    def _(s):
        def scope(qkv):
            with jax.named_scope("A"):
                phase_a(s, qkv)

            with jax.named_scope("B"):
                phase_b(qkv)
        pl.run_scoped(scope, pltpu.VMEM((seq, qkv_cols), bf16))
        with jax.named_scope("D"):
            phase_d(s)

    with jax.named_scope("relay_last"):
        relay_all(batch - 1)

    @pl.loop(0, batch)
    def _(s):
        with jax.named_scope("final"):
            for j in range(NJ):
                to_right(s, 1, j).wait_recv()
                to_left(s, 2, j).wait_recv()
                to_right(s, 1, j).wait_send()
                to_left(s, 2, j).wait_send()
                transit(s, j, right).wait_send()
            for u in range(2 * n_chips):
                d, hf = unit(u)
                d2d_copy(s, u, d, hf, core).wait_send()
                if u >= 2:
                    ici_copy(s, u, d, hf, right).wait_send()


def layer_call(x_blk, ln_gain, ln_bias, wqkv, w_out, w_up, w_down, n_tp):
    batch, rows, dim = x_blk.shape
    ff, attn, qkv_cols = w_up.shape[1], w_out.shape[0], wqkv.shape[0] * 128 // dim
    n_chips = n_tp // 2
    ncol = dim // NJ
    bf16 = jnp.bfloat16
    dma = pltpu.SemaphoreType.DMA
    flops = 2 * batch * n_tp * rows * dim * (qkv_cols + 2 * ff + attn)
    outs = pl.pallas_call(
        layer_kernel,
        name="parallel_layer",
        out_shape=[
            jax.ShapeDtypeStruct((batch, rows, dim), bf16),
            jax.ShapeDtypeStruct((batch, rows, dim), bf16),
            jax.ShapeDtypeStruct((batch, rows, dim), bf16),
            jax.ShapeDtypeStruct((batch, n_chips, 2, rows, dim), bf16),
            jax.ShapeDtypeStruct((n_tp, rows, ff + attn), bf16),
            jax.ShapeDtypeStruct((batch, 4, NJ, rows, ncol), bf16),
            jax.ShapeDtypeStruct((batch, 3, rows, dim), bf16),
            jax.ShapeDtypeStruct((batch, rows, dim), bf16),
        ],
        in_specs=[pl.BlockSpec(memory_space=pl.ANY)] * 7,
        out_specs=[pl.BlockSpec(memory_space=pl.ANY)] * 8,
        scratch_shapes=[
            pltpu.VMEM((dim, qkv_cols), bf16), pltpu.VMEM((dim, ff), bf16), pltpu.VMEM((ff + attn, dim), bf16),
            pltpu.VMEM((1, dim), jnp.float32), pltpu.VMEM((1, dim), jnp.float32),
            dma((batch, 8)), dma((batch, 8)), dma((batch, 8)), dma((batch, 8)),
            dma((2,)), dma((batch, 4 * NJ)), dma((batch, NJ)), dma((batch, NJ)),
            dma((batch, 2 * NJ)), dma((batch, 2 * NJ)),
            dma((3,)), dma((2,)), dma((2, 4)), dma((2,)), dma((2,)), dma((n_tp,)), dma((2, 2)), dma((2,)), dma((2,)),
            dma((3, 2)),
        ],
        compiler_params=pltpu.CompilerParams(
            collective_id=0, has_side_effects=True, vmem_limit_bytes=67043328),
        cost_estimate=pl.CostEstimate(flops=flops, bytes_accessed=256 << 20, transcendentals=0),
    )(x_blk, ln_gain.reshape(1, dim), ln_bias.reshape(1, dim), wqkv, w_out, w_up, w_down)
    return outs[:3]


def solution(mesh):
    n_tp = mesh.shape["tp"]

    def local_layer(x_blk, ln_gain, ln_bias, w_qkv, w_out, w_up, w_down):
        dim = x_blk.shape[2]
        groups, kinds, head = w_qkv.shape[1:]
        wqkv = w_qkv.reshape(dim, groups, kinds, head // 128, 128).transpose(0, 2, 3, 1, 4).reshape(-1, 128)
        own, from_left, from_right = layer_call(x_blk, ln_gain, ln_bias, wqkv, w_out, w_up, w_down, n_tp)
        branch = (own.astype(jnp.float32) + from_left.astype(jnp.float32)
                  + from_right.astype(jnp.float32)).astype(jnp.bfloat16)
        return (x_blk.astype(jnp.float32) + branch.astype(jnp.float32)).astype(jnp.bfloat16)

    return jax.shard_map(
        local_layer, mesh=mesh,
        in_specs=(P("dp", "tp", None), P(), P(), P(None, "tp", None, None),
                  P("tp", None), P(None, "tp"), P("tp", None)),
        out_specs=P("dp", "tp", None), check_vma=False)
```

```python
import jax
import jax.numpy as jnp
from jax import lax
from jax.experimental import pallas as pl
from jax.experimental.pallas import tpu as pltpu
from jax.sharding import PartitionSpec as P

LN_EPS = 1e-5
LOG2_E = 1.4426950408889634
NJ = 4


def layer_kernel(x_ref, gain_ref, bias_ref, wqkv_hbm, wout_hbm, wup_hbm, wdown_hbm,
                 own_out, left_out, right_out, n_all, ho, pbuf, pout, tin,
                 wqkv, wup, wdo, gain, bias,
                 ag_is, ag_ir, ag_ds, ag_dr, p_s, p_r, t_s, t_r, m_s, m_r,
                 w_sem, v_sem, ln_sem, a_sem, h_sem, o_sem, d_sem, pb_sem, os_sem, f_sem):
    batch, rows, dim = x_ref.shape
    half = rows // 2
    ff = wup.shape[1]
    attn = wdo.shape[0] - ff
    qkv_cols = wqkv.shape[1]
    n_heads = 2
    head = attn // n_heads
    n_chips = n_all.shape[1]
    seq = n_chips * 2 * rows
    ncol = dim // NJ
    f32, bf16 = jnp.float32, jnp.bfloat16

    me = lax.axis_index("tp")
    chip, core = me // 2, me % 2
    other = 1 - core
    partner = chip * 2 + other
    right = ((chip + 1) % n_chips) * 2 + core
    left = ((chip + n_chips - 1) % n_chips) * 2 + core

    def remote(src, dst, send, recv, dev):
        return pltpu.make_async_remote_copy(
            src_ref=src, dst_ref=dst, send_sem=send, recv_sem=recv,
            device_id={"tp": dev}, device_id_type=pl.DeviceIdType.MESH)

    barrier = pltpu.get_barrier_semaphore()
    for dev in (partner, right, left):
        pl.semaphore_signal(barrier, inc=1, device_id={"tp": dev}, device_id_type=pl.DeviceIdType.MESH)
    pl.semaphore_wait(barrier, 3)

    w_copies = (
        pltpu.make_async_copy(wup_hbm, wup, w_sem.at[0]),
        pltpu.make_async_copy(wdown_hbm, wdo.at[pl.ds(0, ff)], w_sem.at[1]),
        pltpu.make_async_copy(wout_hbm, wdo.at[pl.ds(ff, attn)], w_sem.at[2]),
    )
    v_copies = (pltpu.make_async_copy(gain_ref, gain, v_sem.at[0]),
                pltpu.make_async_copy(bias_ref, bias, v_sem.at[1]))
    for cp in v_copies:
        cp.start()

    def unit(u):
        g, b = u // 2, u % 2
        near = (g * (3 - g)) // 2
        off = near * (2 * b - 1) + 2 * (g // 3)
        hf = (b + near * (g - 1)) % 2
        return (chip + off + n_chips) % n_chips, hf

    def piece(s, d, hf, k):
        return n_all.at[s, d, hf, pl.ds(pl.multiple_of(k * half, half), half)]

    def ici_copy(s, u, d, hf, dev):
        return remote(piece(s, d, hf, core), piece(s, d, hf, core), ag_is.at[s, u], ag_ir.at[s, u], dev)

    def d2d_copy(s, u, d, hf, k):
        return remote(piece(s, d, hf, k), piece(s, d, hf, k), ag_ds.at[s, u], ag_dr.at[s, u], partner)

    part = rows // 4

    def x_load(s, buf, q):
        at = pl.ds(q * part, part)
        return pltpu.make_async_copy(x_ref.at[s, at], buf.at[at], ln_sem.at[0, q])

    def n_store(s, buf, q):
        dst = n_all.at[s, chip, q // 2, pl.ds(pl.multiple_of(core * half + (q % 2) * part, part), part)]
        return pltpu.make_async_copy(buf.at[pl.ds(q * part, part)], dst, ln_sem.at[1, q])

    def x_start(s, buf):
        for q in range(4):
            x_load(s, buf, q).start()

    def normalise(s, buf, q):
        x_load(s, buf, q).wait()
        at = pl.ds(q * part, part)
        lanes, wide = 128, 512
        total = jnp.zeros((part, lanes), f32)
        for c in range(0, dim, wide):
            v = buf[at, c:c + wide].astype(f32)
            for k in range(0, wide, lanes):
                total = total + v[:, k:k + lanes]
        mean = jnp.sum(total, axis=-1, keepdims=True) * (1.0 / dim)
        total = jnp.zeros((part, lanes), f32)
        for c in range(0, dim, wide):
            cen = buf[at, c:c + wide].astype(f32) - mean
            for k in range(0, wide, lanes):
                total = total + cen[:, k:k + lanes] * cen[:, k:k + lanes]
        inv = lax.rsqrt(jnp.sum(total, axis=-1, keepdims=True) * (1.0 / dim) + LN_EPS)
        for c in range(0, dim, wide):
            cen = buf[at, c:c + wide].astype(f32) - mean
            buf[at, c:c + wide] = (cen * inv * gain[:, c:c + wide] + bias[:, c:c + wide]).astype(bf16)
        n_store(s, buf, q).start()

    def ag_start(s):
        ici_copy(s, 2, chip, 0, right).start()
        ici_copy(s, 3, chip, 1, left).start()
        d2d_copy(s, 0, chip, 0, core).start()
        d2d_copy(s, 1, chip, 1, core).start()
        ici_copy(s, 4, chip, 1, right).start()
        ici_copy(s, 5, chip, 0, left).start()

    def send_first(s, buf):
        n_store(s, buf, 0).wait()
        n_store(s, buf, 1).wait()
        ici_copy(s, 2, chip, 0, right).start()
        d2d_copy(s, 0, chip, 0, core).start()

    def send_rest(s, buf):
        n_store(s, buf, 2).wait()
        n_store(s, buf, 3).wait()
        ici_copy(s, 3, chip, 1, left).start()
        d2d_copy(s, 1, chip, 1, core).start()
        ici_copy(s, 4, chip, 1, right).start()
        ici_copy(s, 5, chip, 0, left).start()

    def forward(s, us):
        for u in us:
            d, hf = unit(u)
            with jax.named_scope(f"ici_wait_{u}"):
                ici_copy(s, u, d, hf, right).wait_recv()
            if u == 2:
                ici_copy(s, 6, d, hf, right).start()
            if u == 3:
                ici_copy(s, 7, d, hf, left).start()
            d2d_copy(s, u, d, hf, core).start()

    def block(b, j):
        near = (b * (3 - b)) // 2
        sign = (2 * (j // (NJ // 2)) - 1) * (3 - 2 * b)
        plus = (near * (1 + sign)) // 2
        return 2 * plus, 1 + 2 * plus + b // 3

    def turn(x):
        return (NJ // 2) * (x % 2) + x // 2

    def cols(j):
        return pl.ds(pl.multiple_of(j * ncol, ncol), ncol)

    def to_right(s, ii, j):
        return remote(pout.at[s, ii, :, cols(j)], left_out.at[s, :, cols(j)], m_s.at[s, j], m_r.at[s, j], right)

    def to_left(s, ii, j):
        return remote(pout.at[s, ii, :, cols(j)], right_out.at[s, :, cols(j)], m_s.at[s, NJ + j], m_r.at[s, NJ + j],
                      left)

    def transit(s, j, dev):
        return remote(pout.at[s, 0, :, cols(j)], tin.at[s, :, cols(j)], t_s.at[s, j], t_r.at[s, j], dev)

    def relay_loads(s, q, k, a, b):
        return (pltpu.make_async_copy(pout.at[s, 2, :, cols(q)], a, f_sem.at[0, k]),
                pltpu.make_async_copy(tin.at[s, :, cols(q)], b, f_sem.at[1, k]))

    def relay_store(s, q, k, a):
        return pltpu.make_async_copy(a, pout.at[s, 2, :, cols(q)], f_sem.at[2, k])

    def relay_start(s, q, k, a, b):
        transit(s, q, right).wait_recv()
        for cp in relay_loads(s, q, k, a, b):
            cp.start()

    def relay_add(s, q, k, a, b):
        for cp in relay_loads(s, q, k, a, b):
            cp.wait()
        step = 64

        @pl.loop(0, rows // step)
        def _(r):
            at = pl.ds(pl.multiple_of(r * step, step), step)
            a[at, :] = (a[at, :].astype(f32) + b[at, :].astype(f32)).astype(bf16)
        relay_store(s, q, k, a).start()

    def relay_send(s, q, k, a):
        relay_store(s, q, k, a).wait()
        if q < NJ // 2:
            to_right(s, 2, q).start()
        else:
            to_left(s, 2, q).start()

    def relay_all(s):
        def scope(a, b):
            order = (0, 2, 1, 3)

            def bufs(n):
                return n % 2, a.at[n % 2], b.at[n % 2]
            relay_start(s, order[0], *bufs(0))
            for n in range(NJ):
                if n + 1 < NJ:
                    if n >= 1:
                        relay_send(s, order[n - 1], *bufs(n - 1)[:2])
                    relay_start(s, order[n + 1], *bufs(n + 1))
                relay_add(s, order[n], *bufs(n))
            for n in (NJ - 2, NJ - 1):
                relay_send(s, order[n], *bufs(n)[:2])
        pl.run_scoped(scope, pltpu.VMEM((2, rows, ncol), bf16), pltpu.VMEM((2, rows, ncol), bf16))

    def gelu(h):
        return (0.5 * h * (1.0 + lax.erf(h * (2.0 ** -0.5)))).astype(bf16)

    def phase_a(s, qkv):
        def scope(nbuf, hbuf):
            first = s == 0

            def load(u):
                d, hf = unit(u)
                return pltpu.make_async_copy(n_all.at[s, d, hf], nbuf.at[u % 2], a_sem.at[u % 2])

            def arrived(u):
                d, hf = unit(u)
                with jax.named_scope("d2d_wait"):
                    d2d_copy(s, u, d, hf, other).wait_recv()

            def hstore(u, k):
                d, hf = unit(u)
                return pltpu.make_async_copy(
                    hbuf.at[pl.ds(k * half, half)],
                    ho.at[2 * d + k, pl.ds(pl.multiple_of(hf * half, half), half), pl.ds(0, ff)],
                    h_sem.at[k])

            def project(u):
                d, hf = unit(u)
                r = jnp.dot(nbuf[u % 2], wqkv[...], preferred_element_type=f32).astype(bf16)
                for k in range(2):
                    pos = pl.multiple_of(d * (2 * rows) + k * rows + hf * half, half)
                    qkv[pl.ds(pos, half), :] = r[k * half:(k + 1) * half]

            arrived(0)
            load(0).start()

            @pl.loop(0, 2 * n_chips)
            def _(u):
                odd = u % 2 == 1
                with jax.named_scope("load_wait"):
                    load(u).wait()

                @pl.when(jnp.logical_and(s > 0, u == 4))
                def _():
                    forward(s, (6, 7))

                @pl.when(jnp.logical_or(jnp.logical_and(s > 0, u < 7), u % 2 == 0))
                def _():
                    arrived(u + 1)
                    load(u + 1).start()

                @pl.when(s > 0)
                def _():
                    project(u)

                @pl.when(first)
                def _():
                    @pl.when(jnp.logical_and(odd, u < 7))
                    def _():
                        x_start((u + 1) // 2, nbuf.at[0])

                    @pl.when(u == 0)
                    def _():
                        w_copies[0].wait()
                    project(u)

                    @pl.when(u >= 1)
                    def _():
                        for k in range(2):
                            hstore(u - 1, k).wait()
                    hbuf[...] = gelu(jnp.dot(nbuf[u % 2], wup[...], preferred_element_type=f32))
                    for k in range(2):
                        hstore(u, k).start()

                    @pl.when(u == 1)
                    def _():
                        forward(0, (2, 3))

                    @pl.when(u == 3)
                    def _():
                        forward(0, (4, 5))

                    @pl.when(u == 5)
                    def _():
                        forward(0, (6, 7))

                    @pl.when(jnp.logical_and(odd, u < 7))
                    def _():
                        with jax.named_scope("norm"):
                            for q in range(4):
                                normalise((u + 1) // 2, nbuf.at[0], q)
                            for q in range(4):
                                n_store((u + 1) // 2, nbuf.at[0], q).wait()

                        @pl.when(u == 1)
                        def _():
                            ag_start(1)
                        arrived(u + 1)
                        load(u + 1).start()

            @pl.when(first)
            def _():
                for k in range(2):
                    hstore(7, k).wait()
        pl.run_scoped(scope, pltpu.VMEM((2, rows, dim), bf16), pltpu.VMEM((rows, ff), bf16))

    def phase_b(qkv):
        def ostore(t):
            return pltpu.make_async_copy(qkv.at[pl.ds(t * rows, rows), pl.ds(0, attn)],
                                         ho.at[t, :, pl.ds(ff, attn)], o_sem.at[t])
        scale = head ** -0.5

        def scope(scores, probs):
            keep = (lax.broadcasted_iota(jnp.int32, (rows, rows), 0)
                    >= lax.broadcasted_iota(jnp.int32, (rows, rows), 1))
            tasks = [(t, h) for t in range(seq // rows) for h in range(n_heads)]
            tops = {}

            def score(i):
                t, h = tasks[i]
                r0, n = t * rows, (t + 1) * rows
                q = qkv[r0:n, h * head:(h + 1) * head]
                k = qkv[0:n, attn + h * head:attn + (h + 1) * head]
                sc = lax.dot_general(q, k, (((1,), (1,)), ((), ())), preferred_element_type=f32)
                diag = jnp.where(keep, sc[:, r0:], -jnp.inf)
                top = jnp.max(diag, axis=1, keepdims=True)
                if t:
                    scores[i % 2, :, 0:r0] = sc[:, :r0]
                    top = jnp.maximum(top, jnp.max(sc[:, :r0], axis=1, keepdims=True))
                scores[i % 2, :, r0:n] = diag
                tops[i] = top

            def soften(i):
                t, h = tasks[i]
                n = (t + 1) * rows
                total = jnp.zeros((rows, rows // 2), f32)
                for c in range(0, n, rows):
                    e = jnp.exp2((scores[i % 2, :, c:c + rows] - tops[i]) * (scale * LOG2_E))
                    scores[i % 2, :, c:c + rows] = e
                    total = total + e[:, :rows // 2] + e[:, rows // 2:]
                inverse = 1.0 / jnp.sum(total, axis=1, keepdims=True)
                for c in range(0, n, rows):
                    probs[i % 2, :, c:c + rows] = (scores[i % 2, :, c:c + rows] * inverse).astype(bf16)

            def mix(i):
                t, h = tasks[i]
                r0, n = t * rows, (t + 1) * rows
                v = qkv[0:n, 2 * attn + h * head:2 * attn + (h + 1) * head]
                o = jnp.dot(probs[i % 2, :, 0:n], v, preferred_element_type=f32)
                qkv[r0:n, h * head:(h + 1) * head] = o.astype(bf16)

            score(0)
            for i in range(len(tasks)):
                if i + 1 < len(tasks):
                    score(i + 1)
                soften(i)
                mix(i)
                if i % n_heads == n_heads - 1 and tasks[i][0] % 4 == 3:
                    for done in range(tasks[i][0] - 3, tasks[i][0] + 1):
                        ostore(done).start()
            for t in range(seq // rows):
                ostore(t).wait()
        pl.run_scoped(scope, pltpu.VMEM((n_heads, rows, seq), f32), pltpu.VMEM((n_heads, rows, seq), bf16))

    def phase_d(s):
        def scope(lhs, nbuf, pst, ost, pb, tb):
            def chip_of(w):
                near = (w * (3 - w)) // 2
                off = near * (3 - 2 * w) + 2 * ((3 - w) // 3)
                plus = near * (2 - w)
                return (chip + off + n_chips) % n_chips, 2 * plus, 1 + 2 * plus + w // 3

            def rows_load(w, own, whole):
                d, slot_p, slot_o = chip_of(w)
                src = ho.at[2 * d + (core if own else other)]
                dst = lhs.at[slot_o if own else slot_p]
                if not whole:
                    src, dst = src.at[:, pl.ds(ff, attn)], dst.at[:, pl.ds(ff, attn)]
                return pltpu.make_async_copy(src, dst, d_sem.at[own])

            def n_load(v):
                d, _, _ = chip_of(v // 2)
                return pltpu.make_async_copy(n_all.at[s, d, v % 2], nbuf.at[v % 2], a_sem.at[v % 2])

            def hide(v):
                _, slot_p, slot_o = chip_of(v // 2)
                r = gelu(jnp.dot(nbuf[v % 2], wup[...], preferred_element_type=f32))
                for k in range(2):
                    own = 1 - (k + core) % 2
                    slot = slot_p + own * (slot_o - slot_p)
                    lhs[slot, pl.ds(pl.multiple_of((v % 2) * half, half), half), 0:ff] = r[k * half:(k + 1) * half]

            def swap(p):
                return remote(pst.at[p % 2], pbuf.at[s, p // NJ, p % NJ], p_s.at[p % 2], p_r.at[s, p], partner)

            def pb_load(q):
                return pltpu.make_async_copy(pbuf.at[s, q // NJ, q % NJ], pb.at[q % 2], pb_sem.at[q % 2])

            def pb_start(q):
                with jax.named_scope("swap_wait"):
                    swap(q).wait_recv()
                pb_load(q).start()

            def t_load(j):
                return pltpu.make_async_copy(tin.at[s, :, cols(j)], tb, f_sem.at[0, 0])

            def stored(q):
                pltpu.make_async_copy(ost.at[q % 2], pout.at[s, 0, :, cols(turn(q % NJ))], os_sem.at[q % 2]).wait()

            def post(q):
                stored(q)
                b, j = q // NJ, turn(q % NJ)
                low = j < NJ // 2

                @pl.when(b == 0)
                def _():
                    @pl.when(low)
                    def _():
                        transit(s, j, right).start()

                    @pl.when(jnp.logical_not(low))
                    def _():
                        transit(s, j, left).start()

                @pl.when(b == 1)
                def _():
                    @pl.when(low)
                    def _():
                        to_left(s, 1, j).start()

                    @pl.when(jnp.logical_not(low))
                    def _():
                        to_right(s, 1, j).start()

                @pl.when(jnp.logical_and(s > 0, b == 2))
                def _():
                    @pl.when(low)
                    def _():
                        to_right(s, 2, j).start()

                    @pl.when(jnp.logical_not(low))
                    def _():
                        to_left(s, 2, j).start()

            def partner_step(g, b, x):
                p, j = b * NJ + x, turn(x)
                slot_p, _ = block(b, j)

                @pl.when(p >= 2)
                def _():
                    swap(p - 2).wait_send()

                @pl.when(jnp.logical_and(x == NJ - 1, jnp.logical_or(g == 0, g == 2)))
                def _():
                    pb_start(2 * g)

                @pl.when(jnp.logical_and(b == 3, s > 0))
                def _():
                    with jax.named_scope("transit_wait"):
                        transit(s, j, right).wait_recv()
                    t_load(j).start()
                r = jnp.dot(lhs[slot_p], wdo[:, cols(j)], preferred_element_type=f32)
                pst[p % 2] = r.astype(bf16)
                swap(p).start()

            def own_step(b, x):
                q, j = b * NJ + x, turn(x)
                _, slot_o = block(b, j)
                pb_load(q).wait()

                @pl.when(jnp.logical_and(q != NJ - 1, q < 4 * NJ - 1))
                def _():
                    pb_start(q + 1)
                r = jnp.dot(lhs[slot_o], wdo[:, cols(j)], preferred_element_type=f32)
                ost[q % 2] = (r + pb[q % 2].astype(f32)).astype(bf16)

                @pl.when(jnp.logical_and(b == 2, s > 0))
                def _():
                    t_load(j).wait()
                    step = 64

                    @pl.loop(0, rows // step)
                    def _(r):
                        at = pl.ds(pl.multiple_of(r * step, step), step)
                        ost[q % 2, at, :] = (ost[q % 2, at, :].astype(f32) + tb[at, :].astype(f32)).astype(bf16)

                @pl.when(b < 3)
                def _():
                    pltpu.make_async_copy(ost.at[q % 2], pout.at[s, b, :, cols(j)], os_sem.at[q % 2]).start()

                @pl.when(b == 3)
                def _():
                    pltpu.make_async_copy(ost.at[q % 2], own_out.at[s, :, cols(j)], os_sem.at[q % 2]).start()

                @pl.when(jnp.logical_or(x >= 1, b == 3))
                def _():
                    post(q - 1)

            @pl.when(s > 0)
            def _():
                n_load(0).start()

            @pl.when(s == 0)
            def _():
                w_copies[1].wait()
                w_copies[2].wait()

            @pl.loop(0, 6)
            def _(g):
                e = g // 2
                w0 = (e * (e + 1)) // 2
                n_w = (1 - g % 2) * (1 + e % 2)

                def flush():
                    @pl.when(jnp.logical_or(jnp.logical_and(g == 2, True), g == 4))
                    def _():
                        post(2 * g - 1)

                @pl.loop(w0, w0 + n_w)
                def _(w):
                    @pl.when(s == 0)
                    def _():
                        for own in range(2):
                            rows_load(w, own, True).start()
                        for own in range(2):
                            rows_load(w, own, True).wait()

                        @pl.when(w == w0)
                        def _():
                            flush()

                    @pl.when(s > 0)
                    def _():
                        for own in range(2):
                            rows_load(w, own, False).start()

                        @pl.loop(2 * w, 2 * w + 2)
                        def _(v):
                            with jax.named_scope("n_wait"):
                                n_load(v).wait()

                            @pl.when(v < 2 * n_chips - 1)
                            def _():
                                n_load(v + 1).start()

                            @pl.when(v == 2 * w0 + 1)
                            def _():
                                flush()
                            with jax.named_scope("hide"):
                                hide(v)
                        for own in range(2):
                            rows_load(w, own, False).wait()

                @pl.loop(0, NJ)
                def _(x):
                    @pl.when(jnp.logical_and(g != 1, g != 5))
                    def _():
                        with jax.named_scope("partner"):
                            partner_step(g, (3 * g) // 4, x)

                    @pl.when(jnp.logical_and(g != 0, g != 2))
                    def _():
                        with jax.named_scope("own"):
                            own_step((g * g) // 8, x)

                @pl.when(jnp.logical_and(s < batch - 1, g == 2))
                def _():
                    forward(s + 1, (2, 3))

                @pl.when(jnp.logical_and(s < batch - 1, g == 4))
                def _():
                    forward(s + 1, (4, 5))

            stored(4 * NJ - 1)
            for p in (4 * NJ - 2, 4 * NJ - 1):
                swap(p).wait_send()

            @pl.when(s < batch - 2)
            def _():
                ag_start(s + 2)
        chunk = pltpu.VMEM((2, rows, ncol), bf16)
        pl.run_scoped(scope, pltpu.VMEM((4, rows, ff + attn), bf16), pltpu.VMEM((2, rows, dim), bf16),
                      chunk, chunk, chunk, pltpu.VMEM((rows, ncol), bf16))

    def opening(raw, wide, xbuf):
        kinds = qkv_cols // attn
        per = qkv_cols // 128
        n_parts = 8
        piece_rows = raw.shape[0] // n_parts
        chunk = wide.shape[0] // per

        def load(q):
            at = pl.ds(q * piece_rows, piece_rows)
            return pltpu.make_async_copy(wqkv_hbm.at[at], raw.at[at], o_sem.at[q])

        x_start(0, xbuf)
        for q in range(n_parts):
            load(q).start()
        w_copies[0].start()
        for cp in v_copies:
            cp.wait()
        with jax.named_scope("send0"):
            normalise(0, xbuf, 0)
            normalise(0, xbuf, 1)
            send_first(0, xbuf)
            normalise(0, xbuf, 2)
            normalise(0, xbuf, 3)
            send_rest(0, xbuf)
        with jax.named_scope("place"):
            for q in range(n_parts):
                load(q).wait()

            @pl.loop(0, dim // chunk)
            def _(q):
                wide[...] = raw[pl.ds(pl.multiple_of(q * (chunk * per), chunk * per), chunk * per), :].astype(f32)
                for j in range(kinds):
                    for c in range(head // 128):
                        for g in range(n_heads):
                            row = (j * (head // 128) + c) * n_heads + g
                            col = j * attn + g * head + c * 128
                            wqkv[pl.ds(pl.multiple_of(q * chunk, chunk), chunk), col:col + 128] = (
                                wide[pl.ds(row, chunk, stride=per), :].astype(bf16))
        for cp in w_copies[1:]:
            cp.start()

    pl.run_scoped(opening, pltpu.VMEM((dim * (qkv_cols // 128), 128), bf16),
                  pltpu.VMEM((128 * (qkv_cols // 128), 128), f32), pltpu.VMEM((rows, dim), bf16))

    @pl.loop(0, batch)
    def _(s):
        def scope(qkv):
            with jax.named_scope("A"):
                phase_a(s, qkv)

            @pl.when(s == 1)
            def _():
                with jax.named_scope("relay0"):
                    relay_all(0)

            with jax.named_scope("B"):
                phase_b(qkv)
        pl.run_scoped(scope, pltpu.VMEM((seq, qkv_cols), bf16))
        with jax.named_scope("D"):
            phase_d(s)

    @pl.loop(0, batch)
    def _(s):
        with jax.named_scope("final"):
            for j in range(NJ):
                to_right(s, 2, j).wait_recv()
                to_left(s, 2, j).wait_recv()
                to_right(s, 2, j).wait_send()
                to_left(s, 2, j).wait_send()
                transit(s, j, right).wait_send()
            for u in range(2 * n_chips):
                d, hf = unit(u)
                d2d_copy(s, u, d, hf, core).wait_send()
                if u >= 2:
                    ici_copy(s, u, d, hf, right).wait_send()


def layer_call(x_blk, ln_gain, ln_bias, wqkv, w_out, w_up, w_down, n_tp):
    batch, rows, dim = x_blk.shape
    ff, attn, qkv_cols = w_up.shape[1], w_out.shape[0], wqkv.shape[0] * 128 // dim
    n_chips = n_tp // 2
    ncol = dim // NJ
    bf16 = jnp.bfloat16
    dma = pltpu.SemaphoreType.DMA
    flops = 2 * batch * n_tp * rows * dim * (qkv_cols + 2 * ff + attn)
    outs = pl.pallas_call(
        layer_kernel,
        name="parallel_layer",
        out_shape=[
            jax.ShapeDtypeStruct((batch, rows, dim), bf16),
            jax.ShapeDtypeStruct((batch, rows, dim), bf16),
            jax.ShapeDtypeStruct((batch, rows, dim), bf16),
            jax.ShapeDtypeStruct((batch, n_chips, 2, rows, dim), bf16),
            jax.ShapeDtypeStruct((n_tp, rows, ff + attn), bf16),
            jax.ShapeDtypeStruct((batch, 4, NJ, rows, ncol), bf16),
            jax.ShapeDtypeStruct((batch, 3, rows, dim), bf16),
            jax.ShapeDtypeStruct((batch, rows, dim), bf16),
        ],
        in_specs=[pl.BlockSpec(memory_space=pl.ANY)] * 7,
        out_specs=[pl.BlockSpec(memory_space=pl.ANY)] * 8,
        scratch_shapes=[
            pltpu.VMEM((dim, qkv_cols), bf16), pltpu.VMEM((dim, ff), bf16), pltpu.VMEM((ff + attn, dim), bf16),
            pltpu.VMEM((1, dim), jnp.float32), pltpu.VMEM((1, dim), jnp.float32),
            dma((batch, 8)), dma((batch, 8)), dma((batch, 8)), dma((batch, 8)),
            dma((2,)), dma((batch, 4 * NJ)), dma((batch, NJ)), dma((batch, NJ)),
            dma((batch, 2 * NJ)), dma((batch, 2 * NJ)),
            dma((3,)), dma((2,)), dma((2, 4)), dma((2,)), dma((2,)), dma((n_tp,)), dma((2,)), dma((2,)), dma((2,)),
            dma((3, 2)),
        ],
        compiler_params=pltpu.CompilerParams(
            collective_id=0, has_side_effects=True, vmem_limit_bytes=67043328),
        cost_estimate=pl.CostEstimate(flops=flops, bytes_accessed=256 << 20, transcendentals=0),
    )(x_blk, ln_gain.reshape(1, dim), ln_bias.reshape(1, dim), wqkv, w_out, w_up, w_down)
    return outs[:3]


def solution(mesh):
    n_tp = mesh.shape["tp"]

    def local_layer(x_blk, ln_gain, ln_bias, w_qkv, w_out, w_up, w_down):
        dim = x_blk.shape[2]
        groups, kinds, head = w_qkv.shape[1:]
        wqkv = w_qkv.reshape(dim, groups, kinds, head // 128, 128).transpose(0, 2, 3, 1, 4).reshape(-1, 128)
        own, from_left, from_right = layer_call(x_blk, ln_gain, ln_bias, wqkv, w_out, w_up, w_down, n_tp)
        branch = (own.astype(jnp.float32) + from_left.astype(jnp.float32)
                  + from_right.astype(jnp.float32)).astype(jnp.bfloat16)
        return (x_blk.astype(jnp.float32) + branch.astype(jnp.float32)).astype(jnp.bfloat16)

    return jax.shard_map(
        local_layer, mesh=mesh,
        in_specs=(P("dp", "tp", None), P(), P(), P(None, "tp", None, None),
                  P("tp", None), P(None, "tp"), P("tp", None)),
        out_specs=P("dp", "tp", None), check_vma=False)
```

```python
import jax
import jax.numpy as jnp
from jax import lax
from jax.experimental import pallas as pl
from jax.experimental.pallas import tpu as pltpu
from jax.sharding import PartitionSpec as P

LN_EPS = 1e-5
LOG2_E = 1.4426950408889634
NJ = 4


def layer_kernel(x_ref, gain_ref, bias_ref, wqkv_hbm, wout_hbm, wup_hbm, wdown_hbm,
                 own_out, left_out, right_out, n_all, ho, pbuf, pout, tin,
                 wqkv, wup, wdo, gain, bias, nbuf,
                 ag_is, ag_ir, ag_ds, ag_dr, p_s, p_r, t_s, t_r, m_s, m_r,
                 w_sem, v_sem, ln_sem, a_sem, h_sem, o_sem, d_sem, pb_sem, os_sem, f_sem):
    batch, rows, dim = x_ref.shape
    half = rows // 2
    ff = wup.shape[1]
    attn = wdo.shape[0] - ff
    qkv_cols = wqkv.shape[1]
    n_heads = 2
    head = attn // n_heads
    n_chips = n_all.shape[1]
    seq = n_chips * 2 * rows
    ncol = dim // NJ
    f32, bf16 = jnp.float32, jnp.bfloat16

    me = lax.axis_index("tp")
    chip, core = me // 2, me % 2
    other = 1 - core
    partner = chip * 2 + other
    right = ((chip + 1) % n_chips) * 2 + core
    left = ((chip + n_chips - 1) % n_chips) * 2 + core

    def remote(src, dst, send, recv, dev):
        return pltpu.make_async_remote_copy(
            src_ref=src, dst_ref=dst, send_sem=send, recv_sem=recv,
            device_id={"tp": dev}, device_id_type=pl.DeviceIdType.MESH)

    barrier = pltpu.get_barrier_semaphore()
    for dev in (partner, right, left):
        pl.semaphore_signal(barrier, inc=1, device_id={"tp": dev}, device_id_type=pl.DeviceIdType.MESH)
    pl.semaphore_wait(barrier, 3)

    w_copies = (
        pltpu.make_async_copy(wup_hbm, wup, w_sem.at[0]),
        pltpu.make_async_copy(wdown_hbm, wdo.at[pl.ds(0, ff)], w_sem.at[1]),
        pltpu.make_async_copy(wout_hbm, wdo.at[pl.ds(ff, attn)], w_sem.at[2]),
    )
    v_copies = (pltpu.make_async_copy(gain_ref, gain, v_sem.at[0]),
                pltpu.make_async_copy(bias_ref, bias, v_sem.at[1]))
    for cp in v_copies:
        cp.start()

    def unit(u):
        g, b = u // 2, u % 2
        near = (g * (3 - g)) // 2
        off = near * (2 * b - 1) + 2 * (g // 3)
        hf = (b + near * (g - 1)) % 2
        return (chip + off + n_chips) % n_chips, hf

    def piece(s, d, hf, k):
        return n_all.at[s, d, hf, pl.ds(pl.multiple_of(k * half, half), half)]

    def ici_copy(s, u, d, hf, dev):
        return remote(piece(s, d, hf, core), piece(s, d, hf, core), ag_is.at[s, u], ag_ir.at[s, u], dev)

    def d2d_copy(s, u, d, hf, k):
        return remote(piece(s, d, hf, k), piece(s, d, hf, k), ag_ds.at[s, u], ag_dr.at[s, u], partner)

    part = rows // 4

    def x_load(s, buf, q):
        at = pl.ds(q * part, part)
        return pltpu.make_async_copy(x_ref.at[s, at], buf.at[at], ln_sem.at[0, q])

    def n_store(s, buf, q):
        dst = n_all.at[s, chip, q // 2, pl.ds(pl.multiple_of(core * half + (q % 2) * part, part), part)]
        return pltpu.make_async_copy(buf.at[pl.ds(q * part, part)], dst, ln_sem.at[1, q])

    def x_start(s, buf):
        for q in range(4):
            x_load(s, buf, q).start()

    def normalise(s, buf, q):
        x_load(s, buf, q).wait()
        at = pl.ds(q * part, part)
        lanes, wide = 128, 512
        total = jnp.zeros((part, lanes), f32)
        for c in range(0, dim, wide):
            v = buf[at, c:c + wide].astype(f32)
            for k in range(0, wide, lanes):
                total = total + v[:, k:k + lanes]
        mean = jnp.sum(total, axis=-1, keepdims=True) * (1.0 / dim)
        total = jnp.zeros((part, lanes), f32)
        for c in range(0, dim, wide):
            cen = buf[at, c:c + wide].astype(f32) - mean
            for k in range(0, wide, lanes):
                total = total + cen[:, k:k + lanes] * cen[:, k:k + lanes]
        inv = lax.rsqrt(jnp.sum(total, axis=-1, keepdims=True) * (1.0 / dim) + LN_EPS)
        for c in range(0, dim, wide):
            cen = buf[at, c:c + wide].astype(f32) - mean
            buf[at, c:c + wide] = (cen * inv * gain[:, c:c + wide] + bias[:, c:c + wide]).astype(bf16)
        n_store(s, buf, q).start()

    def ag_start(s):
        ici_copy(s, 2, chip, 0, right).start()
        ici_copy(s, 3, chip, 1, left).start()
        d2d_copy(s, 0, chip, 0, core).start()
        d2d_copy(s, 1, chip, 1, core).start()
        ici_copy(s, 4, chip, 1, right).start()
        ici_copy(s, 5, chip, 0, left).start()

    def send_first(s, buf):
        n_store(s, buf, 0).wait()
        n_store(s, buf, 1).wait()
        ici_copy(s, 2, chip, 0, right).start()
        d2d_copy(s, 0, chip, 0, core).start()

    def send_rest(s, buf):
        n_store(s, buf, 2).wait()
        n_store(s, buf, 3).wait()
        ici_copy(s, 3, chip, 1, left).start()
        d2d_copy(s, 1, chip, 1, core).start()
        ici_copy(s, 4, chip, 1, right).start()
        ici_copy(s, 5, chip, 0, left).start()

    def forward(s, us):
        for u in us:
            d, hf = unit(u)
            with jax.named_scope(f"ici_wait_{u}"):
                ici_copy(s, u, d, hf, right).wait_recv()
            if u == 2:
                ici_copy(s, 6, d, hf, right).start()
            if u == 3:
                ici_copy(s, 7, d, hf, left).start()
            d2d_copy(s, u, d, hf, core).start()

    def block(b, second):
        near = (b * (3 - b)) // 2
        plus = (near * (1 + (2 * second - 1) * (3 - 2 * b))) // 2
        return 2 * plus, 1 + 2 * plus + b // 3

    def cols(j):
        return pl.ds(pl.multiple_of(j * ncol, ncol), ncol)

    def to_right(s, ii, j):
        return remote(pout.at[s, ii, :, cols(j)], left_out.at[s, :, cols(j)], m_s.at[s, j], m_r.at[s, j], right)

    def to_left(s, ii, j):
        return remote(pout.at[s, ii, :, cols(j)], right_out.at[s, :, cols(j)], m_s.at[s, NJ + j], m_r.at[s, NJ + j],
                      left)

    def transit(s, j, dev):
        return remote(pout.at[s, 0, :, cols(j)], tin.at[s, :, cols(j)], t_s.at[s, j], t_r.at[s, j], dev)

    def first_load(s):
        return pltpu.make_async_copy(n_all.at[s, chip, 0], nbuf.at[0], a_sem.at[0])

    def first_start(s):
        with jax.named_scope("d2d_wait"):
            d2d_copy(s, 0, chip, 0, other).wait_recv()
        first_load(s).start()

    def gelu(h):
        return (0.5 * h * (1.0 + lax.erf(h * (2.0 ** -0.5)))).astype(bf16)

    def phase_a(s, qkv):
        def scope(hbuf):
            first = s == 0

            def load(u):
                d, hf = unit(u)
                return pltpu.make_async_copy(n_all.at[s, d, hf], nbuf.at[u % 2], a_sem.at[u % 2])

            def arrived(u):
                d, hf = unit(u)
                with jax.named_scope("d2d_wait"):
                    d2d_copy(s, u, d, hf, other).wait_recv()

            def hstore(u, k):
                d, hf = unit(u)
                return pltpu.make_async_copy(
                    hbuf.at[pl.ds(k * half, half)],
                    ho.at[2 * d + k, pl.ds(pl.multiple_of(hf * half, half), half), pl.ds(0, ff)],
                    h_sem.at[k])

            def project(u):
                d, hf = unit(u)
                wide = 512
                for c in range(0, qkv_cols, wide):
                    r = jnp.dot(nbuf[u % 2], wqkv[:, c:c + wide], preferred_element_type=f32).astype(bf16)
                    for k in range(2):
                        pos = pl.multiple_of(d * (2 * rows) + k * rows + hf * half, half)
                        qkv[pl.ds(pos, half), c:c + wide] = r[k * half:(k + 1) * half]

            @pl.when(first)
            def _():
                first_start(s)

            @pl.loop(0, 2 * n_chips)
            def _(u):
                odd = u % 2 == 1
                with jax.named_scope("load_wait"):
                    load(u).wait()

                @pl.when(jnp.logical_and(s > 0, u == 4))
                def _():
                    forward(s, (6, 7))

                @pl.when(jnp.logical_or(jnp.logical_and(s > 0, u < 7), u % 2 == 0))
                def _():
                    arrived(u + 1)
                    load(u + 1).start()

                @pl.when(s > 0)
                def _():
                    project(u)

                @pl.when(first)
                def _():
                    @pl.when(jnp.logical_and(odd, u < 7))
                    def _():
                        x_start((u + 1) // 2, nbuf.at[0])

                    @pl.when(u == 0)
                    def _():
                        w_copies[0].wait()
                        for cp in w_copies[1:]:
                            cp.start()
                    project(u)

                    @pl.when(u >= 1)
                    def _():
                        for k in range(2):
                            hstore(u - 1, k).wait()
                    hbuf[...] = gelu(jnp.dot(nbuf[u % 2], wup[...], preferred_element_type=f32))
                    for k in range(2):
                        hstore(u, k).start()

                    @pl.when(u == 1)
                    def _():
                        forward(0, (2, 3))

                    @pl.when(u == 3)
                    def _():
                        forward(0, (4, 5))

                    @pl.when(u == 5)
                    def _():
                        forward(0, (6, 7))

                    @pl.when(jnp.logical_and(odd, u < 7))
                    def _():
                        with jax.named_scope("norm"):
                            for q in range(4):
                                normalise((u + 1) // 2, nbuf.at[0], q)
                            for q in range(4):
                                n_store((u + 1) // 2, nbuf.at[0], q).wait()

                        @pl.when(u == 1)
                        def _():
                            ag_start(1)
                        arrived(u + 1)
                        load(u + 1).start()

            @pl.when(first)
            def _():
                for k in range(2):
                    hstore(7, k).wait()
        pl.run_scoped(scope, pltpu.VMEM((rows, ff), bf16))

    def phase_b(qkv):
        def ostore(t):
            return pltpu.make_async_copy(qkv.at[pl.ds(t * rows, rows), pl.ds(0, attn)],
                                         ho.at[t, :, pl.ds(ff, attn)], o_sem.at[t])
        scale = head ** -0.5

        probs = nbuf.at[1]

        def scope(*scores):
            keep = (lax.broadcasted_iota(jnp.int32, (rows, rows), 0)
                    >= lax.broadcasted_iota(jnp.int32, (rows, rows), 1))
            tasks = [(t, h) for t in range(seq // rows) for h in range(n_heads)]
            tops = {}

            def score(i):
                t, h = tasks[i]
                r0, n = t * rows, (t + 1) * rows
                q = qkv[r0:n, h * head:(h + 1) * head]
                k = qkv[0:n, attn + h * head:attn + (h + 1) * head]
                sc = lax.dot_general(q, k, (((1,), (1,)), ((), ())), preferred_element_type=f32)
                diag = jnp.where(keep, sc[:, r0:], -jnp.inf)
                top = jnp.max(diag, axis=1, keepdims=True)
                if t:
                    scores[i % 2][0, :, 0:r0] = sc[:, :r0]
                    top = jnp.maximum(top, jnp.max(sc[:, :r0], axis=1, keepdims=True))
                scores[i % 2][0, :, r0:n] = diag
                tops[i] = top

            def soften(i):
                t, h = tasks[i]
                n = (t + 1) * rows
                total = jnp.zeros((rows, rows // 2), f32)
                for c in range(0, n, rows):
                    e = jnp.exp2((scores[i % 2][0, :, c:c + rows] - tops[i]) * (scale * LOG2_E))
                    scores[i % 2][0, :, c:c + rows] = e
                    total = total + e[:, :rows // 2] + e[:, rows // 2:]
                inverse = 1.0 / jnp.sum(total, axis=1, keepdims=True)
                for c in range(0, n, rows):
                    probs[:, (i % 2) * seq + c:(i % 2) * seq + c + rows] = (
                        scores[i % 2][0, :, c:c + rows] * inverse).astype(bf16)

            def mix(i):
                t, h = tasks[i]
                r0, n = t * rows, (t + 1) * rows
                v = qkv[0:n, 2 * attn + h * head:2 * attn + (h + 1) * head]
                o = jnp.dot(probs[:, (i % 2) * seq:(i % 2) * seq + n], v, preferred_element_type=f32)
                qkv[r0:n, h * head:(h + 1) * head] = o.astype(bf16)

            score(0)
            for i in range(len(tasks)):
                if i + 1 < len(tasks):
                    score(i + 1)
                soften(i)
                mix(i)
                if i % n_heads == n_heads - 1 and tasks[i][0] % 4 == 3:
                    for done in range(tasks[i][0] - 3, tasks[i][0] + 1):
                        ostore(done).start()
            for t in range(seq // rows):
                ostore(t).wait()
        pl.run_scoped(scope, pltpu.VMEM((1, rows, seq), f32), pltpu.VMEM((1, rows, seq), f32))

    def chip_of(w):
        near = (w * (3 - w)) // 2
        off = near * (3 - 2 * w) + 2 * ((3 - w) // 3)
        plus = near * (2 - w)
        return (chip + off + n_chips) % n_chips, 2 * plus, 1 + 2 * plus + w // 3

    def place_of(v):
        return (v % 3) * (2 - v % 3)

    def rows_load(s, v):
        d, _, _ = chip_of(v // 2)
        return pltpu.make_async_copy(n_all.at[s, d, v % 2], nbuf.at[place_of(v)], a_sem.at[place_of(v)])

    def rows_start(s, v):
        rows_load(s, v).start()

    def phase_d(s):
        def scope(lhs, pst, ost, tb):
            first = s == 0

            def left_load(w, own, whole):
                d, slot_p, slot_o = chip_of(w)
                src = ho.at[2 * d + (core if own else other)]
                dst = lhs.at[slot_o if own else slot_p]
                if not whole:
                    src, dst = src.at[:, pl.ds(ff, attn)], dst.at[:, pl.ds(ff, attn)]
                return pltpu.make_async_copy(src, dst, d_sem.at[w, own])

            def left_start(w):
                for own in range(2):
                    @pl.when(first)
                    def _():
                        left_load(w, own, True).start()

                    @pl.when(s > 0)
                    def _():
                        left_load(w, own, False).start()

            def left_wait(w):
                for own in range(2):
                    @pl.when(first)
                    def _():
                        left_load(w, own, True).wait()

                    @pl.when(s > 0)
                    def _():
                        left_load(w, own, False).wait()

            def hide(v):
                _, slot_p, slot_o = chip_of(v // 2)
                at = pl.multiple_of((v % 2) * half, half)
                wide = 512
                for c in range(0, ff, wide):
                    r = gelu(jnp.dot(nbuf[place_of(v)], wup[:, c:c + wide], preferred_element_type=f32))
                    for k in range(2):
                        own = 1 - (k + core) % 2
                        slot = slot_p + own * (slot_o - slot_p)
                        lhs[slot, pl.ds(at, half), c:c + wide] = r[k * half:(k + 1) * half]

            def swap(b, t, c):
                n = 2 * t + c
                return remote(pst.at[n], pbuf.at[s, b, n], p_s.at[n], p_r.at[s, b * NJ + n], partner)

            def pb_at(t, c):
                return nbuf.at[1, :, cols(2 * t + c)]

            def pb_load(b, t, c):
                return pltpu.make_async_copy(pbuf.at[s, b, 2 * t + c], pb_at(t, c), pb_sem.at[2 * t + c])

            def pb_start(b, t):
                for c in range(2):
                    with jax.named_scope("swap_wait"):
                        swap(b, t, c).wait_recv()
                    pb_load(b, t, c).start()

            def t_load(t, c):
                return pltpu.make_async_copy(tin.at[s, :, cols(2 * c + t)], tb.at[c], f_sem.at[c])

            def stored(t):
                for c in range(2):
                    pltpu.make_async_copy(ost.at[2 * t + c], pout.at[s, 0, :, cols(2 * c + t)],
                                          os_sem.at[2 * t + c]).wait()

            def post(b, t):
                stored(t)

                @pl.when(b == 0)
                def _():
                    transit(s, t, right).start()
                    transit(s, 2 + t, left).start()

                @pl.when(b == 1)
                def _():
                    to_left(s, 1, t).start()
                    to_right(s, 1, 2 + t).start()

                @pl.when(b == 2)
                def _():
                    to_right(s, 2, t).start()
                    to_left(s, 2, 2 + t).start()

            def partner_step(b, t):
                @pl.when(b >= 1)
                def _():
                    for c in range(2):
                        swap(b - 1, t, c).wait_send()

                @pl.when(jnp.logical_and(b == 2, t == 0))
                def _():
                    pb_start(1, 0)
                for c in range(2):
                    slot_p, _ = block(b, c)
                    r = jnp.dot(lhs[slot_p], wdo[:, cols(2 * c + t)], preferred_element_type=f32)
                    pst[2 * t + c] = r.astype(bf16)
                for c in range(2):
                    swap(b, t, c).start()

                @pl.when(jnp.logical_and(b == 2, t == 1))
                def _():
                    post(1, 0)

            def own_step(b, t):
                @pl.when(jnp.logical_and(b == 3, t == 0))
                def _():
                    pb_start(3, 0)

                @pl.when(t == 0)
                def _():
                    pb_start(b, 1)

                @pl.when(jnp.logical_and(b == 1, t == 1))
                def _():
                    pb_start(2, 0)

                @pl.when(b == 2)
                def _():
                    with jax.named_scope("transit_wait"):
                        for c in range(2):
                            transit(s, 2 * c + t, right).wait_recv()
                    for c in range(2):
                        t_load(t, c).start()
                for c in range(2):
                    pb_load(b, t, c).wait()
                for c in range(2):
                    _, slot_o = block(b, c)
                    r = jnp.dot(lhs[slot_o], wdo[:, cols(2 * c + t)], preferred_element_type=f32)
                    ost[2 * t + c] = (r + pb_at(t, c)[...].astype(f32)).astype(bf16)

                @pl.when(b == 2)
                def _():
                    step = 64
                    for c in range(2):
                        t_load(t, c).wait()

                        @pl.loop(0, rows // step)
                        def _(r):
                            at = pl.ds(pl.multiple_of(r * step, step), step)
                            ost[2 * t + c, at, :] = (ost[2 * t + c, at, :].astype(f32)
                                                     + tb[c, at, :].astype(f32)).astype(bf16)

                for c in range(2):
                    @pl.when(b < 3)
                    def _():
                        pltpu.make_async_copy(ost.at[2 * t + c], pout.at[s, b, :, cols(2 * c + t)],
                                              os_sem.at[2 * t + c]).start()

                    @pl.when(b == 3)
                    def _():
                        pltpu.make_async_copy(ost.at[2 * t + c], own_out.at[s, :, cols(2 * c + t)],
                                              os_sem.at[2 * t + c]).start()

                @pl.when(jnp.logical_and(b == 2, t == 0))
                def _():
                    post(1, 1)

                @pl.when(jnp.logical_and(t == 1, b % 2 == 0))
                def _():
                    post(b, 0)

            left_start(0)
            left_start(1)

            @pl.when(first)
            def _():
                w_copies[1].wait()
                w_copies[2].wait()

            n_groups = 7

            def since(g, k):
                return (g + 8 - k) // 8

            def units(g):
                return 2 * since(g, 1) + since(g, 2) + 3 * since(g, 3) + 2 * since(g, 6)

            @pl.loop(0, n_groups)
            def _(g):
                @pl.when(g == 0)
                def _():
                    left_wait(0)

                @pl.when(g == 1)
                def _():
                    pb_start(0, 0)

                @pl.when(g == 2)
                def _():
                    left_start(2)

                @pl.when(g == 4)
                def _():
                    left_start(3)

                @pl.when(s > 0)
                def _():
                    @pl.loop(units(g), units(g + 1))
                    def _(v):
                        with jax.named_scope("n_wait"):
                            rows_load(s, v).wait()

                        @pl.when(jnp.logical_and(v % 3 != 2, v < 2 * n_chips - 1))
                        def _():
                            rows_start(s, v + 1)

                        @pl.when(jnp.logical_and(v == 2 * n_chips - 1, s < batch - 1))
                        def _():
                            first_start(s + 1)
                        with jax.named_scope("hide"):
                            hide(v)

                        @pl.when(v % 3 == 2)
                        def _():
                            rows_start(s, v + 1)

                        @pl.when(v == 3)
                        def _():
                            post(0, 1)

                        @pl.when(v == 6)
                        def _():
                            post(2, 1)

                @pl.when(g == 2)
                def _():
                    left_wait(1)
                    left_wait(2)

                @pl.when(g == 5)
                def _():
                    left_wait(3)

                @pl.when(first)
                def _():
                    @pl.when(g == 2)
                    def _():
                        post(0, 1)

                    @pl.when(g == 5)
                    def _():
                        post(2, 1)

                    @pl.when(g == 6)
                    def _():
                        first_start(s + 1)

                @pl.loop(0, 2)
                def _(t):
                    @pl.when(jnp.logical_or(jnp.logical_or(g == 0, g == 2), jnp.logical_or(g == 3, g == 5)))
                    def _():
                        with jax.named_scope("partner"):
                            partner_step(since(g, 2) + since(g, 3) + since(g, 5), t)

                    @pl.when(jnp.logical_or(jnp.logical_or(g == 1, g == 3), jnp.logical_or(g == 4, g == 6)))
                    def _():
                        with jax.named_scope("own"):
                            own_step(since(g, 3) + since(g, 4) + since(g, 6), t)

                @pl.when(jnp.logical_and(s < batch - 1, g == 2))
                def _():
                    forward(s + 1, (2, 3))

                @pl.when(jnp.logical_and(s < batch - 1, g == 4))
                def _():
                    forward(s + 1, (4, 5))

            stored(0)
            stored(1)
            for t in range(2):
                for c in range(2):
                    swap(3, t, c).wait_send()

            @pl.when(s < batch - 2)
            def _():
                ag_start(s + 2)
        pl.run_scoped(scope, pltpu.VMEM((4, rows, ff + attn), bf16), pltpu.VMEM((NJ, rows, ncol), bf16),
                      pltpu.VMEM((NJ, rows, ncol), bf16), pltpu.VMEM((2, rows, ncol), bf16))

    def opening(raw, wide):
        kinds = qkv_cols // attn
        per = qkv_cols // 128
        slots, part_rows = raw.shape[0], raw.shape[1]
        n_parts = dim * per // part_rows
        chunk = wide.shape[0] // per
        chunks = part_rows // (chunk * per)
        xbuf = nbuf.at[1]

        def load(q):
            at = pl.ds(pl.multiple_of(q * part_rows, part_rows), part_rows)
            return pltpu.make_async_copy(wqkv_hbm.at[at], raw.at[q % slots], o_sem.at[q])

        x_start(0, xbuf)
        for q in range(slots):
            load(q).start()
        w_copies[0].start()
        for cp in v_copies:
            cp.wait()
        with jax.named_scope("send0"):
            normalise(0, xbuf, 0)
            normalise(0, xbuf, 1)
            send_first(0, xbuf)
            normalise(0, xbuf, 2)
            normalise(0, xbuf, 3)
            send_rest(0, xbuf)
        with jax.named_scope("place"):
            @pl.loop(0, n_parts)
            def _(q):
                load(q).wait()

                @pl.loop(0, chunks)
                def _(i):
                    at = pl.ds(pl.multiple_of(i * (chunk * per), chunk * per), chunk * per)
                    wide[...] = raw[q % slots, at, :].astype(f32)
                    to = pl.ds(pl.multiple_of((q * chunks + i) * chunk, chunk), chunk)
                    for j in range(kinds):
                        for c in range(head // 128):
                            for g in range(n_heads):
                                row = (j * (head // 128) + c) * n_heads + g
                                col = j * attn + g * head + c * 128
                                wqkv[to, col:col + 128] = wide[pl.ds(row, chunk, stride=per), :].astype(bf16)

                @pl.when(q + slots < n_parts)
                def _():
                    load(q + slots).start()

    pl.run_scoped(opening, pltpu.VMEM((6, dim * (qkv_cols // 128) // 8, 128), bf16),
                  pltpu.VMEM((128 * (qkv_cols // 128), 128), f32))

    @pl.loop(0, batch)
    def _(s):
        def scope(qkv):
            with jax.named_scope("A"):
                phase_a(s, qkv)

            @pl.when(s > 0)
            def _():
                rows_start(s, 0)
            with jax.named_scope("B"):
                phase_b(qkv)
        pl.run_scoped(scope, pltpu.VMEM((seq, qkv_cols), bf16))
        with jax.named_scope("D"):
            phase_d(s)

    @pl.loop(0, batch)
    def _(s):
        with jax.named_scope("final"):
            for j in range(NJ):
                to_right(s, 2, j).wait_recv()
                to_left(s, 2, j).wait_recv()
                to_right(s, 2, j).wait_send()
                to_left(s, 2, j).wait_send()
                transit(s, j, right).wait_send()
            for u in range(2 * n_chips):
                d, hf = unit(u)
                d2d_copy(s, u, d, hf, core).wait_send()
                if u >= 2:
                    ici_copy(s, u, d, hf, right).wait_send()


def layer_call(x_blk, ln_gain, ln_bias, wqkv, w_out, w_up, w_down, n_tp):
    batch, rows, dim = x_blk.shape
    ff, attn, qkv_cols = w_up.shape[1], w_out.shape[0], wqkv.shape[0] * 128 // dim
    n_chips = n_tp // 2
    ncol = dim // NJ
    bf16 = jnp.bfloat16
    dma = pltpu.SemaphoreType.DMA
    flops = 2 * batch * n_tp * rows * dim * (qkv_cols + 2 * ff + attn)
    outs = pl.pallas_call(
        layer_kernel,
        name="parallel_layer",
        out_shape=[
            jax.ShapeDtypeStruct((batch, rows, dim), bf16),
            jax.ShapeDtypeStruct((batch, rows, dim), bf16),
            jax.ShapeDtypeStruct((batch, rows, dim), bf16),
            jax.ShapeDtypeStruct((batch, n_chips, 2, rows, dim), bf16),
            jax.ShapeDtypeStruct((n_tp, rows, ff + attn), bf16),
            jax.ShapeDtypeStruct((batch, 4, NJ, rows, ncol), bf16),
            jax.ShapeDtypeStruct((batch, 3, rows, dim), bf16),
            jax.ShapeDtypeStruct((batch, rows, dim), bf16),
        ],
        in_specs=[pl.BlockSpec(memory_space=pl.ANY)] * 7,
        out_specs=[pl.BlockSpec(memory_space=pl.ANY)] * 8,
        scratch_shapes=[
            pltpu.VMEM((dim, qkv_cols), bf16), pltpu.VMEM((dim, ff), bf16), pltpu.VMEM((ff + attn, dim), bf16),
            pltpu.VMEM((1, dim), jnp.float32), pltpu.VMEM((1, dim), jnp.float32), pltpu.VMEM((2, rows, dim), bf16),
            dma((batch, 8)), dma((batch, 8)), dma((batch, 8)), dma((batch, 8)),
            dma((NJ,)), dma((batch, 4 * NJ)), dma((batch, NJ)), dma((batch, NJ)),
            dma((batch, 2 * NJ)), dma((batch, 2 * NJ)),
            dma((3,)), dma((2,)), dma((2, 4)), dma((2,)), dma((2,)), dma((n_tp,)), dma((4, 2)), dma((NJ,)), dma((NJ,)),
            dma((2,)),
        ],
        compiler_params=pltpu.CompilerParams(
            collective_id=0, has_side_effects=True, vmem_limit_bytes=67043328),
        cost_estimate=pl.CostEstimate(flops=flops, bytes_accessed=256 << 20, transcendentals=0),
    )(x_blk, ln_gain.reshape(1, dim), ln_bias.reshape(1, dim), wqkv, w_out, w_up, w_down)
    return outs[:3]


def solution(mesh):
    n_tp = mesh.shape["tp"]

    def local_layer(x_blk, ln_gain, ln_bias, w_qkv, w_out, w_up, w_down):
        dim = x_blk.shape[2]
        groups, kinds, head = w_qkv.shape[1:]
        wqkv = w_qkv.reshape(dim, groups, kinds, head // 128, 128).transpose(0, 2, 3, 1, 4).reshape(-1, 128)
        own, from_left, from_right = layer_call(x_blk, ln_gain, ln_bias, wqkv, w_out, w_up, w_down, n_tp)
        branch = (own.astype(jnp.float32) + from_left.astype(jnp.float32)
                  + from_right.astype(jnp.float32)).astype(jnp.bfloat16)
        return (x_blk.astype(jnp.float32) + branch.astype(jnp.float32)).astype(jnp.bfloat16)

    return jax.shard_map(
        local_layer, mesh=mesh,
        in_specs=(P("dp", "tp", None), P(), P(), P(None, "tp", None, None),
                  P("tp", None), P(None, "tp"), P("tp", None)),
        out_specs=P("dp", "tp", None), check_vma=False)
```

```python
import functools

import jax
import jax.numpy as jnp
from jax import lax
from jax.experimental import pallas as pl
from jax.experimental.pallas import tpu as pltpu
from jax.sharding import PartitionSpec as P

LN_EPS = 1e-5
LOG2_E = 1.4426950408889634
BOTH = (0, 1)
N_IN, N_OUT, LANES = 7, 8, 128
PARTNER_GROUPS, OWN_GROUPS = (0, 2, 3, 5), (1, 3, 4, 6)
NJ = 4


def any_of(value, choices):
    return functools.reduce(jnp.logical_or, [value == c for c in choices])


def layer_kernel(x_ref, gain_ref, bias_ref, wqkv_hbm, wout_hbm, wup_hbm, wdown_hbm,
                 own_out, left_out, right_out, n_all, ho, pbuf, pout, tin,
                 wqkv, wup, wdo, gain, bias, nbuf,
                 ag_is, ag_ir, ag_ds, ag_dr, p_s, p_r, t_s, t_r, m_s, m_r,
                 w_sem, v_sem, ln_sem, a_sem, h_sem, o_sem, d_sem, pb_sem, os_sem, f_sem):
    batch, rows, dim = x_ref.shape
    half = rows // 2
    ff = wup.shape[1]
    attn = wdo.shape[0] - ff
    qkv_cols = wqkv.shape[1]
    n_heads = 2
    head = attn // n_heads
    n_chips = n_all.shape[1]
    seq = n_chips * 2 * rows
    ncol = dim // NJ
    f32, bf16 = jnp.float32, jnp.bfloat16

    me = lax.axis_index("tp")
    chip, core = me // 2, me % 2
    other = 1 - core
    partner = chip * 2 + other
    right = ((chip + 1) % n_chips) * 2 + core
    left = ((chip + n_chips - 1) % n_chips) * 2 + core

    def remote(src, dst, send, recv, dev):
        return pltpu.make_async_remote_copy(
            src_ref=src, dst_ref=dst, send_sem=send, recv_sem=recv,
            device_id={"tp": dev}, device_id_type=pl.DeviceIdType.MESH)

    barrier = pltpu.get_barrier_semaphore()
    for dev in (partner, right, left):
        pl.semaphore_signal(barrier, inc=1, device_id={"tp": dev}, device_id_type=pl.DeviceIdType.MESH)
    pl.semaphore_wait(barrier, 3)

    w_copies = (
        pltpu.make_async_copy(wup_hbm, wup, w_sem.at[0]),
        pltpu.make_async_copy(wdown_hbm, wdo.at[pl.ds(0, ff)], w_sem.at[1]),
        pltpu.make_async_copy(wout_hbm, wdo.at[pl.ds(ff, attn)], w_sem.at[2]),
    )
    v_copies = (pltpu.make_async_copy(gain_ref, gain, v_sem.at[0]),
                pltpu.make_async_copy(bias_ref, bias, v_sem.at[1]))
    for cp in v_copies:
        cp.start()

    def unit(u):
        g, b = u // 2, u % 2
        near = (g * (3 - g)) // 2
        off = near * (2 * b - 1) + 2 * (g // 3)
        hf = (b + near * (g - 1)) % 2
        return (chip + off + n_chips) % n_chips, hf

    def piece(s, d, hf, k):
        return n_all.at[s, d, hf, pl.ds(pl.multiple_of(k * half, half), half)]

    def ici_copy(s, u, d, hf, dev):
        return remote(piece(s, d, hf, core), piece(s, d, hf, core), ag_is.at[s, u], ag_ir.at[s, u], dev)

    def d2d_copy(s, u, d, hf, k):
        return remote(piece(s, d, hf, k), piece(s, d, hf, k), ag_ds.at[s, u], ag_dr.at[s, u], partner)

    part = rows // 4

    def x_load(s, buf, q):
        at = pl.ds(q * part, part)
        return pltpu.make_async_copy(x_ref.at[s, at], buf.at[at], ln_sem.at[0, q])

    def n_store(s, buf, q):
        dst = n_all.at[s, chip, q // 2, pl.ds(pl.multiple_of(core * half + (q % 2) * part, part), part)]
        return pltpu.make_async_copy(buf.at[pl.ds(q * part, part)], dst, ln_sem.at[1, q])

    def x_start(s, buf):
        for q in range(4):
            x_load(s, buf, q).start()

    def normalise(s, buf, q):
        x_load(s, buf, q).wait()
        at = pl.ds(q * part, part)
        lanes, wide = LANES, 512
        total = jnp.zeros((part, lanes), f32)
        for c in range(0, dim, wide):
            v = buf[at, c:c + wide].astype(f32)
            for k in range(0, wide, lanes):
                total = total + v[:, k:k + lanes]
        mean = jnp.sum(total, axis=-1, keepdims=True) * (1.0 / dim)
        total = jnp.zeros((part, lanes), f32)
        for c in range(0, dim, wide):
            cen = buf[at, c:c + wide].astype(f32) - mean
            for k in range(0, wide, lanes):
                total = total + cen[:, k:k + lanes] * cen[:, k:k + lanes]
        inv = lax.rsqrt(jnp.sum(total, axis=-1, keepdims=True) * (1.0 / dim) + LN_EPS)
        for c in range(0, dim, wide):
            cen = buf[at, c:c + wide].astype(f32) - mean
            buf[at, c:c + wide] = (cen * inv * gain[:, c:c + wide] + bias[:, c:c + wide]).astype(bf16)
        n_store(s, buf, q).start()

    def ag_first(s):
        ici_copy(s, 2, chip, 0, right).start()
        ici_copy(s, 3, chip, 1, left).start()
        d2d_copy(s, 0, chip, 0, core).start()
        d2d_copy(s, 1, chip, 1, core).start()

    def ag_second(s):
        ici_copy(s, 4, chip, 1, right).start()
        ici_copy(s, 5, chip, 0, left).start()

    def forward(s, us):
        for u in us:
            d, hf = unit(u)
            with jax.named_scope(f"ici_wait_{u}"):
                ici_copy(s, u, d, hf, right).wait_recv()
            if u == 2:
                ici_copy(s, 6, d, hf, right).start()
            if u == 3:
                ici_copy(s, 7, d, hf, left).start()
            d2d_copy(s, u, d, hf, core).start()

    def block(b, second):
        near = (b * (3 - b)) // 2
        plus = (near * (1 + (2 * second - 1) * (3 - 2 * b))) // 2
        return 2 * plus, 1 + 2 * plus + b // 3

    def cols(j):
        return pl.ds(pl.multiple_of(j * ncol, ncol), ncol)

    def to_right(s, ii, j):
        return remote(pout.at[s, ii, :, cols(j)], left_out.at[s, :, cols(j)], m_s.at[s, j], m_r.at[s, j], right)

    def to_left(s, ii, j):
        return remote(pout.at[s, ii, :, cols(j)], right_out.at[s, :, cols(j)], m_s.at[s, NJ + j], m_r.at[s, NJ + j],
                      left)

    def transit(s, j, dev):
        return remote(pout.at[s, 0, :, cols(j)], tin.at[s, :, cols(j)], t_s.at[s, j], t_r.at[s, j], dev)

    def first_load(s):
        return pltpu.make_async_copy(n_all.at[s, chip, 0], nbuf.at[0], a_sem.at[0])

    def first_start(s):
        with jax.named_scope("d2d_wait"):
            d2d_copy(s, 0, chip, 0, other).wait_recv()
        first_load(s).start()

    def gelu(h):
        return (0.5 * h * (1.0 + lax.erf(h * (2.0 ** -0.5)))).astype(bf16)

    def phase_a(s, qkv):
        def scope(hbuf):
            first, later = s == 0, s > 0

            def load(u):
                d, hf = unit(u)
                return pltpu.make_async_copy(n_all.at[s, d, hf], nbuf.at[u % 2], a_sem.at[u % 2])

            def arrived(u):
                d, hf = unit(u)
                with jax.named_scope("d2d_wait"):
                    d2d_copy(s, u, d, hf, other).wait_recv()

            def hstore(u, k):
                d, hf = unit(u)
                return pltpu.make_async_copy(
                    hbuf.at[pl.ds(k * half, half)],
                    ho.at[2 * d + k, pl.ds(pl.multiple_of(hf * half, half), half), pl.ds(0, ff)],
                    h_sem.at[k])

            def project(u):
                d, hf = unit(u)
                wide = 512
                for c in range(0, qkv_cols, wide):
                    r = jnp.dot(nbuf[u % 2], wqkv[:, c:c + wide], preferred_element_type=f32).astype(bf16)
                    for k in BOTH:
                        pos = pl.multiple_of(d * (2 * rows) + k * rows + hf * half, half)
                        qkv[pl.ds(pos, half), c:c + wide] = r[k * half:(k + 1) * half]

            @pl.when(first)
            def _():
                first_start(s)

            @pl.loop(0, 2 * n_chips)
            def _(u):
                odd = u % 2 == 1
                with jax.named_scope("load_wait"):
                    load(u).wait()

                @pl.when(jnp.logical_and(later, u == 4))
                def _():
                    forward(s, (6, 7))

                @pl.when(jnp.logical_or(jnp.logical_and(later, u < 7), u % 2 == 0))
                def _():
                    arrived(u + 1)
                    load(u + 1).start()

                @pl.when(later)
                def _():
                    project(u)

                @pl.when(first)
                def _():
                    @pl.when(jnp.logical_and(odd, u < 7))
                    def _():
                        x_start((u + 1) // 2, nbuf.at[0])

                    @pl.when(u == 0)
                    def _():
                        w_copies[0].wait()
                        for cp in w_copies[1:]:
                            cp.start()
                    project(u)

                    @pl.when(u >= 1)
                    def _():
                        for k in BOTH:
                            hstore(u - 1, k).wait()
                    hbuf[...] = gelu(jnp.dot(nbuf[u % 2], wup[...], preferred_element_type=f32))
                    for k in BOTH:
                        hstore(u, k).start()

                    @pl.when(u == 1)
                    def _():
                        forward(0, (2, 3))

                    @pl.when(u == 3)
                    def _():
                        forward(0, (4, 5))

                    @pl.when(u == 5)
                    def _():
                        forward(0, (6, 7))

                    @pl.when(jnp.logical_and(odd, u < 7))
                    def _():
                        with jax.named_scope("norm"):
                            for q in range(4):
                                normalise((u + 1) // 2, nbuf.at[0], q)
                            for q in range(4):
                                n_store((u + 1) // 2, nbuf.at[0], q).wait()

                        @pl.when(u == 1)
                        def _():
                            ag_first(1)
                            ag_second(1)
                        arrived(u + 1)
                        load(u + 1).start()

            @pl.when(first)
            def _():
                for k in BOTH:
                    hstore(7, k).wait()
        pl.run_scoped(scope, pltpu.VMEM((rows, ff), bf16))

    def phase_b(qkv):
        def ostore(t):
            return pltpu.make_async_copy(qkv.at[pl.ds(t * rows, rows), pl.ds(0, attn)],
                                         ho.at[t, :, pl.ds(ff, attn)], o_sem.at[t])
        scale = head ** -0.5

        probs = nbuf.at[1]

        def scope(*scores):
            keep = (lax.broadcasted_iota(jnp.int32, (rows, rows), 0)
                    >= lax.broadcasted_iota(jnp.int32, (rows, rows), 1))
            tasks = [(t, h) for t in range(seq // rows) for h in range(n_heads)]
            tops = {}

            def score(i):
                t, h = tasks[i]
                r0, n = t * rows, (t + 1) * rows
                q = qkv[r0:n, h * head:(h + 1) * head]
                k = qkv[0:n, attn + h * head:attn + (h + 1) * head]
                sc = lax.dot_general(q, k, (((1,), (1,)), ((), ())), preferred_element_type=f32)
                diag = jnp.where(keep, sc[:, r0:], -jnp.inf)
                top = jnp.max(diag, axis=1, keepdims=True)
                if t:
                    scores[i % 2][0, :, 0:r0] = sc[:, :r0]
                    top = jnp.maximum(top, jnp.max(sc[:, :r0], axis=1, keepdims=True))
                scores[i % 2][0, :, r0:n] = diag
                tops[i] = top

            def soften(i):
                t, h = tasks[i]
                n = (t + 1) * rows
                total = jnp.zeros((rows, rows // 2), f32)
                for c in range(0, n, rows):
                    e = jnp.exp2((scores[i % 2][0, :, c:c + rows] - tops[i]) * (scale * LOG2_E))
                    scores[i % 2][0, :, c:c + rows] = e
                    total = total + e[:, :rows // 2] + e[:, rows // 2:]
                inverse = 1.0 / jnp.sum(total, axis=1, keepdims=True)
                for c in range(0, n, rows):
                    probs[:, (i % 2) * seq + c:(i % 2) * seq + c + rows] = (
                        scores[i % 2][0, :, c:c + rows] * inverse).astype(bf16)

            def mix(i):
                t, h = tasks[i]
                r0, n = t * rows, (t + 1) * rows
                v = qkv[0:n, 2 * attn + h * head:2 * attn + (h + 1) * head]
                o = jnp.dot(probs[:, (i % 2) * seq:(i % 2) * seq + n], v, preferred_element_type=f32)
                qkv[r0:n, h * head:(h + 1) * head] = o.astype(bf16)

            score(0)
            for i in range(len(tasks)):
                if i + 1 < len(tasks):
                    score(i + 1)
                soften(i)
                mix(i)
                if i % n_heads == n_heads - 1:
                    ostore(tasks[i][0]).start()
            for t in range(seq // rows):
                ostore(t).wait()
        pl.run_scoped(scope, pltpu.VMEM((1, rows, seq), f32), pltpu.VMEM((1, rows, seq), f32))

    def chip_of(w):
        near = (w * (3 - w)) // 2
        off = near * (3 - 2 * w) + 2 * ((3 - w) // 3)
        plus = near * (2 - w)
        return (chip + off + n_chips) % n_chips, 2 * plus, 1 + 2 * plus + w // 3

    def place_of(v):
        return (v % 3) * (2 - v % 3)

    def rows_load(s, v):
        d, _, _ = chip_of(v // 2)
        return pltpu.make_async_copy(n_all.at[s, d, v % 2], nbuf.at[place_of(v)], a_sem.at[place_of(v)])

    def rows_start(s, v):
        rows_load(s, v).start()

    def phase_d(s):
        def scope(lhs, pst, ost, tb):
            first, later = s == 0, s > 0

            def left_load(w, own, whole):
                d, slot_p, slot_o = chip_of(w)
                src = ho.at[2 * d + (core if own else other)]
                dst = lhs.at[slot_o if own else slot_p]
                if not whole:
                    src, dst = src.at[:, pl.ds(ff, attn)], dst.at[:, pl.ds(ff, attn)]
                return pltpu.make_async_copy(src, dst, d_sem.at[w, own])

            def left_act(w, own, act):
                @pl.when(first)
                def _():
                    act(left_load(w, own, True))

                @pl.when(later)
                def _():
                    act(left_load(w, own, False))

            def left_start(w, own):
                left_act(w, own, lambda cp: cp.start())

            def left_wait(w, own):
                left_act(w, own, lambda cp: cp.wait())

            def hide(v):
                _, slot_p, slot_o = chip_of(v // 2)
                at = pl.multiple_of((v % 2) * half, half)
                wide = 512
                for c in range(0, ff, wide):
                    r = gelu(jnp.dot(nbuf[place_of(v)], wup[:, c:c + wide], preferred_element_type=f32))
                    for k in BOTH:
                        own = 1 - (k + core) % 2
                        slot = slot_p + own * (slot_o - slot_p)
                        lhs[slot, pl.ds(at, half), c:c + wide] = r[k * half:(k + 1) * half]

            def nth(i, k):
                return 2 * i + k

            def swap(b, t, c):
                n = nth(t, c)
                return remote(pst.at[n], pbuf.at[s, b, n], p_s.at[n], p_r.at[s, b * NJ + n], partner)

            def pb_at(t, c):
                return nbuf.at[1, :, cols(nth(t, c))]

            def pb_load(b, t, c):
                return pltpu.make_async_copy(pbuf.at[s, b, nth(t, c)], pb_at(t, c), pb_sem.at[nth(t, c)])

            def pb_start(b, t):
                for c in BOTH:
                    with jax.named_scope("swap_wait"):
                        swap(b, t, c).wait_recv()
                    pb_load(b, t, c).start()

            def t_load(t, c):
                return pltpu.make_async_copy(tin.at[s, :, cols(nth(c, t))], tb.at[c], f_sem.at[c])

            def stored(t):
                for c in BOTH:
                    pltpu.make_async_copy(ost.at[nth(t, c)], pout.at[s, 0, :, cols(nth(c, t))],
                                          os_sem.at[nth(t, c)]).wait()

            def post(b, t):
                stored(t)

                @pl.when(b == 0)
                def _():
                    transit(s, t, right).start()
                    transit(s, 2 + t, left).start()

                @pl.when(b == 1)
                def _():
                    to_left(s, 1, t).start()
                    to_right(s, 1, 2 + t).start()

                @pl.when(b == 2)
                def _():
                    to_right(s, 2, t).start()
                    to_left(s, 2, 2 + t).start()

            def partner_step(b, t):
                @pl.when(b >= 1)
                def _():
                    for c in BOTH:
                        swap(b - 1, t, c).wait_send()

                @pl.when(jnp.logical_and(b == 2, t == 0))
                def _():
                    pb_start(1, 0)
                for c in BOTH:
                    slot_p, _ = block(b, c)
                    r = jnp.dot(lhs[slot_p], wdo[:, cols(nth(c, t))], preferred_element_type=f32)
                    pst[nth(t, c)] = r.astype(bf16)
                for c in BOTH:
                    swap(b, t, c).start()

                @pl.when(jnp.logical_and(b == 2, t == 1))
                def _():
                    post(1, 0)

            def own_step(b, t):
                @pl.when(jnp.logical_and(b == 3, t == 0))
                def _():
                    pb_start(3, 0)

                @pl.when(t == 0)
                def _():
                    pb_start(b, 1)

                @pl.when(jnp.logical_and(b == 1, t == 1))
                def _():
                    pb_start(2, 0)

                @pl.when(b == 2)
                def _():
                    with jax.named_scope("transit_wait"):
                        for c in BOTH:
                            transit(s, nth(c, t), right).wait_recv()
                    for c in BOTH:
                        t_load(t, c).start()
                for c in BOTH:
                    pb_load(b, t, c).wait()
                for c in BOTH:
                    _, slot_o = block(b, c)
                    r = jnp.dot(lhs[slot_o], wdo[:, cols(nth(c, t))], preferred_element_type=f32)
                    ost[nth(t, c)] = (r + pb_at(t, c)[...].astype(f32)).astype(bf16)

                @pl.when(b == 2)
                def _():
                    step = 64
                    for c in BOTH:
                        t_load(t, c).wait()

                        @pl.loop(0, rows // step)
                        def _(r):
                            at = pl.ds(pl.multiple_of(r * step, step), step)
                            ost[nth(t, c), at, :] = (ost[nth(t, c), at, :].astype(f32)
                                                     + tb[c, at, :].astype(f32)).astype(bf16)

                for c in BOTH:
                    @pl.when(b < 3)
                    def _():
                        pltpu.make_async_copy(ost.at[nth(t, c)], pout.at[s, b, :, cols(nth(c, t))],
                                              os_sem.at[nth(t, c)]).start()

                    @pl.when(b == 3)
                    def _():
                        pltpu.make_async_copy(ost.at[nth(t, c)], own_out.at[s, :, cols(nth(c, t))],
                                              os_sem.at[nth(t, c)]).start()

                @pl.when(jnp.logical_and(b == 2, t == 0))
                def _():
                    post(1, 1)

                @pl.when(jnp.logical_and(t == 1, b % 2 == 0))
                def _():
                    post(b, 0)

            for w in BOTH:
                for own in BOTH:
                    left_start(w, own)

            @pl.when(first)
            def _():
                w_copies[1].wait()
                w_copies[2].wait()

            n_groups = 7

            def since(g, k):
                return (g + 8 - k) // 8

            def step_of(g, groups):
                return sum(since(g, k) for k in groups[1:])

            def units(g):
                return 2 * since(g, 1) + since(g, 2) + 3 * since(g, 3) + 2 * since(g, 6)

            @pl.loop(0, n_groups)
            def _(g):
                @pl.when(g == 0)
                def _():
                    left_wait(0, 0)

                @pl.when(g == 1)
                def _():
                    pb_start(0, 0)
                    left_start(2, 0)
                    left_wait(0, 1)

                @pl.when(g == 2)
                def _():
                    left_start(2, 1)

                @pl.when(g == 3)
                def _():
                    left_wait(1, 1)
                    left_wait(2, 1)

                @pl.when(g == 4)
                def _():
                    left_start(3, 0)
                    left_start(3, 1)

                @pl.when(later)
                def _():
                    @pl.loop(units(g), units(g + 1))
                    def _(v):
                        with jax.named_scope("n_wait"):
                            rows_load(s, v).wait()

                        @pl.when(jnp.logical_and(v % 3 != 2, v < 2 * n_chips - 1))
                        def _():
                            rows_start(s, v + 1)

                        @pl.when(jnp.logical_and(v == 2 * n_chips - 1, s < batch - 1))
                        def _():
                            first_start(s + 1)
                        with jax.named_scope("hide"):
                            hide(v)

                        @pl.when(v % 3 == 2)
                        def _():
                            rows_start(s, v + 1)

                        @pl.when(v == 3)
                        def _():
                            post(0, 1)

                        @pl.when(v == 6)
                        def _():
                            post(2, 1)

                @pl.when(g == 2)
                def _():
                    left_wait(1, 0)
                    left_wait(2, 0)

                @pl.when(g == 5)
                def _():
                    left_wait(3, 0)
                    left_wait(3, 1)

                @pl.when(first)
                def _():
                    @pl.when(g == 2)
                    def _():
                        post(0, 1)

                    @pl.when(g == 5)
                    def _():
                        post(2, 1)

                    @pl.when(g == 6)
                    def _():
                        first_start(s + 1)

                @pl.loop(0, 2)
                def _(t):
                    @pl.when(any_of(g, PARTNER_GROUPS))
                    def _():
                        with jax.named_scope("partner"):
                            partner_step(step_of(g, PARTNER_GROUPS), t)

                    @pl.when(any_of(g, OWN_GROUPS))
                    def _():
                        with jax.named_scope("own"):
                            own_step(step_of(g, OWN_GROUPS), t)

                @pl.when(jnp.logical_and(s < batch - 1, g == 2))
                def _():
                    @pl.when(later)
                    def _():
                        ag_second(s + 1)
                    forward(s + 1, (2, 3))

                @pl.when(jnp.logical_and(s < batch - 1, g == n_groups - 1))
                def _():
                    forward(s + 1, (4, 5))

            stored(0)
            stored(1)
            for t in BOTH:
                for c in BOTH:
                    swap(3, t, c).wait_send()

            @pl.when(s < batch - 2)
            def _():
                ag_first(s + 2)
        pl.run_scoped(scope, pltpu.VMEM((4, rows, ff + attn), bf16), pltpu.VMEM((NJ, rows, ncol), bf16),
                      pltpu.VMEM((NJ, rows, ncol), bf16), pltpu.VMEM((2, rows, ncol), bf16))

    def opening(raw, wide):
        kinds = qkv_cols // attn
        per = qkv_cols // LANES
        slots, part_rows = raw.shape[0], raw.shape[1]
        n_parts = dim * per // part_rows
        chunk = wide.shape[0] // per
        chunks = part_rows // (chunk * per)
        xbuf = nbuf.at[1]

        def load(q):
            at = pl.ds(pl.multiple_of(q * part_rows, part_rows), part_rows)
            return pltpu.make_async_copy(wqkv_hbm.at[at], raw.at[q % slots], o_sem.at[q])

        x_start(0, xbuf)
        for q in range(slots):
            load(q).start()
        w_copies[0].start()
        for cp in v_copies:
            cp.wait()
        with jax.named_scope("send0"):
            for q in range(4):
                normalise(0, xbuf, q)
                if q == 1:
                    n_store(0, xbuf, 0).wait()
                    n_store(0, xbuf, 1).wait()
                    ici_copy(0, 2, chip, 0, right).start()
                    d2d_copy(0, 0, chip, 0, core).start()
            n_store(0, xbuf, 2).wait()
            n_store(0, xbuf, 3).wait()
            ici_copy(0, 3, chip, 1, left).start()
            d2d_copy(0, 1, chip, 1, core).start()
            ag_second(0)
        with jax.named_scope("place"):
            @pl.loop(0, n_parts)
            def _(q):
                load(q).wait()

                @pl.loop(0, chunks)
                def _(i):
                    at = pl.ds(pl.multiple_of(i * (chunk * per), chunk * per), chunk * per)
                    wide[...] = raw[q % slots, at, :].astype(f32)
                    to = pl.ds(pl.multiple_of((q * chunks + i) * chunk, chunk), chunk)
                    for j in range(kinds):
                        for c in range(head // LANES):
                            for g in range(n_heads):
                                row = (j * (head // LANES) + c) * n_heads + g
                                col = j * attn + g * head + c * 128
                                wqkv[to, col:col + 128] = wide[pl.ds(row, chunk, stride=per), :].astype(bf16)

                @pl.when(q + slots < n_parts)
                def _():
                    load(q + slots).start()

    pl.run_scoped(opening, pltpu.VMEM((6, dim * (qkv_cols // LANES) // 8, 128), bf16),
                  pltpu.VMEM((128 * (qkv_cols // LANES), 128), f32))

    @pl.loop(0, batch)
    def _(s):
        def scope(qkv):
            with jax.named_scope("A"):
                phase_a(s, qkv)

            @pl.when(s > 0)
            def _():
                rows_start(s, 0)
            with jax.named_scope("B"):
                phase_b(qkv)
        pl.run_scoped(scope, pltpu.VMEM((seq, qkv_cols), bf16))
        with jax.named_scope("D"):
            phase_d(s)

    @pl.loop(0, batch)
    def _(s):
        with jax.named_scope("final"):
            for j in range(NJ):
                to_right(s, 2, j).wait_recv()
                to_left(s, 2, j).wait_recv()
                to_right(s, 2, j).wait_send()
                to_left(s, 2, j).wait_send()
                transit(s, j, right).wait_send()
            for u in range(2 * n_chips):
                d, hf = unit(u)
                d2d_copy(s, u, d, hf, core).wait_send()
                if u >= 2:
                    ici_copy(s, u, d, hf, right).wait_send()


def layer_call(x_blk, ln_gain, ln_bias, wqkv, w_out, w_up, w_down, n_tp):
    batch, rows, dim = x_blk.shape
    ff, attn, qkv_cols = w_up.shape[1], w_out.shape[0], wqkv.shape[0] * 128 // dim
    n_chips = n_tp // 2
    ncol = dim // NJ
    bf16 = jnp.bfloat16
    dma = pltpu.SemaphoreType.DMA
    flops = 2 * batch * n_tp * rows * dim * (qkv_cols + 2 * ff + attn)
    outs = pl.pallas_call(
        layer_kernel,
        name="parallel_layer",
        out_shape=[
            jax.ShapeDtypeStruct((batch, rows, dim), bf16),
            jax.ShapeDtypeStruct((batch, rows, dim), bf16),
            jax.ShapeDtypeStruct((batch, rows, dim), bf16),
            jax.ShapeDtypeStruct((batch, n_chips, 2, rows, dim), bf16),
            jax.ShapeDtypeStruct((n_tp, rows, ff + attn), bf16),
            jax.ShapeDtypeStruct((batch, 4, NJ, rows, ncol), bf16),
            jax.ShapeDtypeStruct((batch, 3, rows, dim), bf16),
            jax.ShapeDtypeStruct((batch, rows, dim), bf16),
        ],
        in_specs=[pl.BlockSpec(memory_space=pl.ANY)] * N_IN,
        out_specs=[pl.BlockSpec(memory_space=pl.ANY)] * N_OUT,
        scratch_shapes=[
            pltpu.VMEM((dim, qkv_cols), bf16), pltpu.VMEM((dim, ff), bf16), pltpu.VMEM((ff + attn, dim), bf16),
            pltpu.VMEM((1, dim), jnp.float32), pltpu.VMEM((1, dim), jnp.float32), pltpu.VMEM((2, rows, dim), bf16),
            dma((batch, 8)), dma((batch, 8)), dma((batch, 8)), dma((batch, 8)),
            dma((NJ,)), dma((batch, 4 * NJ)), dma((batch, NJ)), dma((batch, NJ)),
            dma((batch, 2 * NJ)), dma((batch, 2 * NJ)),
            dma((3,)), dma((2,)), dma((2, 4)), dma((2,)), dma((2,)), dma((n_tp,)), dma((4, 2)), dma((NJ,)), dma((NJ,)),
            dma((2,)),
        ],
        compiler_params=pltpu.CompilerParams(
            collective_id=0, has_side_effects=True, vmem_limit_bytes=67043328),
        cost_estimate=pl.CostEstimate(flops=flops, bytes_accessed=256 << 20, transcendentals=0),
    )(x_blk, ln_gain.reshape(1, dim), ln_bias.reshape(1, dim), wqkv, w_out, w_up, w_down)
    return outs[:3]


def solution(mesh):
    n_tp = mesh.shape["tp"]

    def local_layer(x_blk, ln_gain, ln_bias, w_qkv, w_out, w_up, w_down):
        dim = x_blk.shape[2]
        groups, kinds, head = w_qkv.shape[1:]
        wqkv = w_qkv.reshape(dim, groups, kinds, head // LANES, 128).transpose(0, 2, 3, 1, 4).reshape(-1, 128)
        own, from_left, from_right = layer_call(x_blk, ln_gain, ln_bias, wqkv, w_out, w_up, w_down, n_tp)
        branch = (own.astype(jnp.float32) + from_left.astype(jnp.float32)
                  + from_right.astype(jnp.float32)).astype(jnp.bfloat16)
        return (x_blk.astype(jnp.float32) + branch.astype(jnp.float32)).astype(jnp.bfloat16)

    return jax.shard_map(
        local_layer, mesh=mesh,
        in_specs=(P("dp", "tp", None), P(), P(), P(None, "tp", None, None),
                  P("tp", None), P(None, "tp"), P("tp", None)),
        out_specs=P("dp", "tp", None), check_vma=False)
```

```python
import functools

import jax
import jax.numpy as jnp
from jax import lax
from jax.experimental import pallas as pl
from jax.experimental.pallas import tpu as pltpu
from jax.sharding import PartitionSpec as P

LN_EPS = 1e-5
LOG2_E = 1.4426950408889634
BOTH, PARTS = (0, 1), 4
N_IN, N_OUT, LANES, WIDE = 7, 9, 128, 512
PARTNER_GROUPS, OWN_GROUPS = (0, 2, 3, 5), (1, 3, 4, 6)
NJ = 4


def any_of(value, choices):
    return functools.reduce(jnp.logical_or, [value == c for c in choices])


def layer_kernel(x_ref, gain_ref, bias_ref, wqkv_hbm, wout_hbm, wup_hbm, wdown_hbm,
                 y_ref, own_out, left_out, right_out, n_all, ho, pbuf, pout, tin,
                 wqkv, wup, wdo, gain, bias, nbuf,
                 ag_is, ag_ir, ag_ds, ag_dr, p_s, p_r, t_s, t_r, m_s, m_r,
                 w_sem, v_sem, ln_sem, a_sem, h_sem, o_sem, d_sem, pb_sem, os_sem, f_sem, y_sem, z_sem):
    batch, rows, dim = x_ref.shape
    half = rows // 2
    ff = wup.shape[1]
    attn = wdo.shape[0] - ff
    qkv_cols = wqkv.shape[1]
    n_heads = 2
    head = attn // n_heads
    n_chips = n_all.shape[1]
    seq = n_chips * 2 * rows
    ncol = dim // NJ
    f32, bf16 = jnp.float32, jnp.bfloat16

    me = lax.axis_index("tp")
    chip, core = me // 2, me % 2
    other = 1 - core
    partner = chip * 2 + other
    right = ((chip + 1) % n_chips) * 2 + core
    left = ((chip + n_chips - 1) % n_chips) * 2 + core

    def remote(src, dst, send, recv, dev):
        return pltpu.make_async_remote_copy(
            src_ref=src, dst_ref=dst, send_sem=send, recv_sem=recv,
            device_id={"tp": dev}, device_id_type=pl.DeviceIdType.MESH)

    barrier = pltpu.get_barrier_semaphore()
    for dev in (partner, right, left):
        pl.semaphore_signal(barrier, inc=1, device_id={"tp": dev}, device_id_type=pl.DeviceIdType.MESH)
    pl.semaphore_wait(barrier, 3)

    w_copies = (
        pltpu.make_async_copy(wup_hbm, wup, w_sem.at[0]),
        pltpu.make_async_copy(wdown_hbm, wdo.at[pl.ds(0, ff)], w_sem.at[1]),
        pltpu.make_async_copy(wout_hbm, wdo.at[pl.ds(ff, attn)], w_sem.at[2]),
    )
    v_copies = (pltpu.make_async_copy(gain_ref, gain, v_sem.at[0]),
                pltpu.make_async_copy(bias_ref, bias, v_sem.at[1]))
    for cp in v_copies:
        cp.start()

    def unit(u):
        g, b = u // 2, u % 2
        near = (g * (3 - g)) // 2
        off = near * (2 * b - 1) + 2 * (g // 3)
        hf = (b + near * (g - 1)) % 2
        return (chip + off + n_chips) % n_chips, hf

    def piece(s, d, hf, k):
        return n_all.at[s, d, hf, pl.ds(pl.multiple_of(k * half, half), half)]

    def ici_copy(s, u, d, hf, dev):
        return remote(piece(s, d, hf, core), piece(s, d, hf, core), ag_is.at[s, u], ag_ir.at[s, u], dev)

    def d2d_copy(s, u, d, hf, k):
        return remote(piece(s, d, hf, k), piece(s, d, hf, k), ag_ds.at[s, u], ag_dr.at[s, u], partner)

    part = rows // PARTS

    def x_load(s, buf, q):
        at = pl.ds(q * part, part)
        return pltpu.make_async_copy(x_ref.at[s, at], buf.at[at], ln_sem.at[0, q])

    def n_store(s, buf, q):
        dst = n_all.at[s, chip, q // 2, pl.ds(pl.multiple_of(core * half + (q % 2) * part, part), part)]
        return pltpu.make_async_copy(buf.at[pl.ds(q * part, part)], dst, ln_sem.at[1, q])

    def x_start(s, buf):
        for q in range(PARTS):
            x_load(s, buf, q).start()

    def normalise(s, buf, q):
        x_load(s, buf, q).wait()
        at = pl.ds(q * part, part)
        lanes, wide = LANES, WIDE
        total = jnp.zeros((part, lanes), f32)
        for c in range(0, dim, wide):
            v = buf[at, c:c + wide].astype(f32)
            for k in range(0, wide, lanes):
                total = total + v[:, k:k + lanes]
        mean = jnp.sum(total, axis=-1, keepdims=True) * (1.0 / dim)
        total = jnp.zeros((part, lanes), f32)
        for c in range(0, dim, wide):
            cen = buf[at, c:c + wide].astype(f32) - mean
            for k in range(0, wide, lanes):
                total = total + cen[:, k:k + lanes] * cen[:, k:k + lanes]
        inv = lax.rsqrt(jnp.sum(total, axis=-1, keepdims=True) * (1.0 / dim) + LN_EPS)
        for c in range(0, dim, wide):
            cen = buf[at, c:c + wide].astype(f32) - mean
            buf[at, c:c + wide] = (cen * inv * gain[:, c:c + wide] + bias[:, c:c + wide]).astype(bf16)
        n_store(s, buf, q).start()

    def ag_first(s):
        ici_copy(s, 2, chip, 0, right).start()
        ici_copy(s, 3, chip, 1, left).start()
        d2d_copy(s, 0, chip, 0, core).start()
        d2d_copy(s, 1, chip, 1, core).start()

    def ag_second(s):
        ici_copy(s, 4, chip, 1, right).start()
        ici_copy(s, 5, chip, 0, left).start()

    def forward(s, us):
        for u in us:
            d, hf = unit(u)
            with jax.named_scope(f"ici_wait_{u}"):
                ici_copy(s, u, d, hf, right).wait_recv()
            if u == 2:
                ici_copy(s, 6, d, hf, right).start()
            if u == 3:
                ici_copy(s, 7, d, hf, left).start()
            d2d_copy(s, u, d, hf, core).start()

    def block(b, second):
        near = (b * (3 - b)) // 2
        plus = (near * (1 + (2 * second - 1) * (3 - 2 * b))) // 2
        return 2 * plus, 1 + 2 * plus + b // 3

    def cols(j):
        return pl.ds(pl.multiple_of(j * ncol, ncol), ncol)

    def to_right(s, ii, j):
        return remote(pout.at[s, ii, :, cols(j)], left_out.at[s, :, cols(j)], m_s.at[s, j], m_r.at[s, j], right)

    def to_left(s, ii, j):
        return remote(pout.at[s, ii, :, cols(j)], right_out.at[s, :, cols(j)], m_s.at[s, NJ + j], m_r.at[s, NJ + j],
                      left)

    def transit(s, j, dev):
        return remote(pout.at[s, 0, :, cols(j)], tin.at[s, :, cols(j)], t_s.at[s, j], t_r.at[s, j], dev)

    def first_load(s):
        return pltpu.make_async_copy(n_all.at[s, chip, 0], nbuf.at[0], a_sem.at[0])

    def first_start(s):
        with jax.named_scope("d2d_wait"):
            d2d_copy(s, 0, chip, 0, other).wait_recv()
        first_load(s).start()

    def gelu(h):
        return (0.5 * h * (1.0 + lax.erf(h * (2.0 ** -0.5)))).astype(bf16)

    def phase_a(s, qkv):
        def scope(hbuf):
            first, later = s == 0, s > 0

            def load(u):
                d, hf = unit(u)
                return pltpu.make_async_copy(n_all.at[s, d, hf], nbuf.at[u % 2], a_sem.at[u % 2])

            def arrived(u):
                d, hf = unit(u)
                with jax.named_scope("d2d_wait"):
                    d2d_copy(s, u, d, hf, other).wait_recv()

            def hstore(u, k):
                d, hf = unit(u)
                return pltpu.make_async_copy(
                    hbuf.at[pl.ds(k * half, half)],
                    ho.at[2 * d + k, pl.ds(pl.multiple_of(hf * half, half), half), pl.ds(0, ff)],
                    h_sem.at[k])

            def project(u):
                d, hf = unit(u)
                wide = WIDE
                for c in range(0, qkv_cols, wide):
                    r = jnp.dot(nbuf[u % 2], wqkv[:, c:c + wide], preferred_element_type=f32).astype(bf16)
                    for k in BOTH:
                        pos = pl.multiple_of(d * (2 * rows) + k * rows + hf * half, half)
                        qkv[pl.ds(pos, half), c:c + wide] = r[k * half:(k + 1) * half]

            @pl.loop(0, 2 * n_chips)
            def _(u):
                odd = u % 2 == 1
                with jax.named_scope("load_wait"):
                    load(u).wait()

                @pl.when(jnp.logical_and(later, u == 4))
                def _():
                    forward(s, (6, 7))

                @pl.when(jnp.logical_or(jnp.logical_and(later, u < 7), u % 2 == 0))
                def _():
                    arrived(u + 1)
                    load(u + 1).start()

                @pl.when(later)
                def _():
                    project(u)

                @pl.when(first)
                def _():
                    @pl.when(jnp.logical_and(odd, u < 7))
                    def _():
                        x_start((u + 1) // 2, nbuf.at[0])

                    project(u)

                    @pl.when(u == 0)
                    def _():
                        w_copies[0].wait()
                        for cp in w_copies[1:]:
                            cp.start()

                    @pl.when(u >= 1)
                    def _():
                        for k in BOTH:
                            hstore(u - 1, k).wait()
                    hbuf[...] = gelu(jnp.dot(nbuf[u % 2], wup[...], preferred_element_type=f32))
                    for k in BOTH:
                        hstore(u, k).start()

                    @pl.when(u == 1)
                    def _():
                        forward(0, (2, 3))

                    @pl.when(u == 3)
                    def _():
                        forward(0, (4, 5))

                    @pl.when(u == 5)
                    def _():
                        forward(0, (6, 7))

                    @pl.when(jnp.logical_and(odd, u < 7))
                    def _():
                        with jax.named_scope("norm"):
                            for q in range(PARTS):
                                normalise((u + 1) // 2, nbuf.at[0], q)
                            for q in range(PARTS):
                                n_store((u + 1) // 2, nbuf.at[0], q).wait()

                        @pl.when(u == 1)
                        def _():
                            ag_first(1)
                            ag_second(1)
                        arrived(u + 1)
                        load(u + 1).start()

            @pl.when(first)
            def _():
                for k in BOTH:
                    hstore(7, k).wait()
        pl.run_scoped(scope, pltpu.VMEM((rows, ff), bf16))

    def phase_b(qkv):
        def ostore(t):
            return pltpu.make_async_copy(qkv.at[pl.ds(t * rows, rows), pl.ds(0, attn)],
                                         ho.at[t, :, pl.ds(ff, attn)], o_sem.at[t])
        scale = head ** -0.5

        probs = nbuf.at[1]

        def scope(*scores):
            keep = (lax.broadcasted_iota(jnp.int32, (rows, rows), 0)
                    >= lax.broadcasted_iota(jnp.int32, (rows, rows), 1))
            tasks = [(t, h) for t in range(seq // rows) for h in range(n_heads)]
            tops = {}

            def score(i):
                t, h = tasks[i]
                r0, n = t * rows, (t + 1) * rows
                q = qkv[r0:n, h * head:(h + 1) * head]
                k = qkv[0:n, attn + h * head:attn + (h + 1) * head]
                sc = lax.dot_general(q, k, (((1,), (1,)), ((), ())), preferred_element_type=f32)
                diag = jnp.where(keep, sc[:, r0:], -jnp.inf)
                top = jnp.max(diag, axis=1, keepdims=True)
                if t:
                    scores[i % 2][0, :, 0:r0] = sc[:, :r0]
                    top = jnp.maximum(top, jnp.max(sc[:, :r0], axis=1, keepdims=True))
                scores[i % 2][0, :, r0:n] = diag
                tops[i] = top

            def soften(i):
                t, h = tasks[i]
                n = (t + 1) * rows
                total = jnp.zeros((rows, rows // 2), f32)
                for c in range(0, n, rows):
                    e = jnp.exp2((scores[i % 2][0, :, c:c + rows] - tops[i]) * (scale * LOG2_E))
                    scores[i % 2][0, :, c:c + rows] = e
                    total = total + e[:, :rows // 2] + e[:, rows // 2:]
                inverse = 1.0 / jnp.sum(total, axis=1, keepdims=True)
                for c in range(0, n, rows):
                    probs[:, (i % 2) * seq + c:(i % 2) * seq + c + rows] = (
                        scores[i % 2][0, :, c:c + rows] * inverse).astype(bf16)

            def mix(i):
                t, h = tasks[i]
                r0, n = t * rows, (t + 1) * rows
                v = qkv[0:n, 2 * attn + h * head:2 * attn + (h + 1) * head]
                o = jnp.dot(probs[:, (i % 2) * seq:(i % 2) * seq + n], v, preferred_element_type=f32)
                qkv[r0:n, h * head:(h + 1) * head] = o.astype(bf16)

            score(0)
            for i in range(len(tasks)):
                if i + 1 < len(tasks):
                    score(i + 1)
                soften(i)
                mix(i)
                if i % n_heads == n_heads - 1 and tasks[i][0] % PARTS == PARTS - 1:
                    for done in range(tasks[i][0] - PARTS + 1, tasks[i][0] + 1):
                        ostore(done).start()
            for t in range(seq // rows):
                ostore(t).wait()
        pl.run_scoped(scope, pltpu.VMEM((1, rows, seq), f32), pltpu.VMEM((1, rows, seq), f32))

    def chip_of(w):
        near = (w * (3 - w)) // 2
        off = near * (3 - 2 * w) + 2 * ((3 - w) // 3)
        plus = near * (2 - w)
        return (chip + off + n_chips) % n_chips, 2 * plus, 1 + 2 * plus + w // 3

    def place_of(v):
        return (v % 3) * (2 - v % 3)

    def rows_load(s, v):
        d, _, _ = chip_of(v // 2)
        return pltpu.make_async_copy(n_all.at[s, d, v % 2], nbuf.at[place_of(v)], a_sem.at[place_of(v)])

    def rows_start(s, v):
        rows_load(s, v).start()

    def phase_d(s):
        def scope(lhs, pst, ost, tb):
            first, later = s == 0, s > 0

            def left_load(w, own, whole):
                d, slot_p, slot_o = chip_of(w)
                src = ho.at[2 * d + (core if own else other)]
                dst = lhs.at[slot_o if own else slot_p]
                if not whole:
                    src, dst = src.at[:, pl.ds(ff, attn)], dst.at[:, pl.ds(ff, attn)]
                return pltpu.make_async_copy(src, dst, d_sem.at[w, own])

            def left_act(w, own, act):
                @pl.when(first)
                def _():
                    act(left_load(w, own, True))

                @pl.when(later)
                def _():
                    act(left_load(w, own, False))

            def left_start(w, own):
                left_act(w, own, lambda cp: cp.start())

            def left_wait(w, own):
                left_act(w, own, lambda cp: cp.wait())

            def hide(v):
                _, slot_p, slot_o = chip_of(v // 2)
                at = pl.multiple_of((v % 2) * half, half)
                wide = WIDE
                for c in range(0, ff, wide):
                    r = gelu(jnp.dot(nbuf[place_of(v)], wup[:, c:c + wide], preferred_element_type=f32))
                    for k in BOTH:
                        own = 1 - (k + core) % 2
                        slot = slot_p + own * (slot_o - slot_p)
                        lhs[slot, pl.ds(at, half), c:c + wide] = r[k * half:(k + 1) * half]

            def nth(i, k):
                return 2 * i + k

            def swap(b, t, c):
                n = nth(t, c)
                return remote(pst.at[n], pbuf.at[s, b, n], p_s.at[n], p_r.at[s, b * NJ + n], partner)

            def pb_at(t, c):
                return nbuf.at[1, :, cols(nth(t, c))]

            def pb_load(b, t, c):
                return pltpu.make_async_copy(pbuf.at[s, b, nth(t, c)], pb_at(t, c), pb_sem.at[nth(t, c)])

            def pb_start(b, t):
                for c in BOTH:
                    with jax.named_scope("swap_wait"):
                        swap(b, t, c).wait_recv()
                    pb_load(b, t, c).start()

            def t_load(t, c):
                return pltpu.make_async_copy(tin.at[s, :, cols(nth(c, t))], tb.at[c], f_sem.at[c])

            def stored(t):
                for c in BOTH:
                    pltpu.make_async_copy(ost.at[nth(t, c)], pout.at[s, 0, :, cols(nth(c, t))],
                                          os_sem.at[nth(t, c)]).wait()

            def post(b, t):
                stored(t)

                @pl.when(b == 0)
                def _():
                    transit(s, t, right).start()
                    transit(s, 2 + t, left).start()

                @pl.when(b == 1)
                def _():
                    to_left(s, 1, t).start()
                    to_right(s, 1, 2 + t).start()

                @pl.when(b == 2)
                def _():
                    to_right(s, 2, t).start()
                    to_left(s, 2, 2 + t).start()

            def partner_step(b, t):
                @pl.when(b >= 1)
                def _():
                    for c in BOTH:
                        swap(b - 1, t, c).wait_send()

                @pl.when(jnp.logical_and(b == 2, t == 0))
                def _():
                    pb_start(1, 0)
                for c in BOTH:
                    slot_p, _ = block(b, c)
                    r = jnp.dot(lhs[slot_p], wdo[:, cols(nth(c, t))], preferred_element_type=f32)
                    pst[nth(t, c)] = r.astype(bf16)
                for c in BOTH:
                    swap(b, t, c).start()

                @pl.when(jnp.logical_and(b == 2, t == 1))
                def _():
                    post(1, 0)

            def own_step(b, t):
                @pl.when(jnp.logical_and(b == 3, t == 0))
                def _():
                    pb_start(3, 0)

                @pl.when(t == 0)
                def _():
                    pb_start(b, 1)

                @pl.when(jnp.logical_and(b == 1, t == 1))
                def _():
                    pb_start(2, 0)

                @pl.when(b == 2)
                def _():
                    with jax.named_scope("transit_wait"):
                        for c in BOTH:
                            transit(s, nth(c, t), right).wait_recv()
                    for c in BOTH:
                        t_load(t, c).start()
                for c in BOTH:
                    pb_load(b, t, c).wait()
                for c in BOTH:
                    _, slot_o = block(b, c)
                    r = jnp.dot(lhs[slot_o], wdo[:, cols(nth(c, t))], preferred_element_type=f32)
                    ost[nth(t, c)] = (r + pb_at(t, c)[...].astype(f32)).astype(bf16)

                @pl.when(b == 2)
                def _():
                    for c in BOTH:
                        t_load(t, c).wait()

                        @pl.loop(0, PARTS)
                        def _(r):
                            at = pl.ds(pl.multiple_of(r * part, part), part)
                            ost[nth(t, c), at, :] = (ost[nth(t, c), at, :].astype(f32)
                                                     + tb[c, at, :].astype(f32)).astype(bf16)

                for c in BOTH:
                    @pl.when(b < 3)
                    def _():
                        pltpu.make_async_copy(ost.at[nth(t, c)], pout.at[s, b, :, cols(nth(c, t))],
                                              os_sem.at[nth(t, c)]).start()

                    @pl.when(b == 3)
                    def _():
                        pltpu.make_async_copy(ost.at[nth(t, c)], own_out.at[s, :, cols(nth(c, t))],
                                              os_sem.at[nth(t, c)]).start()

                @pl.when(jnp.logical_and(b == 2, t == 0))
                def _():
                    post(1, 1)

                @pl.when(jnp.logical_and(t == 1, b % 2 == 0))
                def _():
                    post(b, 0)

            for w in BOTH:
                for own in BOTH:
                    left_start(w, own)

            @pl.when(first)
            def _():
                w_copies[1].wait()
                w_copies[2].wait()

            n_groups = 7

            def since(g, k):
                return (g + 8 - k) // 8

            def step_of(g, groups):
                return sum(since(g, k) for k in groups[1:])

            def units(g):
                return 2 * since(g, 1) + since(g, 2) + 3 * since(g, 3) + 2 * since(g, 6)

            @pl.loop(0, n_groups)
            def _(g):
                @pl.when(g == 0)
                def _():
                    left_wait(0, 0)

                @pl.when(g == 1)
                def _():
                    pb_start(0, 0)
                    left_start(2, 0)
                    left_wait(0, 1)

                @pl.when(g == 2)
                def _():
                    left_start(2, 1)

                @pl.when(g == 3)
                def _():
                    left_wait(1, 1)
                    left_wait(2, 1)

                @pl.when(g == 4)
                def _():
                    left_start(3, 0)
                    left_start(3, 1)

                @pl.when(later)
                def _():
                    @pl.loop(units(g), units(g + 1))
                    def _(v):
                        with jax.named_scope("n_wait"):
                            rows_load(s, v).wait()

                        @pl.when(jnp.logical_and(v % 3 != 2, v < 2 * n_chips - 1))
                        def _():
                            rows_start(s, v + 1)

                        @pl.when(jnp.logical_and(v == 2 * n_chips - 1, s < batch - 1))
                        def _():
                            first_start(s + 1)
                        with jax.named_scope("hide"):
                            hide(v)

                        @pl.when(v % 3 == 2)
                        def _():
                            rows_start(s, v + 1)

                        @pl.when(v == 3)
                        def _():
                            post(0, 1)

                        @pl.when(v == 6)
                        def _():
                            post(2, 1)

                @pl.when(g == 2)
                def _():
                    left_wait(1, 0)
                    left_wait(2, 0)

                @pl.when(g == 5)
                def _():
                    left_wait(3, 0)
                    left_wait(3, 1)

                @pl.when(first)
                def _():
                    @pl.when(g == 2)
                    def _():
                        post(0, 1)

                    @pl.when(g == 5)
                    def _():
                        post(2, 1)

                    @pl.when(g == 6)
                    def _():
                        first_start(s + 1)

                @pl.loop(0, 2)
                def _(t):
                    @pl.when(any_of(g, PARTNER_GROUPS))
                    def _():
                        with jax.named_scope("partner"):
                            partner_step(step_of(g, PARTNER_GROUPS), t)

                    @pl.when(any_of(g, OWN_GROUPS))
                    def _():
                        with jax.named_scope("own"):
                            own_step(step_of(g, OWN_GROUPS), t)

                @pl.when(jnp.logical_and(s < batch - 1, g == 2))
                def _():
                    @pl.when(later)
                    def _():
                        ag_second(s + 1)
                    forward(s + 1, (2, 3))

                @pl.when(jnp.logical_and(s < batch - 1, g == n_groups - 1))
                def _():
                    forward(s + 1, (4, 5))

            stored(0)
            stored(1)
            for t in BOTH:
                for c in BOTH:
                    swap(3, t, c).wait_send()

            @pl.when(s < batch - 2)
            def _():
                ag_first(s + 2)
        pl.run_scoped(scope, pltpu.VMEM((4, rows, ff + attn), bf16), pltpu.VMEM((NJ, rows, ncol), bf16),
                      pltpu.VMEM((NJ, rows, ncol), bf16), pltpu.VMEM((2, rows, ncol), bf16))

    def opening(raw, wide):
        kinds = qkv_cols // attn
        per = qkv_cols // LANES
        slots, part_rows = raw.shape[0], raw.shape[1]
        n_parts = dim * per // part_rows
        chunk = wide.shape[0] // per
        chunks = part_rows // (chunk * per)
        xbuf = nbuf.at[1]

        def load(q):
            at = pl.ds(pl.multiple_of(q * part_rows, part_rows), part_rows)
            return pltpu.make_async_copy(wqkv_hbm.at[at], raw.at[q % slots], o_sem.at[q])

        x_start(0, xbuf)
        for q in range(slots):
            load(q).start()
        for cp in v_copies:
            cp.wait()
        with jax.named_scope("send0"):
            for q in range(PARTS):
                normalise(0, xbuf, q)
                if q == 1:
                    n_store(0, xbuf, 0).wait()
                    n_store(0, xbuf, 1).wait()
                    ici_copy(0, 2, chip, 0, right).start()
                    d2d_copy(0, 0, chip, 0, core).start()
            n_store(0, xbuf, 2).wait()
            n_store(0, xbuf, 3).wait()
            ici_copy(0, 3, chip, 1, left).start()
            d2d_copy(0, 1, chip, 1, core).start()
            ag_second(0)
        with jax.named_scope("place"):
            @pl.loop(0, n_parts)
            def _(q):
                load(q).wait()

                @pl.loop(0, chunks)
                def _(i):
                    at = pl.ds(pl.multiple_of(i * (chunk * per), chunk * per), chunk * per)
                    wide[...] = raw[q % slots, at, :].astype(f32)
                    to = pl.ds(pl.multiple_of((q * chunks + i) * chunk, chunk), chunk)
                    for j in range(kinds):
                        for c in range(head // LANES):
                            for g in range(n_heads):
                                row = (j * (head // LANES) + c) * n_heads + g
                                col = j * attn + g * head + c * LANES
                                wqkv[to, col:col + LANES] = wide[pl.ds(row, chunk, stride=per), :].astype(bf16)

                @pl.when(q + slots < n_parts)
                def _():
                    load(q + slots).start()

                @pl.when(q == n_parts - slots)
                def _():
                    w_copies[0].start()
                    first_start(0)

    pl.run_scoped(opening, pltpu.VMEM((6, dim * (qkv_cols // LANES) // 8, LANES), bf16),
                  pltpu.VMEM((LANES * (qkv_cols // LANES), LANES), f32))

    @pl.loop(0, batch)
    def _(s):
        def scope(qkv):
            with jax.named_scope("A"):
                phase_a(s, qkv)

            @pl.when(s > 0)
            def _():
                rows_start(s, 0)
            with jax.named_scope("B"):
                phase_b(qkv)
        pl.run_scoped(scope, pltpu.VMEM((seq, qkv_cols), bf16))
        with jax.named_scope("D"):
            phase_d(s)

    def finish(buf):
        n_steps, depth = batch * PARTS, buf.shape[0]

        def rows_at(n):
            return n // PARTS, pl.ds(pl.multiple_of((n % PARTS) * part, part), part)

        def loads(n):
            s, at = rows_at(n)
            return [pltpu.make_async_copy(src.at[s, at], buf.at[n % depth, i], y_sem.at[n % depth, i])
                    for i, src in enumerate((own_out, left_out, right_out, x_ref))]

        def store(n):
            s, at = rows_at(n)
            return pltpu.make_async_copy(buf.at[n % depth, PARTS - 1], y_ref.at[s, at], z_sem.at[n % depth])

        def begin(n):
            @pl.when(n % PARTS == 0)
            def _():
                for j in range(NJ):
                    to_right(n // PARTS, 2, j).wait_recv()
                    to_left(n // PARTS, 2, j).wait_recv()
            for cp in loads(n):
                cp.start()

        begin(0)
        begin(1)

        @pl.loop(0, n_steps)
        def _(n):
            k = n % depth
            for cp in loads(n):
                cp.wait()
            for c in range(0, dim, ncol):
                own, from_left, from_right, x = (buf[k, i, :, c:c + ncol].astype(f32) for i in range(PARTS))
                branch = (own + from_left + from_right).astype(bf16)
                buf[k, PARTS - 1, :, c:c + ncol] = (x + branch.astype(f32)).astype(bf16)
            store(n).start()

            @pl.when(n + 2 < n_steps)
            def _():
                @pl.when(n >= 1)
                def _():
                    store(n - 1).wait()
                begin(n + 2)
        for n in range(n_steps - depth, n_steps):
            store(n).wait()

    with jax.named_scope("finish"):
        pl.run_scoped(finish, pltpu.VMEM((3, PARTS, part, dim), bf16))

    @pl.loop(0, batch)
    def _(s):
        for j in range(NJ):
            to_right(s, 2, j).wait_send()
            to_left(s, 2, j).wait_send()
            transit(s, j, right).wait_send()
        for u in range(2 * n_chips):
            d, hf = unit(u)
            d2d_copy(s, u, d, hf, core).wait_send()
            if u >= 2:
                ici_copy(s, u, d, hf, right).wait_send()


def layer_call(x_blk, ln_gain, ln_bias, wqkv, w_out, w_up, w_down, n_tp):
    batch, rows, dim = x_blk.shape
    ff, attn, qkv_cols = w_up.shape[1], w_out.shape[0], wqkv.shape[0] * LANES // dim
    n_chips = n_tp // 2
    ncol = dim // NJ
    bf16 = jnp.bfloat16
    dma = pltpu.SemaphoreType.DMA
    flops = 2 * batch * n_tp * rows * dim * (qkv_cols + 2 * ff + attn)
    outs = pl.pallas_call(
        layer_kernel,
        name="parallel_layer",
        out_shape=[
            jax.ShapeDtypeStruct((batch, rows, dim), bf16),
            jax.ShapeDtypeStruct((batch, rows, dim), bf16),
            jax.ShapeDtypeStruct((batch, rows, dim), bf16),
            jax.ShapeDtypeStruct((batch, rows, dim), bf16),
            jax.ShapeDtypeStruct((batch, n_chips, 2, rows, dim), bf16),
            jax.ShapeDtypeStruct((n_tp, rows, ff + attn), bf16),
            jax.ShapeDtypeStruct((batch, 4, NJ, rows, ncol), bf16),
            jax.ShapeDtypeStruct((batch, 3, rows, dim), bf16),
            jax.ShapeDtypeStruct((batch, rows, dim), bf16),
        ],
        in_specs=[pl.BlockSpec(memory_space=pl.ANY)] * N_IN,
        out_specs=[pl.BlockSpec(memory_space=pl.ANY)] * N_OUT,
        scratch_shapes=[
            pltpu.VMEM((dim, qkv_cols), bf16), pltpu.VMEM((dim, ff), bf16), pltpu.VMEM((ff + attn, dim), bf16),
            pltpu.VMEM((1, dim), jnp.float32), pltpu.VMEM((1, dim), jnp.float32), pltpu.VMEM((2, rows, dim), bf16),
            dma((batch, 8)), dma((batch, 8)), dma((batch, 8)), dma((batch, 8)),
            dma((NJ,)), dma((batch, 4 * NJ)), dma((batch, NJ)), dma((batch, NJ)),
            dma((batch, 2 * NJ)), dma((batch, 2 * NJ)),
            dma((3,)), dma((2,)), dma((2, 4)), dma((2,)), dma((2,)), dma((n_tp,)), dma((4, 2)), dma((NJ,)), dma((NJ,)),
            dma((2,)), dma((3, PARTS)), dma((3,)),
        ],
        compiler_params=pltpu.CompilerParams(
            collective_id=0, has_side_effects=True, vmem_limit_bytes=67043328),
        cost_estimate=pl.CostEstimate(flops=flops, bytes_accessed=256 << 20, transcendentals=0),
    )(x_blk, ln_gain.reshape(1, dim), ln_bias.reshape(1, dim), wqkv, w_out, w_up, w_down)
    return outs[0]


def solution(mesh):
    n_tp = mesh.shape["tp"]

    def local_layer(x_blk, ln_gain, ln_bias, w_qkv, w_out, w_up, w_down):
        dim = x_blk.shape[2]
        groups, kinds, head = w_qkv.shape[1:]
        wqkv = w_qkv.reshape(dim, groups, kinds, head // LANES, LANES).transpose(0, 2, 3, 1, 4).reshape(-1, LANES)
        return layer_call(x_blk, ln_gain, ln_bias, wqkv, w_out, w_up, w_down, n_tp)

    return jax.shard_map(
        local_layer, mesh=mesh,
        in_specs=(P("dp", "tp", None), P(), P(), P(None, "tp", None, None),
                  P("tp", None), P(None, "tp"), P("tp", None)),
        out_specs=P("dp", "tp", None), check_vma=False)
```

```python
import functools

import jax
import jax.numpy as jnp
from jax import lax
from jax.experimental import pallas as pl
from jax.experimental.pallas import tpu as pltpu
from jax.sharding import PartitionSpec as P

LN_EPS = 1e-5
LOG2_E = 1.4426950408889634
BOTH, PARTS = (0, 1), 4
N_IN, N_OUT, LANES, WIDE = 7, 9, 128, 512
PARTNER_GROUPS, OWN_GROUPS = (0, 2, 3, 5), (1, 3, 4, 6)
NJ = 4


def any_of(value, choices):
    return functools.reduce(jnp.logical_or, [value == c for c in choices])


def layer_kernel(x_ref, gain_ref, bias_ref, wqkv_hbm, wout_hbm, wup_hbm, wdown_hbm,
                 y_ref, own_out, left_out, right_out, n_all, ho, pbuf, pout, tin,
                 wqkv, wup, wdo, gain, bias, nbuf,
                 ag_is, ag_ir, ag_ds, ag_dr, p_s, p_r, t_s, t_r, m_s, m_r,
                 w_sem, v_sem, ln_sem, a_sem, h_sem, o_sem, d_sem, pb_sem, os_sem, f_sem, y_sem, z_sem):
    batch, rows, dim = x_ref.shape
    half = rows // 2
    ff = wup.shape[1]
    attn = wdo.shape[0] - ff
    qkv_cols = wqkv.shape[1]
    n_heads = 2
    head = attn // n_heads
    n_chips = n_all.shape[1]
    seq = n_chips * 2 * rows
    ncol = dim // NJ
    f32, bf16 = jnp.float32, jnp.bfloat16

    me = lax.axis_index("tp")
    chip, core = me // 2, me % 2
    other = 1 - core
    partner = chip * 2 + other
    right = ((chip + 1) % n_chips) * 2 + core
    left = ((chip + n_chips - 1) % n_chips) * 2 + core

    def remote(src, dst, send, recv, dev):
        return pltpu.make_async_remote_copy(
            src_ref=src, dst_ref=dst, send_sem=send, recv_sem=recv,
            device_id={"tp": dev}, device_id_type=pl.DeviceIdType.MESH)

    barrier = pltpu.get_barrier_semaphore()
    for dev in (partner, right, left):
        pl.semaphore_signal(barrier, inc=1, device_id={"tp": dev}, device_id_type=pl.DeviceIdType.MESH)

    w_copies = (
        pltpu.make_async_copy(wup_hbm, wup, w_sem.at[0]),
        pltpu.make_async_copy(wdown_hbm, wdo.at[pl.ds(0, ff)], w_sem.at[1]),
        pltpu.make_async_copy(wout_hbm, wdo.at[pl.ds(ff, attn)], w_sem.at[2]),
    )
    v_copies = (pltpu.make_async_copy(gain_ref, gain, v_sem.at[0]),
                pltpu.make_async_copy(bias_ref, bias, v_sem.at[1]))
    for cp in v_copies:
        cp.start()

    def unit(u):
        g, b = u // 2, u % 2
        near = (g * (3 - g)) // 2
        off = near * (2 * b - 1) + 2 * (g // 3)
        hf = (b + near * (g - 1)) % 2
        return (chip + off + n_chips) % n_chips, hf

    def piece(s, d, hf, k):
        return n_all.at[s, d, hf, pl.ds(pl.multiple_of(k * half, half), half)]

    def ici_copy(s, u, d, hf, dev):
        return remote(piece(s, d, hf, core), piece(s, d, hf, core), ag_is.at[s, u], ag_ir.at[s, u], dev)

    def d2d_copy(s, u, d, hf, k):
        return remote(piece(s, d, hf, k), piece(s, d, hf, k), ag_ds.at[s, u], ag_dr.at[s, u], partner)

    part = rows // PARTS

    def x_load(s, buf, q):
        at = pl.ds(q * part, part)
        return pltpu.make_async_copy(x_ref.at[s, at], buf.at[at], ln_sem.at[0, q])

    def n_store(s, buf, q):
        dst = n_all.at[s, chip, q // 2, pl.ds(pl.multiple_of(core * half + (q % 2) * part, part), part)]
        return pltpu.make_async_copy(buf.at[pl.ds(q * part, part)], dst, ln_sem.at[1, q])

    def x_start(s, buf):
        for q in range(PARTS):
            x_load(s, buf, q).start()

    def normalise(s, buf, q):
        x_load(s, buf, q).wait()
        at = pl.ds(q * part, part)
        lanes, wide = LANES, WIDE
        total = jnp.zeros((part, lanes), f32)
        for c in range(0, dim, wide):
            v = buf[at, c:c + wide].astype(f32)
            for k in range(0, wide, lanes):
                total = total + v[:, k:k + lanes]
        mean = jnp.sum(total, axis=-1, keepdims=True) * (1.0 / dim)
        total = jnp.zeros((part, lanes), f32)
        for c in range(0, dim, wide):
            cen = buf[at, c:c + wide].astype(f32) - mean
            for k in range(0, wide, lanes):
                total = total + cen[:, k:k + lanes] * cen[:, k:k + lanes]
        inv = lax.rsqrt(jnp.sum(total, axis=-1, keepdims=True) * (1.0 / dim) + LN_EPS)
        for c in range(0, dim, wide):
            cen = buf[at, c:c + wide].astype(f32) - mean
            buf[at, c:c + wide] = (cen * inv * gain[:, c:c + wide] + bias[:, c:c + wide]).astype(bf16)
        n_store(s, buf, q).start()

    def ag_first(s):
        ici_copy(s, 2, chip, 0, right).start()
        ici_copy(s, 3, chip, 1, left).start()
        d2d_copy(s, 0, chip, 0, core).start()
        d2d_copy(s, 1, chip, 1, core).start()

    def ag_second(s):
        ici_copy(s, 4, chip, 1, right).start()
        ici_copy(s, 5, chip, 0, left).start()

    def forward(s, us):
        for u in us:
            d, hf = unit(u)
            with jax.named_scope(f"ici_wait_{u}"):
                ici_copy(s, u, d, hf, right).wait_recv()
            if u == 2:
                ici_copy(s, 6, d, hf, right).start()
            if u == 3:
                ici_copy(s, 7, d, hf, left).start()
            d2d_copy(s, u, d, hf, core).start()

    def block(b, second):
        near = (b * (3 - b)) // 2
        plus = (near * (1 + (2 * second - 1) * (3 - 2 * b))) // 2
        return 2 * plus, 1 + 2 * plus + b // 3

    def cols(j):
        return pl.ds(pl.multiple_of(j * ncol, ncol), ncol)

    def to_right(s, ii, j):
        return remote(pout.at[s, ii, :, cols(j)], left_out.at[s, :, cols(j)], m_s.at[s, j], m_r.at[s, j], right)

    def to_left(s, ii, j):
        return remote(pout.at[s, ii, :, cols(j)], right_out.at[s, :, cols(j)], m_s.at[s, NJ + j], m_r.at[s, NJ + j],
                      left)

    def transit(s, j, dev):
        return remote(pout.at[s, 0, :, cols(j)], tin.at[s, :, cols(j)], t_s.at[s, j], t_r.at[s, j], dev)

    def first_load(s):
        return pltpu.make_async_copy(n_all.at[s, chip, 0], nbuf.at[0], a_sem.at[0])

    def first_start(s):
        with jax.named_scope("d2d_wait"):
            d2d_copy(s, 0, chip, 0, other).wait_recv()
        first_load(s).start()

    def gelu(h):
        return (0.5 * h * (1.0 + lax.erf(h * (2.0 ** -0.5)))).astype(bf16)

    def phase_a(s, qkv):
        def scope(hbuf):
            first, later = s == 0, s > 0

            def load(u):
                d, hf = unit(u)
                return pltpu.make_async_copy(n_all.at[s, d, hf], nbuf.at[u % 2], a_sem.at[u % 2])

            def arrived(u):
                d, hf = unit(u)
                with jax.named_scope("d2d_wait"):
                    d2d_copy(s, u, d, hf, other).wait_recv()

            def hstore(u, k):
                d, hf = unit(u)
                return pltpu.make_async_copy(
                    hbuf.at[pl.ds(k * half, half)],
                    ho.at[2 * d + k, pl.ds(pl.multiple_of(hf * half, half), half), pl.ds(0, ff)],
                    h_sem.at[k])

            def project(u):
                d, hf = unit(u)
                wide = WIDE
                for c in range(0, qkv_cols, wide):
                    r = jnp.dot(nbuf[u % 2], wqkv[:, c:c + wide], preferred_element_type=f32).astype(bf16)
                    for k in BOTH:
                        pos = pl.multiple_of(d * (2 * rows) + k * rows + hf * half, half)
                        qkv[pl.ds(pos, half), c:c + wide] = r[k * half:(k + 1) * half]

            @pl.loop(0, 2 * n_chips)
            def _(u):
                odd = u % 2 == 1
                with jax.named_scope("load_wait"):
                    load(u).wait()

                @pl.when(jnp.logical_and(later, u == 4))
                def _():
                    forward(s, (6, 7))

                @pl.when(jnp.logical_or(jnp.logical_and(later, u < 7), u % 2 == 0))
                def _():
                    arrived(u + 1)
                    load(u + 1).start()

                @pl.when(later)
                def _():
                    project(u)

                @pl.when(first)
                def _():
                    @pl.when(jnp.logical_and(odd, u < 7))
                    def _():
                        x_start((u + 1) // 2, nbuf.at[0])

                    project(u)

                    @pl.when(u == 0)
                    def _():
                        w_copies[0].wait()
                        for cp in w_copies[1:]:
                            cp.start()

                    @pl.when(u >= 1)
                    def _():
                        for k in BOTH:
                            hstore(u - 1, k).wait()
                    hbuf[...] = gelu(jnp.dot(nbuf[u % 2], wup[...], preferred_element_type=f32))
                    for k in BOTH:
                        hstore(u, k).start()

                    @pl.when(u == 1)
                    def _():
                        forward(0, (2, 3))

                    @pl.when(u == 3)
                    def _():
                        forward(0, (4, 5))

                    @pl.when(u == 5)
                    def _():
                        forward(0, (6, 7))

                    @pl.when(jnp.logical_and(odd, u < 7))
                    def _():
                        with jax.named_scope("norm"):
                            for q in range(PARTS):
                                normalise((u + 1) // 2, nbuf.at[0], q)
                            for q in range(PARTS):
                                n_store((u + 1) // 2, nbuf.at[0], q).wait()

                        @pl.when(u == 1)
                        def _():
                            ag_first(1)
                            ag_second(1)
                        arrived(u + 1)
                        load(u + 1).start()

            @pl.when(first)
            def _():
                for k in BOTH:
                    hstore(7, k).wait()
        pl.run_scoped(scope, pltpu.VMEM((rows, ff), bf16))

    def phase_b(qkv):
        def ostore(t):
            return pltpu.make_async_copy(qkv.at[pl.ds(t * rows, rows), pl.ds(0, attn)],
                                         ho.at[t, :, pl.ds(ff, attn)], o_sem.at[t])
        scale = head ** -0.5

        probs = nbuf.at[1]

        def scope(*scores):
            keep = (lax.broadcasted_iota(jnp.int32, (rows, rows), 0)
                    >= lax.broadcasted_iota(jnp.int32, (rows, rows), 1))
            tasks = [(t, h) for t in range(seq // rows) for h in range(n_heads)]
            tops = {}

            def score(i):
                t, h = tasks[i]
                r0, n = t * rows, (t + 1) * rows
                q = qkv[r0:n, h * head:(h + 1) * head]
                k = qkv[0:n, attn + h * head:attn + (h + 1) * head]
                sc = lax.dot_general(q, k, (((1,), (1,)), ((), ())), preferred_element_type=f32)
                diag = jnp.where(keep, sc[:, r0:], -jnp.inf)
                top = jnp.max(diag, axis=1, keepdims=True)
                if t:
                    scores[i % 2][0, :, 0:r0] = sc[:, :r0]
                    top = jnp.maximum(top, jnp.max(sc[:, :r0], axis=1, keepdims=True))
                scores[i % 2][0, :, r0:n] = diag
                tops[i] = top

            def soften(i):
                t, h = tasks[i]
                n = (t + 1) * rows
                total = jnp.zeros((rows, rows // 2), f32)
                for c in range(0, n, rows):
                    e = jnp.exp2((scores[i % 2][0, :, c:c + rows] - tops[i]) * (scale * LOG2_E))
                    scores[i % 2][0, :, c:c + rows] = e
                    total = total + e[:, :rows // 2] + e[:, rows // 2:]
                inverse = 1.0 / jnp.sum(total, axis=1, keepdims=True)
                for c in range(0, n, rows):
                    probs[:, (i % 2) * seq + c:(i % 2) * seq + c + rows] = (
                        scores[i % 2][0, :, c:c + rows] * inverse).astype(bf16)

            def mix(i):
                t, h = tasks[i]
                r0, n = t * rows, (t + 1) * rows
                v = qkv[0:n, 2 * attn + h * head:2 * attn + (h + 1) * head]
                o = jnp.dot(probs[:, (i % 2) * seq:(i % 2) * seq + n], v, preferred_element_type=f32)
                qkv[r0:n, h * head:(h + 1) * head] = o.astype(bf16)

            score(0)
            for i in range(len(tasks)):
                if i + 1 < len(tasks):
                    score(i + 1)
                soften(i)
                mix(i)
                if i % n_heads == n_heads - 1 and tasks[i][0] % PARTS == PARTS - 1:
                    for done in range(tasks[i][0] - PARTS + 1, tasks[i][0] + 1):
                        ostore(done).start()
            for t in range(seq // rows):
                ostore(t).wait()
        pl.run_scoped(scope, pltpu.VMEM((1, rows, seq), f32), pltpu.VMEM((1, rows, seq), f32))

    def chip_of(w):
        near = (w * (3 - w)) // 2
        off = near * (3 - 2 * w) + 2 * ((3 - w) // 3)
        plus = near * (2 - w)
        return (chip + off + n_chips) % n_chips, 2 * plus, 1 + 2 * plus + w // 3

    def place_of(v):
        return (v % 3) * (2 - v % 3)

    def rows_load(s, v):
        d, _, _ = chip_of(v // 2)
        return pltpu.make_async_copy(n_all.at[s, d, v % 2], nbuf.at[place_of(v)], a_sem.at[place_of(v)])

    def rows_start(s, v):
        rows_load(s, v).start()

    def phase_d(s):
        def scope(lhs, pst, ost, tb):
            first, later = s == 0, s > 0

            def left_load(w, own, whole):
                d, slot_p, slot_o = chip_of(w)
                src = ho.at[2 * d + (core if own else other)]
                dst = lhs.at[slot_o if own else slot_p]
                if not whole:
                    src, dst = src.at[:, pl.ds(ff, attn)], dst.at[:, pl.ds(ff, attn)]
                return pltpu.make_async_copy(src, dst, d_sem.at[w, own])

            def left_act(w, own, act):
                @pl.when(first)
                def _():
                    act(left_load(w, own, True))

                @pl.when(later)
                def _():
                    act(left_load(w, own, False))

            def left_start(w, own):
                left_act(w, own, lambda cp: cp.start())

            def left_wait(w, own):
                left_act(w, own, lambda cp: cp.wait())

            def hide(v):
                _, slot_p, slot_o = chip_of(v // 2)
                at = pl.multiple_of((v % 2) * half, half)
                wide = WIDE
                for c in range(0, ff, wide):
                    r = gelu(jnp.dot(nbuf[place_of(v)], wup[:, c:c + wide], preferred_element_type=f32))
                    for k in BOTH:
                        own = 1 - (k + core) % 2
                        slot = slot_p + own * (slot_o - slot_p)
                        lhs[slot, pl.ds(at, half), c:c + wide] = r[k * half:(k + 1) * half]

            def nth(i, k):
                return 2 * i + k

            def swap(b, t, c):
                n = nth(t, c)
                return remote(pst.at[n], pbuf.at[s, b, n], p_s.at[n], p_r.at[s, b * NJ + n], partner)

            def pb_at(t, c):
                return nbuf.at[1, :, cols(nth(t, c))]

            def pb_load(b, t, c):
                return pltpu.make_async_copy(pbuf.at[s, b, nth(t, c)], pb_at(t, c), pb_sem.at[nth(t, c)])

            def pb_start(b, t):
                for c in BOTH:
                    with jax.named_scope("swap_wait"):
                        swap(b, t, c).wait_recv()
                    pb_load(b, t, c).start()

            def t_load(t, c):
                return pltpu.make_async_copy(tin.at[s, :, cols(nth(c, t))], tb.at[c], f_sem.at[c])

            def stored(t):
                for c in BOTH:
                    pltpu.make_async_copy(ost.at[nth(t, c)], pout.at[s, 0, :, cols(nth(c, t))],
                                          os_sem.at[nth(t, c)]).wait()

            def post(b, t):
                stored(t)

                @pl.when(b == 0)
                def _():
                    transit(s, t, right).start()
                    transit(s, 2 + t, left).start()

                @pl.when(b == 1)
                def _():
                    to_left(s, 1, t).start()
                    to_right(s, 1, 2 + t).start()

                @pl.when(b == 2)
                def _():
                    to_right(s, 2, t).start()
                    to_left(s, 2, 2 + t).start()

            def partner_step(b, t):
                @pl.when(b >= 1)
                def _():
                    for c in BOTH:
                        swap(b - 1, t, c).wait_send()

                @pl.when(jnp.logical_and(b == 2, t == 0))
                def _():
                    pb_start(1, 0)
                for c in BOTH:
                    slot_p, _ = block(b, c)
                    r = jnp.dot(lhs[slot_p], wdo[:, cols(nth(c, t))], preferred_element_type=f32)
                    pst[nth(t, c)] = r.astype(bf16)
                for c in BOTH:
                    swap(b, t, c).start()

                @pl.when(jnp.logical_and(b == 2, t == 1))
                def _():
                    post(1, 0)

            def own_step(b, t):
                @pl.when(jnp.logical_and(b == 3, t == 0))
                def _():
                    pb_start(3, 0)

                @pl.when(t == 0)
                def _():
                    pb_start(b, 1)

                @pl.when(jnp.logical_and(b == 1, t == 1))
                def _():
                    pb_start(2, 0)

                @pl.when(b == 2)
                def _():
                    with jax.named_scope("transit_wait"):
                        for c in BOTH:
                            transit(s, nth(c, t), right).wait_recv()
                    for c in BOTH:
                        t_load(t, c).start()
                for c in BOTH:
                    pb_load(b, t, c).wait()
                for c in BOTH:
                    _, slot_o = block(b, c)
                    r = jnp.dot(lhs[slot_o], wdo[:, cols(nth(c, t))], preferred_element_type=f32)
                    ost[nth(t, c)] = (r + pb_at(t, c)[...].astype(f32)).astype(bf16)

                @pl.when(b == 2)
                def _():
                    for c in BOTH:
                        t_load(t, c).wait()

                        @pl.loop(0, PARTS)
                        def _(r):
                            at = pl.ds(pl.multiple_of(r * part, part), part)
                            ost[nth(t, c), at, :] = (ost[nth(t, c), at, :].astype(f32)
                                                     + tb[c, at, :].astype(f32)).astype(bf16)

                for c in BOTH:
                    @pl.when(b < 3)
                    def _():
                        pltpu.make_async_copy(ost.at[nth(t, c)], pout.at[s, b, :, cols(nth(c, t))],
                                              os_sem.at[nth(t, c)]).start()

                    @pl.when(b == 3)
                    def _():
                        pltpu.make_async_copy(ost.at[nth(t, c)], own_out.at[s, :, cols(nth(c, t))],
                                              os_sem.at[nth(t, c)]).start()

                @pl.when(jnp.logical_and(b == 2, t == 0))
                def _():
                    post(1, 1)

                @pl.when(jnp.logical_and(t == 1, b % 2 == 0))
                def _():
                    post(b, 0)

            for w in BOTH:
                for own in BOTH:
                    left_start(w, own)

            @pl.when(first)
            def _():
                w_copies[1].wait()
                w_copies[2].wait()

            n_groups = 7

            def since(g, k):
                return (g + 8 - k) // 8

            def step_of(g, groups):
                return sum(since(g, k) for k in groups[1:])

            def units(g):
                return 2 * since(g, 1) + since(g, 2) + 3 * since(g, 3) + 2 * since(g, 6)

            @pl.loop(0, n_groups)
            def _(g):
                @pl.when(g == 1)
                def _():
                    pb_start(0, 0)
                    left_start(2, 0)

                @pl.when(g == 2)
                def _():
                    left_start(2, 1)

                @pl.when(g == 3)
                def _():
                    left_wait(1, 1)
                    left_wait(2, 1)

                @pl.when(g == 4)
                def _():
                    left_start(3, 0)
                    left_start(3, 1)

                @pl.when(later)
                def _():
                    @pl.loop(units(g), units(g + 1))
                    def _(v):
                        with jax.named_scope("n_wait"):
                            rows_load(s, v).wait()

                        @pl.when(jnp.logical_and(v % 3 != 2, v < 2 * n_chips - 1))
                        def _():
                            rows_start(s, v + 1)

                        @pl.when(jnp.logical_and(v == 2 * n_chips - 1, s < batch - 1))
                        def _():
                            first_start(s + 1)
                        with jax.named_scope("hide"):
                            hide(v)

                        @pl.when(v % 3 == 2)
                        def _():
                            rows_start(s, v + 1)

                        @pl.when(v == 3)
                        def _():
                            post(0, 1)

                        @pl.when(v == 6)
                        def _():
                            post(2, 1)

                @pl.when(g == 0)
                def _():
                    left_wait(0, 0)

                @pl.when(g == 1)
                def _():
                    left_wait(0, 1)

                @pl.when(g == 2)
                def _():
                    left_wait(1, 0)
                    left_wait(2, 0)

                @pl.when(g == 5)
                def _():
                    left_wait(3, 0)
                    left_wait(3, 1)

                @pl.when(first)
                def _():
                    @pl.when(g == 2)
                    def _():
                        post(0, 1)

                    @pl.when(g == 5)
                    def _():
                        post(2, 1)

                    @pl.when(g == 6)
                    def _():
                        first_start(s + 1)

                @pl.loop(0, 2)
                def _(t):
                    @pl.when(any_of(g, PARTNER_GROUPS))
                    def _():
                        with jax.named_scope("partner"):
                            partner_step(step_of(g, PARTNER_GROUPS), t)

                    @pl.when(any_of(g, OWN_GROUPS))
                    def _():
                        with jax.named_scope("own"):
                            own_step(step_of(g, OWN_GROUPS), t)

                @pl.when(jnp.logical_and(s < batch - 1, g == 2))
                def _():
                    @pl.when(later)
                    def _():
                        ag_second(s + 1)
                    forward(s + 1, (2, 3))

                @pl.when(jnp.logical_and(s < batch - 1, g == n_groups - 1))
                def _():
                    forward(s + 1, (4, 5))

            stored(0)
            stored(1)
            for t in BOTH:
                for c in BOTH:
                    swap(3, t, c).wait_send()

            @pl.when(s < batch - 2)
            def _():
                ag_first(s + 2)
        pl.run_scoped(scope, pltpu.VMEM((4, rows, ff + attn), bf16), pltpu.VMEM((NJ, rows, ncol), bf16),
                      pltpu.VMEM((NJ, rows, ncol), bf16), pltpu.VMEM((2, rows, ncol), bf16))

    def opening(raw, wide):
        kinds = qkv_cols // attn
        per = qkv_cols // LANES
        slots, part_rows = raw.shape[0], raw.shape[1]
        n_parts = dim * per // part_rows
        chunk = wide.shape[0] // per
        chunks = part_rows // (chunk * per)
        xbuf = nbuf.at[1]

        def load(q):
            at = pl.ds(pl.multiple_of(q * part_rows, part_rows), part_rows)
            return pltpu.make_async_copy(wqkv_hbm.at[at], raw.at[q % slots], o_sem.at[q])

        x_start(0, xbuf)
        for q in range(slots):
            load(q).start()
        for cp in v_copies:
            cp.wait()
        with jax.named_scope("send0"):
            for q in range(PARTS):
                normalise(0, xbuf, q)
                if q == 1:
                    n_store(0, xbuf, 0).wait()
                    n_store(0, xbuf, 1).wait()
                    pl.semaphore_wait(barrier, 3)
                    ici_copy(0, 2, chip, 0, right).start()
                    d2d_copy(0, 0, chip, 0, core).start()
            n_store(0, xbuf, 2).wait()
            n_store(0, xbuf, 3).wait()
            ici_copy(0, 3, chip, 1, left).start()
            d2d_copy(0, 1, chip, 1, core).start()
            ag_second(0)
        with jax.named_scope("place"):
            @pl.loop(0, n_parts)
            def _(q):
                load(q).wait()

                @pl.loop(0, chunks)
                def _(i):
                    at = pl.ds(pl.multiple_of(i * (chunk * per), chunk * per), chunk * per)
                    wide[...] = raw[q % slots, at, :].astype(f32)
                    to = pl.ds(pl.multiple_of((q * chunks + i) * chunk, chunk), chunk)
                    for j in range(kinds):
                        for c in range(head // LANES):
                            for g in range(n_heads):
                                row = (j * (head // LANES) + c) * n_heads + g
                                col = j * attn + g * head + c * LANES
                                wqkv[to, col:col + LANES] = wide[pl.ds(row, chunk, stride=per), :].astype(bf16)

                @pl.when(q + slots < n_parts)
                def _():
                    load(q + slots).start()

                @pl.when(q == n_parts - slots)
                def _():
                    w_copies[0].start()
                    first_start(0)

    pl.run_scoped(opening, pltpu.VMEM((6, dim * (qkv_cols // LANES) // 8, LANES), bf16),
                  pltpu.VMEM((LANES * (qkv_cols // LANES), LANES), f32))

    @pl.loop(0, batch)
    def _(s):
        def scope(qkv):
            with jax.named_scope("A"):
                phase_a(s, qkv)

            @pl.when(s > 0)
            def _():
                rows_start(s, 0)
            with jax.named_scope("B"):
                phase_b(qkv)
        pl.run_scoped(scope, pltpu.VMEM((seq, qkv_cols), bf16))
        with jax.named_scope("D"):
            phase_d(s)

    def finish(buf, out):
        n_steps, depth, n_out = batch * PARTS, buf.shape[0], out.shape[0]

        def rows_at(n):
            return n // PARTS, pl.ds(pl.multiple_of((n % PARTS) * part, part), part)

        def loads(n):
            s, at = rows_at(n)
            return [pltpu.make_async_copy(src.at[s, at], buf.at[n % depth, i], y_sem.at[n % depth, i])
                    for i, src in enumerate((own_out, left_out, right_out, x_ref))]

        def store(n):
            s, at = rows_at(n)
            return pltpu.make_async_copy(out.at[n % n_out], y_ref.at[s, at], z_sem.at[n % n_out])

        def begin(n):
            @pl.when(n % PARTS == 0)
            def _():
                with jax.named_scope("last_wait"):
                    for j in range(NJ):
                        to_right(n // PARTS, 2, j).wait_recv()
                        to_left(n // PARTS, 2, j).wait_recv()
            for cp in loads(n):
                cp.start()

        def sweep(start, stop):
            for n in range(start, start + depth):
                begin(n)

            @pl.loop(start, stop)
            def _(n):
                k = n % depth
                for cp in loads(n):
                    cp.wait()

                @pl.when(n >= n_out)
                def _():
                    store(n - n_out).wait()
                for c in range(0, dim, ncol):
                    own, from_left, from_right, x = (buf[k, i, :, c:c + ncol].astype(f32) for i in range(PARTS))
                    branch = (own + from_left + from_right).astype(bf16)
                    out[n % n_out, :, c:c + ncol] = (x + branch.astype(f32)).astype(bf16)
                store(n).start()

                @pl.when(n + depth < stop)
                def _():
                    begin(n + depth)

        sweep(0, n_steps - PARTS)
        sweep(n_steps - PARTS, n_steps)
        for n in range(n_steps - n_out, n_steps):
            store(n).wait()

    with jax.named_scope("finish"):
        pl.run_scoped(finish, pltpu.VMEM((PARTS, PARTS, part, dim), bf16), pltpu.VMEM((3, part, dim), bf16))

    @pl.loop(0, batch)
    def _(s):
        for j in range(NJ):
            to_right(s, 2, j).wait_send()
            to_left(s, 2, j).wait_send()
            transit(s, j, right).wait_send()
        for u in range(2 * n_chips):
            d, hf = unit(u)
            d2d_copy(s, u, d, hf, core).wait_send()
            if u >= 2:
                ici_copy(s, u, d, hf, right).wait_send()


def layer_call(x_blk, ln_gain, ln_bias, wqkv, w_out, w_up, w_down, n_tp):
    batch, rows, dim = x_blk.shape
    ff, attn, qkv_cols = w_up.shape[1], w_out.shape[0], wqkv.shape[0] * LANES // dim
    n_chips = n_tp // 2
    ncol = dim // NJ
    bf16 = jnp.bfloat16
    dma = pltpu.SemaphoreType.DMA
    flops = 2 * batch * n_tp * rows * dim * (qkv_cols + 2 * ff + attn)
    outs = pl.pallas_call(
        layer_kernel,
        name="parallel_layer",
        out_shape=[
            jax.ShapeDtypeStruct((batch, rows, dim), bf16),
            jax.ShapeDtypeStruct((batch, rows, dim), bf16),
            jax.ShapeDtypeStruct((batch, rows, dim), bf16),
            jax.ShapeDtypeStruct((batch, rows, dim), bf16),
            jax.ShapeDtypeStruct((batch, n_chips, 2, rows, dim), bf16),
            jax.ShapeDtypeStruct((n_tp, rows, ff + attn), bf16),
            jax.ShapeDtypeStruct((batch, 4, NJ, rows, ncol), bf16),
            jax.ShapeDtypeStruct((batch, 3, rows, dim), bf16),
            jax.ShapeDtypeStruct((batch, rows, dim), bf16),
        ],
        in_specs=[pl.BlockSpec(memory_space=pl.ANY)] * N_IN,
        out_specs=[pl.BlockSpec(memory_space=pl.ANY)] * N_OUT,
        scratch_shapes=[
            pltpu.VMEM((dim, qkv_cols), bf16), pltpu.VMEM((dim, ff), bf16), pltpu.VMEM((ff + attn, dim), bf16),
            pltpu.VMEM((1, dim), jnp.float32), pltpu.VMEM((1, dim), jnp.float32), pltpu.VMEM((2, rows, dim), bf16),
            dma((batch, 8)), dma((batch, 8)), dma((batch, 8)), dma((batch, 8)),
            dma((NJ,)), dma((batch, 4 * NJ)), dma((batch, NJ)), dma((batch, NJ)),
            dma((batch, 2 * NJ)), dma((batch, 2 * NJ)),
            dma((3,)), dma((2,)), dma((2, 4)), dma((2,)), dma((2,)), dma((n_tp,)), dma((4, 2)), dma((NJ,)), dma((NJ,)),
            dma((2,)), dma((PARTS, PARTS)), dma((3,)),
        ],
        compiler_params=pltpu.CompilerParams(
            collective_id=0, has_side_effects=True, vmem_limit_bytes=67043328),
        cost_estimate=pl.CostEstimate(flops=flops, bytes_accessed=256 << 20, transcendentals=0),
    )(x_blk, ln_gain.reshape(1, dim), ln_bias.reshape(1, dim), wqkv, w_out, w_up, w_down)
    return outs[0]


def solution(mesh):
    n_tp = mesh.shape["tp"]

    def local_layer(x_blk, ln_gain, ln_bias, w_qkv, w_out, w_up, w_down):
        dim = x_blk.shape[2]
        groups, kinds, head = w_qkv.shape[1:]
        wqkv = w_qkv.reshape(dim, groups, kinds, head // LANES, LANES).transpose(0, 2, 3, 1, 4).reshape(-1, LANES)
        return layer_call(x_blk, ln_gain, ln_bias, wqkv, w_out, w_up, w_down, n_tp)

    return jax.shard_map(
        local_layer, mesh=mesh,
        in_specs=(P("dp", "tp", None), P(), P(), P(None, "tp", None, None),
                  P("tp", None), P(None, "tp"), P("tp", None)),
        out_specs=P("dp", "tp", None), check_vma=False)
```

```python
import functools

import jax
import jax.numpy as jnp
from jax import lax
from jax.experimental import pallas as pl
from jax.experimental.pallas import tpu as pltpu
from jax.sharding import PartitionSpec as P

LN_EPS = 1e-5
LOG2_E = 1.4426950408889634
BOTH, PARTS = (0, 1), 4
N_IN, N_OUT, LANES, WIDE = 7, 9, 128, 512
PARTNER_GROUPS, OWN_GROUPS = (0, 2, 3, 5), (1, 3, 4, 6)
NJ = 4


def any_of(value, choices):
    return functools.reduce(jnp.logical_or, [value == c for c in choices])


def layer_kernel(x_ref, gain_ref, bias_ref, wqkv_hbm, wout_hbm, wup_hbm, wdown_hbm,
                 y_ref, own_out, left_out, right_out, n_all, ho, pbuf, pout, tin,
                 wqkv, wup, wdo, gain, bias, nbuf,
                 ag_is, ag_ir, ag_ds, ag_dr, p_s, p_r, t_s, t_r, m_s, m_r,
                 w_sem, v_sem, ln_sem, a_sem, h_sem, o_sem, d_sem, pb_sem, os_sem, f_sem, y_sem, z_sem):
    batch, rows, dim = x_ref.shape
    half = rows // 2
    ff = wup.shape[1]
    attn = wdo.shape[0] - ff
    qkv_cols = wqkv.shape[1]
    n_heads = 2
    head = attn // n_heads
    n_chips = n_all.shape[1]
    seq = n_chips * 2 * rows
    ncol = dim // NJ
    f32, bf16 = jnp.float32, jnp.bfloat16

    me = lax.axis_index("tp")
    chip, core = me // 2, me % 2
    other = 1 - core
    partner = chip * 2 + other
    right = ((chip + 1) % n_chips) * 2 + core
    left = ((chip + n_chips - 1) % n_chips) * 2 + core

    def remote(src, dst, send, recv, dev):
        return pltpu.make_async_remote_copy(
            src_ref=src, dst_ref=dst, send_sem=send, recv_sem=recv,
            device_id={"tp": dev}, device_id_type=pl.DeviceIdType.MESH)

    barrier = pltpu.get_barrier_semaphore()
    for dev in (partner, right, left):
        pl.semaphore_signal(barrier, inc=1, device_id={"tp": dev}, device_id_type=pl.DeviceIdType.MESH)

    w_copies = (
        pltpu.make_async_copy(wup_hbm, wup, w_sem.at[0]),
        pltpu.make_async_copy(wdown_hbm, wdo.at[pl.ds(0, ff)], w_sem.at[1]),
        pltpu.make_async_copy(wout_hbm, wdo.at[pl.ds(ff, attn)], w_sem.at[2]),
    )
    v_copies = (pltpu.make_async_copy(gain_ref, gain, v_sem.at[0]),
                pltpu.make_async_copy(bias_ref, bias, v_sem.at[1]))
    for cp in v_copies:
        cp.start()

    def unit(u):
        g, b = u // 2, u % 2
        near = (g * (3 - g)) // 2
        off = near * (2 * b - 1) + 2 * (g // 3)
        hf = (b + near * (g - 1)) % 2
        return (chip + off + n_chips) % n_chips, hf

    def piece(s, d, hf, k):
        return n_all.at[s, d, hf, pl.ds(pl.multiple_of(k * half, half), half)]

    def ici_copy(s, u, d, hf, dev):
        return remote(piece(s, d, hf, core), piece(s, d, hf, core), ag_is.at[s, u], ag_ir.at[s, u], dev)

    def d2d_copy(s, u, d, hf, k):
        return remote(piece(s, d, hf, k), piece(s, d, hf, k), ag_ds.at[s, u], ag_dr.at[s, u], partner)

    part = rows // PARTS

    def x_load(s, buf, q):
        at = pl.ds(q * part, part)
        return pltpu.make_async_copy(x_ref.at[s, at], buf.at[at], ln_sem.at[0, q])

    def n_store(s, buf, q):
        dst = n_all.at[s, chip, q // 2, pl.ds(pl.multiple_of(core * half + (q % 2) * part, part), part)]
        return pltpu.make_async_copy(buf.at[pl.ds(q * part, part)], dst, ln_sem.at[1, q])

    def x_start(s, buf):
        for q in range(PARTS):
            x_load(s, buf, q).start()

    def normalise(s, buf, q):
        x_load(s, buf, q).wait()
        at = pl.ds(q * part, part)
        lanes, wide = LANES, WIDE
        total = jnp.zeros((part, lanes), f32)
        for c in range(0, dim, wide):
            v = buf[at, c:c + wide].astype(f32)
            for k in range(0, wide, lanes):
                total = total + v[:, k:k + lanes]
        mean = jnp.sum(total, axis=-1, keepdims=True) * (1.0 / dim)
        total = jnp.zeros((part, lanes), f32)
        for c in range(0, dim, wide):
            cen = buf[at, c:c + wide].astype(f32) - mean
            for k in range(0, wide, lanes):
                total = total + cen[:, k:k + lanes] * cen[:, k:k + lanes]
        inv = lax.rsqrt(jnp.sum(total, axis=-1, keepdims=True) * (1.0 / dim) + LN_EPS)
        for c in range(0, dim, wide):
            cen = buf[at, c:c + wide].astype(f32) - mean
            buf[at, c:c + wide] = (cen * inv * gain[:, c:c + wide] + bias[:, c:c + wide]).astype(bf16)
        n_store(s, buf, q).start()

    def ag_first(s):
        ici_copy(s, 2, chip, 0, right).start()
        ici_copy(s, 3, chip, 1, left).start()
        d2d_copy(s, 0, chip, 0, core).start()
        d2d_copy(s, 1, chip, 1, core).start()

    def ag_second(s):
        ici_copy(s, 4, chip, 1, right).start()
        ici_copy(s, 5, chip, 0, left).start()

    def forward(s, us):
        for u in us:
            d, hf = unit(u)
            with jax.named_scope(f"ici_wait_{u}"):
                ici_copy(s, u, d, hf, right).wait_recv()
            if u == 2:
                ici_copy(s, 6, d, hf, right).start()
            if u == 3:
                ici_copy(s, 7, d, hf, left).start()
            d2d_copy(s, u, d, hf, core).start()

    def block(b, second):
        near = (b * (3 - b)) // 2
        plus = (near * (1 + (2 * second - 1) * (3 - 2 * b))) // 2
        return 2 * plus, 1 + 2 * plus + b // 3

    def cols(j):
        return pl.ds(pl.multiple_of(j * ncol, ncol), ncol)

    def to_right(s, ii, j):
        return remote(pout.at[s, ii, :, cols(j)], left_out.at[s, :, cols(j)], m_s.at[s, j], m_r.at[s, j], right)

    def to_left(s, ii, j):
        return remote(pout.at[s, ii, :, cols(j)], right_out.at[s, :, cols(j)], m_s.at[s, NJ + j], m_r.at[s, NJ + j],
                      left)

    def transit(s, j, dev):
        return remote(pout.at[s, 0, :, cols(j)], tin.at[s, :, cols(j)], t_s.at[s, j], t_r.at[s, j], dev)

    def first_load(s):
        return pltpu.make_async_copy(n_all.at[s, chip, 0], nbuf.at[0], a_sem.at[0])

    def first_start(s):
        with jax.named_scope("d2d_wait"):
            d2d_copy(s, 0, chip, 0, other).wait_recv()
        first_load(s).start()

    def gelu(h):
        return (0.5 * h * (1.0 + lax.erf(h * (2.0 ** -0.5)))).astype(bf16)

    def phase_a(s, qkv):
        def scope(hbuf):
            first, later = s == 0, s > 0

            def load(u):
                d, hf = unit(u)
                return pltpu.make_async_copy(n_all.at[s, d, hf], nbuf.at[u % 2], a_sem.at[u % 2])

            def arrived(u):
                d, hf = unit(u)
                with jax.named_scope("d2d_wait"):
                    d2d_copy(s, u, d, hf, other).wait_recv()

            def hstore(u, k):
                d, hf = unit(u)
                return pltpu.make_async_copy(
                    hbuf.at[pl.ds(k * half, half)],
                    ho.at[2 * d + k, pl.ds(pl.multiple_of(hf * half, half), half), pl.ds(0, ff)],
                    h_sem.at[k])

            def project(u):
                d, hf = unit(u)
                wide = WIDE
                for c in range(0, qkv_cols, wide):
                    r = jnp.dot(nbuf[u % 2], wqkv[:, c:c + wide], preferred_element_type=f32).astype(bf16)
                    for k in BOTH:
                        pos = pl.multiple_of(d * (2 * rows) + k * rows + hf * half, half)
                        qkv[pl.ds(pos, half), c:c + wide] = r[k * half:(k + 1) * half]

            @pl.loop(0, 2 * n_chips)
            def _(u):
                odd = u % 2 == 1
                with jax.named_scope("load_wait"):
                    load(u).wait()

                @pl.when(jnp.logical_and(later, u == 4))
                def _():
                    forward(s, (6, 7))

                @pl.when(jnp.logical_or(jnp.logical_and(later, u < 7), u % 2 == 0))
                def _():
                    arrived(u + 1)
                    load(u + 1).start()

                @pl.when(later)
                def _():
                    project(u)

                @pl.when(first)
                def _():
                    @pl.when(jnp.logical_and(odd, u < 7))
                    def _():
                        x_start((u + 1) // 2, nbuf.at[0])

                    project(u)

                    @pl.when(u == 0)
                    def _():
                        w_copies[0].wait()
                        for cp in w_copies[1:]:
                            cp.start()

                    @pl.when(u >= 1)
                    def _():
                        for k in BOTH:
                            hstore(u - 1, k).wait()
                    hbuf[...] = gelu(jnp.dot(nbuf[u % 2], wup[...], preferred_element_type=f32))
                    for k in BOTH:
                        hstore(u, k).start()

                    @pl.when(u == 1)
                    def _():
                        forward(0, (2, 3))

                    @pl.when(u == 3)
                    def _():
                        forward(0, (4, 5))

                    @pl.when(u == 5)
                    def _():
                        forward(0, (6, 7))

                    @pl.when(jnp.logical_and(odd, u < 7))
                    def _():
                        with jax.named_scope("norm"):
                            for q in range(PARTS):
                                normalise((u + 1) // 2, nbuf.at[0], q)
                            for q in range(PARTS):
                                n_store((u + 1) // 2, nbuf.at[0], q).wait()

                        @pl.when(u == 1)
                        def _():
                            ag_first(1)
                            ag_second(1)
                        arrived(u + 1)
                        load(u + 1).start()

            @pl.when(first)
            def _():
                for k in BOTH:
                    hstore(7, k).wait()
        pl.run_scoped(scope, pltpu.VMEM((rows, ff), bf16))

    def phase_b(qkv):
        def ostore(t):
            return pltpu.make_async_copy(qkv.at[pl.ds(t * rows, rows), pl.ds(0, attn)],
                                         ho.at[t, :, pl.ds(ff, attn)], o_sem.at[t])
        scale = head ** -0.5

        probs = nbuf.at[1]

        def scope(*scores):
            keep = (lax.broadcasted_iota(jnp.int32, (rows, rows), 0)
                    >= lax.broadcasted_iota(jnp.int32, (rows, rows), 1))
            tasks = [(t, h) for t in range(seq // rows) for h in range(n_heads)]
            tops = {}

            def score(i):
                t, h = tasks[i]
                r0, n = t * rows, (t + 1) * rows
                q = qkv[r0:n, h * head:(h + 1) * head]
                k = qkv[0:n, attn + h * head:attn + (h + 1) * head]
                sc = lax.dot_general(q, k, (((1,), (1,)), ((), ())), preferred_element_type=f32)
                diag = jnp.where(keep, sc[:, r0:], -jnp.inf)
                top = jnp.max(diag, axis=1, keepdims=True)
                if t:
                    scores[i % 2][0, :, 0:r0] = sc[:, :r0]
                    top = jnp.maximum(top, jnp.max(sc[:, :r0], axis=1, keepdims=True))
                scores[i % 2][0, :, r0:n] = diag
                tops[i] = top

            def soften(i):
                t, h = tasks[i]
                n = (t + 1) * rows
                total = jnp.zeros((rows, rows // 2), f32)
                for c in range(0, n, rows):
                    e = jnp.exp2((scores[i % 2][0, :, c:c + rows] - tops[i]) * (scale * LOG2_E))
                    scores[i % 2][0, :, c:c + rows] = e
                    total = total + e[:, :rows // 2] + e[:, rows // 2:]
                inverse = 1.0 / jnp.sum(total, axis=1, keepdims=True)
                for c in range(0, n, rows):
                    probs[:, (i % 2) * seq + c:(i % 2) * seq + c + rows] = (
                        scores[i % 2][0, :, c:c + rows] * inverse).astype(bf16)

            def mix(i):
                t, h = tasks[i]
                r0, n = t * rows, (t + 1) * rows
                v = qkv[0:n, 2 * attn + h * head:2 * attn + (h + 1) * head]
                o = jnp.dot(probs[:, (i % 2) * seq:(i % 2) * seq + n], v, preferred_element_type=f32)
                qkv[r0:n, h * head:(h + 1) * head] = o.astype(bf16)

            score(0)
            for i in range(len(tasks)):
                if i + 1 < len(tasks):
                    score(i + 1)
                soften(i)
                mix(i)
                if i % n_heads == n_heads - 1 and tasks[i][0] % PARTS == PARTS - 1:
                    for done in range(tasks[i][0] - PARTS + 1, tasks[i][0] + 1):
                        ostore(done).start()
            for t in range(seq // rows):
                ostore(t).wait()
        pl.run_scoped(scope, pltpu.VMEM((1, rows, seq), f32), pltpu.VMEM((1, rows, seq), f32))

    def chip_of(w):
        near = (w * (3 - w)) // 2
        off = near * (3 - 2 * w) + 2 * ((3 - w) // 3)
        plus = near * (2 - w)
        return (chip + off + n_chips) % n_chips, 2 * plus, 1 + 2 * plus + w // 3

    def place_of(v):
        return (v % 3) * (2 - v % 3)

    def rows_load(s, v):
        d, _, _ = chip_of(v // 2)
        return pltpu.make_async_copy(n_all.at[s, d, v % 2], nbuf.at[place_of(v)], a_sem.at[place_of(v)])

    def rows_start(s, v):
        rows_load(s, v).start()

    def phase_d(s):
        def scope(lhs, pst, ost, tb):
            first, later, last = s == 0, s > 0, s == batch - 1

            def left_load(w, own, whole):
                d, slot_p, slot_o = chip_of(w)
                src = ho.at[2 * d + (core if own else other)]
                dst = lhs.at[slot_o if own else slot_p]
                if not whole:
                    src, dst = src.at[:, pl.ds(ff, attn)], dst.at[:, pl.ds(ff, attn)]
                return pltpu.make_async_copy(src, dst, d_sem.at[w, own])

            def left_act(w, own, act):
                @pl.when(first)
                def _():
                    act(left_load(w, own, True))

                @pl.when(later)
                def _():
                    act(left_load(w, own, False))

            def left_start(w, own):
                left_act(w, own, lambda cp: cp.start())

            def left_wait(w, own):
                left_act(w, own, lambda cp: cp.wait())

            def hide(v):
                _, slot_p, slot_o = chip_of(v // 2)
                at = pl.multiple_of((v % 2) * half, half)
                wide = WIDE
                for c in range(0, ff, wide):
                    r = gelu(jnp.dot(nbuf[place_of(v)], wup[:, c:c + wide], preferred_element_type=f32))
                    for k in BOTH:
                        own = 1 - (k + core) % 2
                        slot = slot_p + own * (slot_o - slot_p)
                        lhs[slot, pl.ds(at, half), c:c + wide] = r[k * half:(k + 1) * half]

            def nth(i, k):
                return 2 * i + k

            def swap(b, t, c):
                n = nth(t, c)
                return remote(pst.at[n], pbuf.at[s, b, n], p_s.at[n], p_r.at[s, b * NJ + n], partner)

            def pb_at(t, c):
                return nbuf.at[1, :, cols(nth(t, c))]

            def pb_load(b, t, c):
                return pltpu.make_async_copy(pbuf.at[s, b, nth(t, c)], pb_at(t, c), pb_sem.at[nth(t, c)])

            def pb_start(b, t):
                for c in BOTH:
                    with jax.named_scope("swap_wait"):
                        swap(b, t, c).wait_recv()
                    pb_load(b, t, c).start()

            def t_load(t, c):
                return pltpu.make_async_copy(tin.at[s, :, cols(nth(c, t))], tb.at[c], f_sem.at[c])

            def stored(t):
                for c in BOTH:
                    pltpu.make_async_copy(ost.at[nth(t, c)], pout.at[s, 0, :, cols(nth(c, t))],
                                          os_sem.at[nth(t, c)]).wait()

            def post(b, t):
                stored(t)

                @pl.when(b == 0)
                def _():
                    transit(s, t, right).start()
                    transit(s, 2 + t, left).start()

                @pl.when(b == 1)
                def _():
                    to_left(s, 1, t).start()
                    to_right(s, 1, 2 + t).start()

                @pl.when(b == 2)
                def _():
                    to_right(s, 2, t).start()
                    to_left(s, 2, 2 + t).start()

            def partner_step(b, t):
                @pl.when(b >= 1)
                def _():
                    for c in BOTH:
                        swap(b - 1, t, c).wait_send()

                @pl.when(jnp.logical_and(b == 2, t == 0))
                def _():
                    pb_start(1, 0)
                for c in BOTH:
                    slot_p, _ = block(b, c)
                    r = jnp.dot(lhs[slot_p], wdo[:, cols(nth(c, t))], preferred_element_type=f32)
                    pst[nth(t, c)] = r.astype(bf16)
                for c in BOTH:
                    swap(b, t, c).start()

                @pl.when(jnp.logical_and(jnp.logical_not(last), jnp.logical_and(b == 2, t == 1)))
                def _():
                    post(1, 0)

            def own_step(b, t):
                @pl.when(jnp.logical_and(b == 3, t == 0))
                def _():
                    pb_start(3, 0)

                late = jnp.logical_and(t == 0, jnp.logical_or(b == 3, jnp.logical_and(first, b == 0)))

                @pl.when(jnp.logical_and(t == 0, jnp.logical_not(late)))
                def _():
                    pb_start(b, 1)

                @pl.when(jnp.logical_and(b == 1, t == 1))
                def _():
                    pb_start(2, 0)

                @pl.when(b == 2)
                def _():
                    with jax.named_scope("transit_wait"):
                        for c in BOTH:
                            transit(s, nth(c, t), right).wait_recv()
                    for c in BOTH:
                        t_load(t, c).start()
                for c in BOTH:
                    pb_load(b, t, c).wait()
                for c in BOTH:
                    _, slot_o = block(b, c)
                    r = jnp.dot(lhs[slot_o], wdo[:, cols(nth(c, t))], preferred_element_type=f32)
                    ost[nth(t, c)] = (r + pb_at(t, c)[...].astype(f32)).astype(bf16)

                @pl.when(b == 2)
                def _():
                    for c in BOTH:
                        t_load(t, c).wait()

                        @pl.loop(0, PARTS)
                        def _(r):
                            at = pl.ds(pl.multiple_of(r * part, part), part)
                            ost[nth(t, c), at, :] = (ost[nth(t, c), at, :].astype(f32)
                                                     + tb[c, at, :].astype(f32)).astype(bf16)

                for c in BOTH:
                    @pl.when(b < 3)
                    def _():
                        pltpu.make_async_copy(ost.at[nth(t, c)], pout.at[s, b, :, cols(nth(c, t))],
                                              os_sem.at[nth(t, c)]).start()

                    @pl.when(b == 3)
                    def _():
                        pltpu.make_async_copy(ost.at[nth(t, c)], own_out.at[s, :, cols(nth(c, t))],
                                              os_sem.at[nth(t, c)]).start()

                @pl.when(late)
                def _():
                    pb_start(b, 1)

                @pl.when(jnp.logical_and(last, jnp.logical_and(b == 1, t == 0)))
                def _():
                    post(1, 0)

                @pl.when(jnp.logical_and(b == 2, t == 0))
                def _():
                    post(1, 1)

                @pl.when(jnp.logical_and(t == 1, b % 2 == 0))
                def _():
                    post(b, 0)

            for w in BOTH:
                for own in BOTH:
                    left_start(w, own)

            @pl.when(first)
            def _():
                w_copies[1].wait()
                w_copies[2].wait()

            n_groups = 7

            def since(g, k):
                return (g + 8 - k) // 8

            def step_of(g, groups):
                return sum(since(g, k) for k in groups[1:])

            def units(g):
                return 2 * since(g, 1) + since(g, 2) + 3 * since(g, 3) + 2 * since(g, 6)

            @pl.loop(0, n_groups)
            def _(g):
                @pl.when(g == 1)
                def _():
                    pb_start(0, 0)
                    left_start(2, 0)

                @pl.when(g == 2)
                def _():
                    left_start(2, 1)

                @pl.when(g == 3)
                def _():
                    left_wait(1, 1)
                    left_wait(2, 1)

                @pl.when(g == 4)
                def _():
                    left_start(3, 0)
                    left_start(3, 1)

                @pl.when(later)
                def _():
                    @pl.loop(units(g), units(g + 1))
                    def _(v):
                        with jax.named_scope("n_wait"):
                            rows_load(s, v).wait()

                        @pl.when(jnp.logical_and(v % 3 != 2, v < 2 * n_chips - 1))
                        def _():
                            rows_start(s, v + 1)

                        @pl.when(jnp.logical_and(v == 2 * n_chips - 1, s < batch - 1))
                        def _():
                            first_start(s + 1)
                        with jax.named_scope("hide"):
                            hide(v)

                        @pl.when(v % 3 == 2)
                        def _():
                            rows_start(s, v + 1)

                        @pl.when(v == 3)
                        def _():
                            post(0, 1)

                        @pl.when(v == 6)
                        def _():
                            post(2, 1)

                @pl.when(g == 0)
                def _():
                    left_wait(0, 0)

                @pl.when(g == 1)
                def _():
                    left_wait(0, 1)

                @pl.when(g == 2)
                def _():
                    left_wait(1, 0)
                    left_wait(2, 0)

                @pl.when(g == 5)
                def _():
                    left_wait(3, 0)
                    left_wait(3, 1)

                @pl.when(first)
                def _():
                    @pl.when(g == 2)
                    def _():
                        post(0, 1)

                    @pl.when(g == 5)
                    def _():
                        post(2, 1)

                    @pl.when(g == 6)
                    def _():
                        first_start(s + 1)

                @pl.loop(0, 2)
                def _(t):
                    @pl.when(any_of(g, PARTNER_GROUPS))
                    def _():
                        with jax.named_scope("partner"):
                            partner_step(step_of(g, PARTNER_GROUPS), t)

                    @pl.when(any_of(g, OWN_GROUPS))
                    def _():
                        with jax.named_scope("own"):
                            own_step(step_of(g, OWN_GROUPS), t)

                @pl.when(jnp.logical_and(s < batch - 1, g == 2))
                def _():
                    @pl.when(later)
                    def _():
                        ag_second(s + 1)
                    forward(s + 1, (2, 3))

                @pl.when(jnp.logical_and(s < batch - 1, g == n_groups - 1))
                def _():
                    forward(s + 1, (4, 5))

            stored(0)
            stored(1)
            for t in BOTH:
                for c in BOTH:
                    swap(3, t, c).wait_send()

            @pl.when(s < batch - 2)
            def _():
                ag_first(s + 2)
        pl.run_scoped(scope, pltpu.VMEM((4, rows, ff + attn), bf16), pltpu.VMEM((NJ, rows, ncol), bf16),
                      pltpu.VMEM((NJ, rows, ncol), bf16), pltpu.VMEM((2, rows, ncol), bf16))

    def opening(raw, wide):
        kinds = qkv_cols // attn
        per = qkv_cols // LANES
        slots, part_rows = raw.shape[0], raw.shape[1]
        n_parts = dim * per // part_rows
        chunk = wide.shape[0] // per
        chunks = part_rows // (chunk * per)
        xbuf = nbuf.at[1]

        def load(q):
            at = pl.ds(pl.multiple_of(q * part_rows, part_rows), part_rows)
            return pltpu.make_async_copy(wqkv_hbm.at[at], raw.at[q % slots], o_sem.at[q])

        x_start(0, xbuf)
        for q in range(slots):
            load(q).start()
        for cp in v_copies:
            cp.wait()
        with jax.named_scope("send0"):
            for q in range(PARTS):
                normalise(0, xbuf, q)
                if q == 1:
                    n_store(0, xbuf, 0).wait()
                    n_store(0, xbuf, 1).wait()
                    pl.semaphore_wait(barrier, 3)
                    ici_copy(0, 2, chip, 0, right).start()
                    d2d_copy(0, 0, chip, 0, core).start()
            n_store(0, xbuf, 2).wait()
            n_store(0, xbuf, 3).wait()
            ici_copy(0, 3, chip, 1, left).start()
            d2d_copy(0, 1, chip, 1, core).start()
            ag_second(0)
        with jax.named_scope("place"):
            @pl.loop(0, n_parts)
            def _(q):
                load(q).wait()

                @pl.loop(0, chunks)
                def _(i):
                    at = pl.ds(pl.multiple_of(i * (chunk * per), chunk * per), chunk * per)
                    wide[...] = raw[q % slots, at, :].astype(f32)
                    to = pl.ds(pl.multiple_of((q * chunks + i) * chunk, chunk), chunk)
                    for j in range(kinds):
                        for c in range(head // LANES):
                            for g in range(n_heads):
                                row = (j * (head // LANES) + c) * n_heads + g
                                col = j * attn + g * head + c * LANES
                                wqkv[to, col:col + LANES] = wide[pl.ds(row, chunk, stride=per), :].astype(bf16)

                @pl.when(q + slots < n_parts)
                def _():
                    load(q + slots).start()

                @pl.when(q == n_parts - slots)
                def _():
                    w_copies[0].start()
                    first_start(0)

    pl.run_scoped(opening, pltpu.VMEM((6, dim * (qkv_cols // LANES) // 8, LANES), bf16),
                  pltpu.VMEM((LANES * (qkv_cols // LANES), LANES), f32))

    @pl.loop(0, batch)
    def _(s):
        def scope(qkv):
            with jax.named_scope("A"):
                phase_a(s, qkv)

            @pl.when(s > 0)
            def _():
                rows_start(s, 0)
            with jax.named_scope("B"):
                phase_b(qkv)
        pl.run_scoped(scope, pltpu.VMEM((seq, qkv_cols), bf16))
        with jax.named_scope("D"):
            phase_d(s)

    def finish(buf, out):
        n_steps, depth, n_out = batch * PARTS, buf.shape[0], out.shape[0]

        def rows_at(n):
            return n // PARTS, pl.ds(pl.multiple_of((n % PARTS) * part, part), part)

        def loads(n):
            s, at = rows_at(n)
            return [pltpu.make_async_copy(src.at[s, at], buf.at[n % depth, i], y_sem.at[n % depth, i])
                    for i, src in enumerate((own_out, left_out, right_out, x_ref))]

        def store(n):
            s, at = rows_at(n)
            return pltpu.make_async_copy(out.at[n % n_out], y_ref.at[s, at], z_sem.at[n % n_out])

        def begin(n):
            @pl.when(n % PARTS == 0)
            def _():
                with jax.named_scope("last_wait"):
                    for j in range(NJ):
                        to_right(n // PARTS, 2, j).wait_recv()
                        to_left(n // PARTS, 2, j).wait_recv()
            for cp in loads(n):
                cp.start()

        def sweep(start, stop):
            for n in range(start, start + depth):
                begin(n)

            @pl.loop(start, stop)
            def _(n):
                k = n % depth
                for cp in loads(n):
                    cp.wait()

                @pl.when(n >= n_out)
                def _():
                    store(n - n_out).wait()
                for c in range(0, dim, ncol):
                    own, from_left, from_right, x = (buf[k, i, :, c:c + ncol].astype(f32) for i in range(PARTS))
                    branch = (own + from_left + from_right).astype(bf16)
                    out[n % n_out, :, c:c + ncol] = (x + branch.astype(f32)).astype(bf16)
                store(n).start()

                @pl.when(n + depth < stop)
                def _():
                    begin(n + depth)

        sweep(0, n_steps - PARTS)
        sweep(n_steps - PARTS, n_steps)
        for n in range(n_steps - n_out, n_steps):
            store(n).wait()

    with jax.named_scope("finish"):
        pl.run_scoped(finish, pltpu.VMEM((PARTS, PARTS, part, dim), bf16), pltpu.VMEM((3, part, dim), bf16))

    @pl.loop(0, batch)
    def _(s):
        for j in range(NJ):
            to_right(s, 2, j).wait_send()
            to_left(s, 2, j).wait_send()
            transit(s, j, right).wait_send()
        for u in range(2 * n_chips):
            d, hf = unit(u)
            d2d_copy(s, u, d, hf, core).wait_send()
            if u >= 2:
                ici_copy(s, u, d, hf, right).wait_send()


def layer_call(x_blk, ln_gain, ln_bias, wqkv, w_out, w_up, w_down, n_tp):
    batch, rows, dim = x_blk.shape
    ff, attn, qkv_cols = w_up.shape[1], w_out.shape[0], wqkv.shape[0] * LANES // dim
    n_chips = n_tp // 2
    ncol = dim // NJ
    bf16 = jnp.bfloat16
    dma = pltpu.SemaphoreType.DMA
    flops = 2 * batch * n_tp * rows * dim * (qkv_cols + 2 * ff + attn)
    outs = pl.pallas_call(
        layer_kernel,
        name="parallel_layer",
        out_shape=[
            jax.ShapeDtypeStruct((batch, rows, dim), bf16),
            jax.ShapeDtypeStruct((batch, rows, dim), bf16),
            jax.ShapeDtypeStruct((batch, rows, dim), bf16),
            jax.ShapeDtypeStruct((batch, rows, dim), bf16),
            jax.ShapeDtypeStruct((batch, n_chips, 2, rows, dim), bf16),
            jax.ShapeDtypeStruct((n_tp, rows, ff + attn), bf16),
            jax.ShapeDtypeStruct((batch, 4, NJ, rows, ncol), bf16),
            jax.ShapeDtypeStruct((batch, 3, rows, dim), bf16),
            jax.ShapeDtypeStruct((batch, rows, dim), bf16),
        ],
        in_specs=[pl.BlockSpec(memory_space=pl.ANY)] * N_IN,
        out_specs=[pl.BlockSpec(memory_space=pl.ANY)] * N_OUT,
        scratch_shapes=[
            pltpu.VMEM((dim, qkv_cols), bf16), pltpu.VMEM((dim, ff), bf16), pltpu.VMEM((ff + attn, dim), bf16),
            pltpu.VMEM((1, dim), jnp.float32), pltpu.VMEM((1, dim), jnp.float32), pltpu.VMEM((2, rows, dim), bf16),
            dma((batch, 8)), dma((batch, 8)), dma((batch, 8)), dma((batch, 8)),
            dma((NJ,)), dma((batch, 4 * NJ)), dma((batch, NJ)), dma((batch, NJ)),
            dma((batch, 2 * NJ)), dma((batch, 2 * NJ)),
            dma((3,)), dma((2,)), dma((2, 4)), dma((2,)), dma((2,)), dma((n_tp,)), dma((4, 2)), dma((NJ,)), dma((NJ,)),
            dma((2,)), dma((PARTS, PARTS)), dma((3,)),
        ],
        compiler_params=pltpu.CompilerParams(
            collective_id=0, has_side_effects=True, vmem_limit_bytes=67043328),
        cost_estimate=pl.CostEstimate(flops=flops, bytes_accessed=256 << 20, transcendentals=0),
    )(x_blk, ln_gain.reshape(1, dim), ln_bias.reshape(1, dim), wqkv, w_out, w_up, w_down)
    return outs[0]


def solution(mesh):
    n_tp = mesh.shape["tp"]

    def local_layer(x_blk, ln_gain, ln_bias, w_qkv, w_out, w_up, w_down):
        dim = x_blk.shape[2]
        groups, kinds, head = w_qkv.shape[1:]
        wqkv = w_qkv.reshape(dim, groups, kinds, head // LANES, LANES).transpose(0, 2, 3, 1, 4).reshape(-1, LANES)
        return layer_call(x_blk, ln_gain, ln_bias, wqkv, w_out, w_up, w_down, n_tp)

    return jax.shard_map(
        local_layer, mesh=mesh,
        in_specs=(P("dp", "tp", None), P(), P(), P(None, "tp", None, None),
                  P("tp", None), P(None, "tp"), P("tp", None)),
        out_specs=P("dp", "tp", None), check_vma=False)
```

```python
import functools

import jax
import jax.numpy as jnp
from jax import lax
from jax.experimental import pallas as pl
from jax.experimental.pallas import tpu as pltpu
from jax.sharding import PartitionSpec as P

LN_EPS = 1e-5
LOG2_E = 1.4426950408889634
BOTH, PARTS = (0, 1), 4
N_IN, N_OUT, LANES, WIDE = 7, 9, 128, 512
PARTNER_GROUPS, OWN_GROUPS = (0, 2, 3, 5), (1, 3, 4, 6)
NJ = 4


def any_of(value, choices):
    return functools.reduce(jnp.logical_or, [value == c for c in choices])


def layer_kernel(x_ref, gain_ref, bias_ref, wqkv_hbm, wout_hbm, wup_hbm, wdown_hbm,
                 y_ref, own_out, left_out, right_out, n_all, ho, pbuf, pout, tin,
                 wqkv, wup, wdo, gain, bias, nbuf,
                 ag_is, ag_ir, ag_ds, ag_dr, p_s, p_r, t_s, t_r, m_s, m_r,
                 w_sem, v_sem, ln_sem, a_sem, h_sem, o_sem, d_sem, pb_sem, os_sem, f_sem, y_sem, z_sem):
    batch, rows, dim = x_ref.shape
    half = rows // 2
    ff = wup.shape[1]
    attn = wdo.shape[0] - ff
    qkv_cols = wqkv.shape[1]
    n_heads = 2
    head = attn // n_heads
    n_chips = n_all.shape[1]
    seq = n_chips * 2 * rows
    ncol = dim // NJ
    f32, bf16 = jnp.float32, jnp.bfloat16

    me = lax.axis_index("tp")
    chip, core = me // 2, me % 2
    other = 1 - core
    partner = chip * 2 + other
    right = ((chip + 1) % n_chips) * 2 + core
    left = ((chip + n_chips - 1) % n_chips) * 2 + core

    def remote(src, dst, send, recv, dev):
        return pltpu.make_async_remote_copy(
            src_ref=src, dst_ref=dst, send_sem=send, recv_sem=recv,
            device_id={"tp": dev}, device_id_type=pl.DeviceIdType.MESH)

    barrier = pltpu.get_barrier_semaphore()
    for dev in (partner, right, left):
        pl.semaphore_signal(barrier, inc=1, device_id={"tp": dev}, device_id_type=pl.DeviceIdType.MESH)

    w_copies = (
        pltpu.make_async_copy(wup_hbm, wup, w_sem.at[0]),
        pltpu.make_async_copy(wdown_hbm, wdo.at[pl.ds(0, ff)], w_sem.at[1]),
        pltpu.make_async_copy(wout_hbm, wdo.at[pl.ds(ff, attn)], w_sem.at[2]),
    )
    v_copies = (pltpu.make_async_copy(gain_ref, gain, v_sem.at[0]),
                pltpu.make_async_copy(bias_ref, bias, v_sem.at[1]))
    for cp in v_copies:
        cp.start()

    def unit(u):
        g, b = u // 2, u % 2
        near = (g * (3 - g)) // 2
        off = near * (2 * b - 1) + 2 * (g // 3)
        hf = (b + near * (g - 1)) % 2
        return (chip + off + n_chips) % n_chips, hf

    def piece(s, d, hf, k):
        return n_all.at[s, d, hf, pl.ds(pl.multiple_of(k * half, half), half)]

    def ici_copy(s, u, d, hf, dev):
        return remote(piece(s, d, hf, core), piece(s, d, hf, core), ag_is.at[s, u], ag_ir.at[s, u], dev)

    def d2d_copy(s, u, d, hf, k):
        return remote(piece(s, d, hf, k), piece(s, d, hf, k), ag_ds.at[s, u], ag_dr.at[s, u], partner)

    part = rows // PARTS

    def x_load(s, buf, q):
        at = pl.ds(q * part, part)
        return pltpu.make_async_copy(x_ref.at[s, at], buf.at[at], ln_sem.at[0, q])

    def n_store(s, buf, q):
        dst = n_all.at[s, chip, q // 2, pl.ds(pl.multiple_of(core * half + (q % 2) * part, part), part)]
        return pltpu.make_async_copy(buf.at[pl.ds(q * part, part)], dst, ln_sem.at[1, q])

    def x_start(s, buf):
        for q in range(PARTS):
            x_load(s, buf, q).start()

    def normalise(s, buf, q):
        x_load(s, buf, q).wait()
        at = pl.ds(q * part, part)
        lanes, wide = LANES, WIDE
        total = jnp.zeros((part, lanes), f32)
        for c in range(0, dim, wide):
            v = buf[at, c:c + wide].astype(f32)
            for k in range(0, wide, lanes):
                total = total + v[:, k:k + lanes]
        mean = jnp.sum(total, axis=-1, keepdims=True) * (1.0 / dim)
        total = jnp.zeros((part, lanes), f32)
        for c in range(0, dim, wide):
            cen = buf[at, c:c + wide].astype(f32) - mean
            for k in range(0, wide, lanes):
                total = total + cen[:, k:k + lanes] * cen[:, k:k + lanes]
        inv = lax.rsqrt(jnp.sum(total, axis=-1, keepdims=True) * (1.0 / dim) + LN_EPS)
        for c in range(0, dim, wide):
            cen = buf[at, c:c + wide].astype(f32) - mean
            buf[at, c:c + wide] = (cen * inv * gain[:, c:c + wide] + bias[:, c:c + wide]).astype(bf16)
        n_store(s, buf, q).start()

    def ag_first(s):
        ici_copy(s, 2, chip, 0, right).start()
        ici_copy(s, 3, chip, 1, left).start()
        d2d_copy(s, 0, chip, 0, core).start()
        d2d_copy(s, 1, chip, 1, core).start()

    def ag_second(s):
        ici_copy(s, 4, chip, 1, right).start()
        ici_copy(s, 5, chip, 0, left).start()

    def forward(s, us):
        for u in us:
            d, hf = unit(u)
            with jax.named_scope(f"ici_wait_{u}"):
                ici_copy(s, u, d, hf, right).wait_recv()
            if u == 2:
                ici_copy(s, 6, d, hf, right).start()
            if u == 3:
                ici_copy(s, 7, d, hf, left).start()
            d2d_copy(s, u, d, hf, core).start()

    def block(b, second):
        near = (b * (3 - b)) // 2
        plus = (near * (1 + (2 * second - 1) * (3 - 2 * b))) // 2
        return 2 * plus, 1 + 2 * plus + b // 3

    def cols(j):
        return pl.ds(pl.multiple_of(j * ncol, ncol), ncol)

    def to_right(s, ii, j):
        return remote(pout.at[s, ii, :, cols(j)], left_out.at[s, :, cols(j)], m_s.at[s, j], m_r.at[s, j], right)

    def to_left(s, ii, j):
        return remote(pout.at[s, ii, :, cols(j)], right_out.at[s, :, cols(j)], m_s.at[s, NJ + j], m_r.at[s, NJ + j],
                      left)

    def transit(s, j, dev):
        return remote(pout.at[s, 0, :, cols(j)], tin.at[s, :, cols(j)], t_s.at[s, j], t_r.at[s, j], dev)

    def first_load(s):
        return pltpu.make_async_copy(n_all.at[s, chip, 0], nbuf.at[0], a_sem.at[0])

    def first_start(s):
        with jax.named_scope("d2d_wait"):
            d2d_copy(s, 0, chip, 0, other).wait_recv()
        first_load(s).start()

    def gelu(h):
        return (0.5 * h * (1.0 + lax.erf(h * (2.0 ** -0.5)))).astype(bf16)

    def phase_a(s, qkv):
        def scope(hbuf):
            first, later = s == 0, s > 0

            def load(u):
                d, hf = unit(u)
                return pltpu.make_async_copy(n_all.at[s, d, hf], nbuf.at[u % 2], a_sem.at[u % 2])

            def arrived(u):
                d, hf = unit(u)
                with jax.named_scope("d2d_wait"):
                    d2d_copy(s, u, d, hf, other).wait_recv()

            def hstore(u, k):
                d, hf = unit(u)
                return pltpu.make_async_copy(
                    hbuf.at[pl.ds(k * half, half)],
                    ho.at[2 * d + k, pl.ds(pl.multiple_of(hf * half, half), half), pl.ds(0, ff)],
                    h_sem.at[k])

            def project(u):
                d, hf = unit(u)
                wide = WIDE
                for c in range(0, qkv_cols, wide):
                    r = jnp.dot(nbuf[u % 2], wqkv[:, c:c + wide], preferred_element_type=f32).astype(bf16)
                    for k in BOTH:
                        pos = pl.multiple_of(d * (2 * rows) + k * rows + hf * half, half)
                        qkv[pl.ds(pos, half), c:c + wide] = r[k * half:(k + 1) * half]

            @pl.loop(0, 2 * n_chips)
            def _(u):
                odd = u % 2 == 1
                with jax.named_scope("load_wait"):
                    load(u).wait()

                @pl.when(jnp.logical_and(later, u == 4))
                def _():
                    forward(s, (6, 7))

                @pl.when(jnp.logical_or(jnp.logical_and(later, u < 7), u % 2 == 0))
                def _():
                    arrived(u + 1)
                    load(u + 1).start()

                @pl.when(later)
                def _():
                    project(u)

                @pl.when(first)
                def _():
                    @pl.when(jnp.logical_and(odd, u < 7))
                    def _():
                        x_start((u + 1) // 2, nbuf.at[0])

                    project(u)

                    @pl.when(u == 0)
                    def _():
                        w_copies[0].wait()
                        for cp in w_copies[1:]:
                            cp.start()

                    @pl.when(u >= 1)
                    def _():
                        for k in BOTH:
                            hstore(u - 1, k).wait()
                    hbuf[...] = gelu(jnp.dot(nbuf[u % 2], wup[...], preferred_element_type=f32))
                    for k in BOTH:
                        hstore(u, k).start()

                    @pl.when(u == 1)
                    def _():
                        forward(0, (2, 3))

                    @pl.when(u == 3)
                    def _():
                        forward(0, (4, 5))

                    @pl.when(u == 5)
                    def _():
                        forward(0, (6, 7))

                    @pl.when(jnp.logical_and(odd, u < 7))
                    def _():
                        with jax.named_scope("norm"):
                            for q in range(PARTS):
                                normalise((u + 1) // 2, nbuf.at[0], q)
                            for q in range(PARTS):
                                n_store((u + 1) // 2, nbuf.at[0], q).wait()

                        @pl.when(u == 1)
                        def _():
                            ag_first(1)
                            ag_second(1)
                        arrived(u + 1)
                        load(u + 1).start()

            @pl.when(first)
            def _():
                for k in BOTH:
                    hstore(7, k).wait()
        pl.run_scoped(scope, pltpu.VMEM((rows, ff), bf16))

    def phase_b(qkv):
        def ostore(t):
            return pltpu.make_async_copy(qkv.at[pl.ds(t * rows, rows), pl.ds(0, attn)],
                                         ho.at[t, :, pl.ds(ff, attn)], o_sem.at[t])
        scale = head ** -0.5

        probs = nbuf.at[1]

        def scope(*scores):
            keep = (lax.broadcasted_iota(jnp.int32, (rows, rows), 0)
                    >= lax.broadcasted_iota(jnp.int32, (rows, rows), 1))
            tasks = [(t, h) for t in range(seq // rows) for h in range(n_heads)]
            tops = {}

            def score(i):
                t, h = tasks[i]
                r0, n = t * rows, (t + 1) * rows
                q = qkv[r0:n, h * head:(h + 1) * head]
                k = qkv[0:n, attn + h * head:attn + (h + 1) * head]
                sc = lax.dot_general(q, k, (((1,), (1,)), ((), ())), preferred_element_type=f32)
                diag = jnp.where(keep, sc[:, r0:], -jnp.inf)
                top = jnp.max(diag, axis=1, keepdims=True)
                if t:
                    scores[i % 2][0, :, 0:r0] = sc[:, :r0]
                    top = jnp.maximum(top, jnp.max(sc[:, :r0], axis=1, keepdims=True))
                scores[i % 2][0, :, r0:n] = diag
                tops[i] = top

            def soften(i):
                t, h = tasks[i]
                n = (t + 1) * rows
                total = jnp.zeros((rows, rows // 2), f32)
                for c in range(0, n, rows):
                    e = jnp.exp2((scores[i % 2][0, :, c:c + rows] - tops[i]) * (scale * LOG2_E))
                    scores[i % 2][0, :, c:c + rows] = e
                    total = total + e[:, :rows // 2] + e[:, rows // 2:]
                inverse = 1.0 / jnp.sum(total, axis=1, keepdims=True)
                for c in range(0, n, rows):
                    probs[:, (i % 2) * seq + c:(i % 2) * seq + c + rows] = (
                        scores[i % 2][0, :, c:c + rows] * inverse).astype(bf16)

            def mix(i):
                t, h = tasks[i]
                r0, n = t * rows, (t + 1) * rows
                v = qkv[0:n, 2 * attn + h * head:2 * attn + (h + 1) * head]
                o = jnp.dot(probs[:, (i % 2) * seq:(i % 2) * seq + n], v, preferred_element_type=f32)
                qkv[r0:n, h * head:(h + 1) * head] = o.astype(bf16)

            score(0)
            for i in range(len(tasks)):
                if i + 1 < len(tasks):
                    score(i + 1)
                soften(i)
                mix(i)
                if i % n_heads == n_heads - 1 and tasks[i][0] % PARTS == PARTS - 1:
                    for done in range(tasks[i][0] - PARTS + 1, tasks[i][0] + 1):
                        ostore(done).start()
            for t in range(seq // rows):
                ostore(t).wait()
        pl.run_scoped(scope, pltpu.VMEM((1, rows, seq), f32), pltpu.VMEM((1, rows, seq), f32))

    def chip_of(w):
        near = (w * (3 - w)) // 2
        off = near * (3 - 2 * w) + 2 * ((3 - w) // 3)
        plus = near * (2 - w)
        return (chip + off + n_chips) % n_chips, 2 * plus, 1 + 2 * plus + w // 3

    def place_of(v):
        return (v % 3) * (2 - v % 3)

    def rows_load(s, v):
        d, _, _ = chip_of(v // 2)
        return pltpu.make_async_copy(n_all.at[s, d, v % 2], nbuf.at[place_of(v)], a_sem.at[place_of(v)])

    def rows_start(s, v):
        rows_load(s, v).start()

    def phase_d(s):
        def scope(lhs, pst, ost, tb):
            first, later, last = s == 0, s > 0, s == batch - 1

            def left_load(w, own, whole):
                d, slot_p, slot_o = chip_of(w)
                src = ho.at[2 * d + (core if own else other)]
                dst = lhs.at[slot_o if own else slot_p]
                if not whole:
                    src, dst = src.at[:, pl.ds(ff, attn)], dst.at[:, pl.ds(ff, attn)]
                return pltpu.make_async_copy(src, dst, d_sem.at[w, own])

            def left_act(w, own, act):
                @pl.when(first)
                def _():
                    act(left_load(w, own, True))

                @pl.when(later)
                def _():
                    act(left_load(w, own, False))

            def left_start(w, own):
                left_act(w, own, lambda cp: cp.start())

            def left_wait(w, own):
                left_act(w, own, lambda cp: cp.wait())

            def hide(v):
                _, slot_p, slot_o = chip_of(v // 2)
                at = pl.multiple_of((v % 2) * half, half)
                wide = WIDE
                for c in range(0, ff, wide):
                    r = gelu(jnp.dot(nbuf[place_of(v)], wup[:, c:c + wide], preferred_element_type=f32))
                    for k in BOTH:
                        own = 1 - (k + core) % 2
                        slot = slot_p + own * (slot_o - slot_p)
                        lhs[slot, pl.ds(at, half), c:c + wide] = r[k * half:(k + 1) * half]

            def nth(i, k):
                return 2 * i + k

            def swap(b, t, c):
                n = nth(t, c)
                return remote(pst.at[n], pbuf.at[s, b, n], p_s.at[n], p_r.at[s, b * NJ + n], partner)

            def pb_at(t, c):
                return nbuf.at[1, :, cols(nth(t, c))]

            def pb_load(b, t, c):
                return pltpu.make_async_copy(pbuf.at[s, b, nth(t, c)], pb_at(t, c), pb_sem.at[nth(t, c)])

            def pb_start(b, t):
                for c in BOTH:
                    with jax.named_scope("swap_wait"):
                        swap(b, t, c).wait_recv()
                    pb_load(b, t, c).start()

            def t_load(t, c):
                return pltpu.make_async_copy(tin.at[s, :, cols(nth(c, t))], tb.at[c], f_sem.at[c])

            def stored(t):
                for c in BOTH:
                    pltpu.make_async_copy(ost.at[nth(t, c)], pout.at[s, 0, :, cols(nth(c, t))],
                                          os_sem.at[nth(t, c)]).wait()

            def post(b, t):
                stored(t)

                @pl.when(b == 0)
                def _():
                    transit(s, t, right).start()
                    transit(s, 2 + t, left).start()

                @pl.when(b == 1)
                def _():
                    to_left(s, 1, t).start()
                    to_right(s, 1, 2 + t).start()

                @pl.when(b == 2)
                def _():
                    to_right(s, 2, t).start()
                    to_left(s, 2, 2 + t).start()

            def partner_step(b, t):
                @pl.when(b >= 1)
                def _():
                    for c in BOTH:
                        swap(b - 1, t, c).wait_send()

                @pl.when(jnp.logical_and(b == 2, t == 0))
                def _():
                    pb_start(1, 0)
                for c in BOTH:
                    slot_p, _ = block(b, c)
                    r = jnp.dot(lhs[slot_p], wdo[:, cols(nth(c, t))], preferred_element_type=f32)
                    pst[nth(t, c)] = r.astype(bf16)
                for c in BOTH:
                    swap(b, t, c).start()

                @pl.when(jnp.logical_and(jnp.logical_not(last), jnp.logical_and(b == 2, t == 1)))
                def _():
                    post(1, 0)

            def own_step(b, t):
                @pl.when(jnp.logical_and(b == 3, t == 0))
                def _():
                    pb_start(3, 0)

                late = jnp.logical_and(t == 0, jnp.logical_or(b == 3, jnp.logical_and(first, b == 0)))

                @pl.when(jnp.logical_and(t == 0, jnp.logical_not(late)))
                def _():
                    pb_start(b, 1)

                @pl.when(jnp.logical_and(b == 1, t == 1))
                def _():
                    pb_start(2, 0)

                @pl.when(b == 2)
                def _():
                    with jax.named_scope("transit_wait"):
                        for c in BOTH:
                            transit(s, nth(c, t), right).wait_recv()
                    for c in BOTH:
                        t_load(t, c).start()
                for c in BOTH:
                    pb_load(b, t, c).wait()
                for c in BOTH:
                    _, slot_o = block(b, c)
                    r = jnp.dot(lhs[slot_o], wdo[:, cols(nth(c, t))], preferred_element_type=f32)
                    ost[nth(t, c)] = (r + pb_at(t, c)[...].astype(f32)).astype(bf16)

                @pl.when(b == 2)
                def _():
                    for c in BOTH:
                        t_load(t, c).wait()

                        @pl.loop(0, PARTS)
                        def _(r):
                            at = pl.ds(pl.multiple_of(r * part, part), part)
                            ost[nth(t, c), at, :] = (ost[nth(t, c), at, :].astype(f32)
                                                     + tb[c, at, :].astype(f32)).astype(bf16)

                for c in BOTH:
                    @pl.when(b < 3)
                    def _():
                        pltpu.make_async_copy(ost.at[nth(t, c)], pout.at[s, b, :, cols(nth(c, t))],
                                              os_sem.at[nth(t, c)]).start()

                    @pl.when(b == 3)
                    def _():
                        pltpu.make_async_copy(ost.at[nth(t, c)], own_out.at[s, :, cols(nth(c, t))],
                                              os_sem.at[nth(t, c)]).start()

                @pl.when(late)
                def _():
                    pb_start(b, 1)

                @pl.when(jnp.logical_and(last, jnp.logical_and(b == 1, t == 0)))
                def _():
                    post(1, 0)

                @pl.when(jnp.logical_and(b == 2, t == 0))
                def _():
                    post(1, 1)

                @pl.when(jnp.logical_and(t == 1, b % 2 == 0))
                def _():
                    post(b, 0)

            @pl.when(s == batch - 2)
            def _():
                ag_second(s + 1)

            for w in BOTH:
                for own in BOTH:
                    left_start(w, own)

            @pl.when(first)
            def _():
                w_copies[1].wait()
                w_copies[2].wait()

            n_groups = 7

            def since(g, k):
                return (g + 8 - k) // 8

            def step_of(g, groups):
                return sum(since(g, k) for k in groups[1:])

            def units(g):
                return 2 * since(g, 1) + since(g, 2) + 3 * since(g, 3) + 2 * since(g, 6)

            @pl.loop(0, n_groups)
            def _(g):
                @pl.when(g == 1)
                def _():
                    pb_start(0, 0)
                    left_start(2, 0)

                @pl.when(g == 2)
                def _():
                    left_start(2, 1)

                @pl.when(g == 3)
                def _():
                    left_wait(1, 1)
                    left_wait(2, 1)

                @pl.when(g == 4)
                def _():
                    left_start(3, 0)
                    left_start(3, 1)

                @pl.when(later)
                def _():
                    @pl.loop(units(g), units(g + 1))
                    def _(v):
                        with jax.named_scope("n_wait"):
                            rows_load(s, v).wait()

                        @pl.when(jnp.logical_and(v % 3 != 2, v < 2 * n_chips - 1))
                        def _():
                            rows_start(s, v + 1)

                        @pl.when(jnp.logical_and(v == 2 * n_chips - 1, s < batch - 1))
                        def _():
                            first_start(s + 1)
                        with jax.named_scope("hide"):
                            hide(v)

                        @pl.when(v % 3 == 2)
                        def _():
                            rows_start(s, v + 1)

                        @pl.when(v == 3)
                        def _():
                            post(0, 1)

                        @pl.when(v == 6)
                        def _():
                            post(2, 1)

                @pl.when(g == 0)
                def _():
                    left_wait(0, 0)

                @pl.when(g == 1)
                def _():
                    left_wait(0, 1)

                @pl.when(g == 2)
                def _():
                    left_wait(1, 0)
                    left_wait(2, 0)

                @pl.when(g == 5)
                def _():
                    left_wait(3, 0)
                    left_wait(3, 1)

                @pl.when(first)
                def _():
                    @pl.when(g == 2)
                    def _():
                        post(0, 1)

                    @pl.when(g == 5)
                    def _():
                        post(2, 1)

                    @pl.when(g == 6)
                    def _():
                        first_start(s + 1)

                @pl.loop(0, 2)
                def _(t):
                    @pl.when(any_of(g, PARTNER_GROUPS))
                    def _():
                        with jax.named_scope("partner"):
                            partner_step(step_of(g, PARTNER_GROUPS), t)

                    @pl.when(any_of(g, OWN_GROUPS))
                    def _():
                        with jax.named_scope("own"):
                            own_step(step_of(g, OWN_GROUPS), t)

                @pl.when(jnp.logical_and(s < batch - 1, g == 2))
                def _():
                    @pl.when(jnp.logical_and(later, s < batch - 2))
                    def _():
                        ag_second(s + 1)
                    forward(s + 1, (2, 3))

                @pl.when(jnp.logical_and(s < batch - 1, g == n_groups - 1))
                def _():
                    forward(s + 1, (4, 5))

            stored(0)
            stored(1)
            for t in BOTH:
                for c in BOTH:
                    swap(3, t, c).wait_send()

            @pl.when(s < batch - 2)
            def _():
                ag_first(s + 2)
        pl.run_scoped(scope, pltpu.VMEM((4, rows, ff + attn), bf16), pltpu.VMEM((NJ, rows, ncol), bf16),
                      pltpu.VMEM((NJ, rows, ncol), bf16), pltpu.VMEM((2, rows, ncol), bf16))

    def opening(raw, wide):
        kinds = qkv_cols // attn
        per = qkv_cols // LANES
        slots, part_rows = raw.shape[0], raw.shape[1]
        n_parts = dim * per // part_rows
        chunk = wide.shape[0] // per
        chunks = part_rows // (chunk * per)
        xbuf = nbuf.at[1]

        def load(q):
            at = pl.ds(pl.multiple_of(q * part_rows, part_rows), part_rows)
            return pltpu.make_async_copy(wqkv_hbm.at[at], raw.at[q % slots], o_sem.at[q])

        x_start(0, xbuf)
        for q in range(slots):
            load(q).start()
        for cp in v_copies:
            cp.wait()
        with jax.named_scope("send0"):
            for q in range(PARTS):
                normalise(0, xbuf, q)
                if q == 1:
                    n_store(0, xbuf, 0).wait()
                    n_store(0, xbuf, 1).wait()
                    pl.semaphore_wait(barrier, 3)
                    ici_copy(0, 2, chip, 0, right).start()
                    d2d_copy(0, 0, chip, 0, core).start()
            n_store(0, xbuf, 2).wait()
            n_store(0, xbuf, 3).wait()
            ici_copy(0, 3, chip, 1, left).start()
            d2d_copy(0, 1, chip, 1, core).start()
            ag_second(0)
        with jax.named_scope("place"):
            @pl.loop(0, n_parts)
            def _(q):
                load(q).wait()

                @pl.loop(0, chunks)
                def _(i):
                    at = pl.ds(pl.multiple_of(i * (chunk * per), chunk * per), chunk * per)
                    wide[...] = raw[q % slots, at, :].astype(f32)
                    to = pl.ds(pl.multiple_of((q * chunks + i) * chunk, chunk), chunk)
                    for j in range(kinds):
                        for c in range(head // LANES):
                            for g in range(n_heads):
                                row = (j * (head // LANES) + c) * n_heads + g
                                col = j * attn + g * head + c * LANES
                                wqkv[to, col:col + LANES] = wide[pl.ds(row, chunk, stride=per), :].astype(bf16)

                @pl.when(q + slots < n_parts)
                def _():
                    load(q + slots).start()

                @pl.when(q == n_parts - slots)
                def _():
                    w_copies[0].start()
                    first_start(0)

    pl.run_scoped(opening, pltpu.VMEM((6, dim * (qkv_cols // LANES) // 8, LANES), bf16),
                  pltpu.VMEM((LANES * (qkv_cols // LANES), LANES), f32))

    @pl.loop(0, batch)
    def _(s):
        def scope(qkv):
            with jax.named_scope("A"):
                phase_a(s, qkv)

            @pl.when(s > 0)
            def _():
                rows_start(s, 0)
            with jax.named_scope("B"):
                phase_b(qkv)
        pl.run_scoped(scope, pltpu.VMEM((seq, qkv_cols), bf16))
        with jax.named_scope("D"):
            phase_d(s)

    def finish(buf, out):
        n_steps, depth, n_out = batch * PARTS, buf.shape[0], out.shape[0]

        def rows_at(n):
            return n // PARTS, pl.ds(pl.multiple_of((n % PARTS) * part, part), part)

        def loads(n):
            s, at = rows_at(n)
            return [pltpu.make_async_copy(src.at[s, at], buf.at[n % depth, i], y_sem.at[n % depth, i])
                    for i, src in enumerate((own_out, left_out, right_out, x_ref))]

        def store(n):
            s, at = rows_at(n)
            return pltpu.make_async_copy(out.at[n % n_out], y_ref.at[s, at], z_sem.at[n % n_out])

        def begin(n):
            @pl.when(n % PARTS == 0)
            def _():
                with jax.named_scope("last_wait"):
                    for j in range(NJ):
                        to_right(n // PARTS, 2, j).wait_recv()
                        to_left(n // PARTS, 2, j).wait_recv()
            for cp in loads(n):
                cp.start()

        def sweep(start, stop):
            for n in range(start, start + depth):
                begin(n)

            @pl.loop(start, stop)
            def _(n):
                k = n % depth
                for cp in loads(n):
                    cp.wait()

                @pl.when(n >= n_out)
                def _():
                    store(n - n_out).wait()
                for c in range(0, dim, ncol):
                    own, from_left, from_right, x = (buf[k, i, :, c:c + ncol].astype(f32) for i in range(PARTS))
                    branch = (own + from_left + from_right).astype(bf16)
                    out[n % n_out, :, c:c + ncol] = (x + branch.astype(f32)).astype(bf16)
                store(n).start()

                @pl.when(n + depth < stop)
                def _():
                    begin(n + depth)

        sweep(0, n_steps - PARTS)
        sweep(n_steps - PARTS, n_steps)
        for n in range(n_steps - n_out, n_steps):
            store(n).wait()

    with jax.named_scope("finish"):
        pl.run_scoped(finish, pltpu.VMEM((PARTS, PARTS, part, dim), bf16), pltpu.VMEM((3, part, dim), bf16))

    @pl.loop(0, batch)
    def _(s):
        for j in range(NJ):
            to_right(s, 2, j).wait_send()
            to_left(s, 2, j).wait_send()
            transit(s, j, right).wait_send()
        for u in range(2 * n_chips):
            d, hf = unit(u)
            d2d_copy(s, u, d, hf, core).wait_send()
            if u >= 2:
                ici_copy(s, u, d, hf, right).wait_send()


def layer_call(x_blk, ln_gain, ln_bias, wqkv, w_out, w_up, w_down, n_tp):
    batch, rows, dim = x_blk.shape
    ff, attn, qkv_cols = w_up.shape[1], w_out.shape[0], wqkv.shape[0] * LANES // dim
    n_chips = n_tp // 2
    ncol = dim // NJ
    bf16 = jnp.bfloat16
    dma = pltpu.SemaphoreType.DMA
    flops = 2 * batch * n_tp * rows * dim * (qkv_cols + 2 * ff + attn)
    outs = pl.pallas_call(
        layer_kernel,
        name="parallel_layer",
        out_shape=[
            jax.ShapeDtypeStruct((batch, rows, dim), bf16),
            jax.ShapeDtypeStruct((batch, rows, dim), bf16),
            jax.ShapeDtypeStruct((batch, rows, dim), bf16),
            jax.ShapeDtypeStruct((batch, rows, dim), bf16),
            jax.ShapeDtypeStruct((batch, n_chips, 2, rows, dim), bf16),
            jax.ShapeDtypeStruct((n_tp, rows, ff + attn), bf16),
            jax.ShapeDtypeStruct((batch, 4, NJ, rows, ncol), bf16),
            jax.ShapeDtypeStruct((batch, 3, rows, dim), bf16),
            jax.ShapeDtypeStruct((batch, rows, dim), bf16),
        ],
        in_specs=[pl.BlockSpec(memory_space=pl.ANY)] * N_IN,
        out_specs=[pl.BlockSpec(memory_space=pl.ANY)] * N_OUT,
        scratch_shapes=[
            pltpu.VMEM((dim, qkv_cols), bf16), pltpu.VMEM((dim, ff), bf16), pltpu.VMEM((ff + attn, dim), bf16),
            pltpu.VMEM((1, dim), jnp.float32), pltpu.VMEM((1, dim), jnp.float32), pltpu.VMEM((2, rows, dim), bf16),
            dma((batch, 8)), dma((batch, 8)), dma((batch, 8)), dma((batch, 8)),
            dma((NJ,)), dma((batch, 4 * NJ)), dma((batch, NJ)), dma((batch, NJ)),
            dma((batch, 2 * NJ)), dma((batch, 2 * NJ)),
            dma((3,)), dma((2,)), dma((2, 4)), dma((2,)), dma((2,)), dma((n_tp,)), dma((4, 2)), dma((NJ,)), dma((NJ,)),
            dma((2,)), dma((PARTS, PARTS)), dma((3,)),
        ],
        compiler_params=pltpu.CompilerParams(
            collective_id=0, has_side_effects=True, vmem_limit_bytes=67043328),
        cost_estimate=pl.CostEstimate(flops=flops, bytes_accessed=256 << 20, transcendentals=0),
    )(x_blk, ln_gain.reshape(1, dim), ln_bias.reshape(1, dim), wqkv, w_out, w_up, w_down)
    return outs[0]


def solution(mesh):
    n_tp = mesh.shape["tp"]

    def local_layer(x_blk, ln_gain, ln_bias, w_qkv, w_out, w_up, w_down):
        dim = x_blk.shape[2]
        groups, kinds, head = w_qkv.shape[1:]
        wqkv = w_qkv.reshape(dim, groups, kinds, head // LANES, LANES).transpose(0, 2, 3, 1, 4).reshape(-1, LANES)
        return layer_call(x_blk, ln_gain, ln_bias, wqkv, w_out, w_up, w_down, n_tp)

    return jax.shard_map(
        local_layer, mesh=mesh,
        in_specs=(P("dp", "tp", None), P(), P(), P(None, "tp", None, None),
                  P("tp", None), P(None, "tp"), P("tp", None)),
        out_specs=P("dp", "tp", None), check_vma=False)
```
